128 devices in a mesh: rep: 1, shard: 128 (over z, y, x, core).
Axes of the slice: x: 4, y: 4, z: 4, core: 2. Of those that a mesh axis runs over, the one named last changes fastest.
Arguments:
- ratings: float32 [8192, 16384], P(('rep', 'shard'))
- observed: int32 [8192, 16384], P(('rep', 'shard'))
- user_init: float32 [8192, 192], P(('rep', 'shard'))
- item_init: float32 [16384, 192], P(('rep', 'shard'))
Outputs:
- output 1: float32 [8192, 192], P(('rep', 'shard'))
- output 2: float32 [16384, 192], P(('rep', 'shard'))
All inputs are finite; a program needn't handle non-finite values.
Results may differ from the reference program's by a relative error of at most 0.0169468.
Values are sent between devices in bfloat16 or wider.
A program may use at most 1 GiB of HBM per device.

```python
import jax
import jax.numpy as jnp
import math
from jax import lax

GROUP_DEVS = 128
USERS_DEV = 64
ITEMS_DEV = 128
FACTOR_RANK = 192
STRATUM_STEPS = 4
EPOCHS = 2

USERS = USERS_DEV * GROUP_DEVS
ITEMS = ITEMS_DEV * GROUP_DEVS
STEP_SCALE = (USERS_DEV + ITEMS_DEV + FACTOR_RANK) / math.sqrt(FACTOR_RANK)
STEP_SIZE = 0.5 / STEP_SCALE
WEIGHT_DECAY = 0.03 * math.sqrt(USERS_DEV * ITEMS_DEV / FACTOR_RANK)


def setup_inputs(seed: int = 0, part: int = 0) -> dict:
    base_key = jax.random.fold_in(jax.random.key(seed), part)
    sub_keys = jax.random.split(base_key, 6)
    init_scale = FACTOR_RANK ** -0.25
    true_users = jax.random.normal(sub_keys[0], (USERS, FACTOR_RANK), jnp.float32) * init_scale
    true_items = jax.random.normal(sub_keys[1], (ITEMS, FACTOR_RANK), jnp.float32) * init_scale
    rating_noise = 0.3 * jax.random.normal(sub_keys[2], (USERS, ITEMS), jnp.float32)
    ratings = jnp.dot(true_users, true_items.T) + rating_noise
    observed = (jax.random.randint(sub_keys[3], (USERS, ITEMS), 0, 10) < 3).astype(jnp.int32)
    user_init = jax.random.normal(sub_keys[4], (USERS, FACTOR_RANK), jnp.float32) * init_scale
    item_init = jax.random.normal(sub_keys[5], (ITEMS, FACTOR_RANK), jnp.float32) * init_scale
    return {"ratings": ratings, "observed": observed, "user_init": user_init, "item_init": item_init}


def to_bf16(values):
    return values.astype(jnp.bfloat16).astype(jnp.float32)


def reference(ratings, observed, user_init, item_init):
    rating_grid = ratings.reshape(GROUP_DEVS, USERS_DEV, GROUP_DEVS, ITEMS_DEV)
    seen_grid = (observed != 0).reshape(GROUP_DEVS, USERS_DEV, GROUP_DEVS, ITEMS_DEV)
    dev_ids = jnp.arange(GROUP_DEVS)
    user_blocks = user_init.reshape(GROUP_DEVS, USERS_DEV, FACTOR_RANK)
    held_items = item_init.reshape(GROUP_DEVS, ITEMS_DEV, FACTOR_RANK)

    def stratum(loop_state, stratum_idx):
        user_now, held_now = loop_state
        col_ids = (dev_ids + stratum_idx) % GROUP_DEVS
        rating_blk = rating_grid[dev_ids, :, col_ids]
        seen_blk = seen_grid[dev_ids, :, col_ids]

        def step(state_pair, unused):
            user_cur, item_cur = state_pair
            item_bf = to_bf16(item_cur)
            predicted = jnp.einsum("pur,pir->pui", to_bf16(user_cur), item_bf)
            residual = to_bf16(jnp.where(seen_blk, predicted - rating_blk, 0.0))
            user_new = user_cur - STEP_SIZE * (jnp.einsum("pui,pir->pur", residual, item_bf) + WEIGHT_DECAY * user_cur)
            user_bf = to_bf16(user_new)
            predicted = jnp.einsum("pur,pir->pui", user_bf, item_bf)
            residual = to_bf16(jnp.where(seen_blk, predicted - rating_blk, 0.0))
            item_new = item_cur - STEP_SIZE * (jnp.einsum("pui,pur->pir", residual, user_bf) + WEIGHT_DECAY * item_cur)
            return (user_new, item_new), None

        (user_now, held_now), unused = lax.scan(step, (user_now, held_now), None, length=STRATUM_STEPS)
        held_now = jnp.roll(held_now, -1, axis=0)
        return (user_now, held_now), None

    stratum_order = jnp.tile(dev_ids, EPOCHS)
    (user_blocks, held_items), unused = lax.scan(stratum, (user_blocks, held_items), stratum_order)
    return user_blocks.reshape(USERS, FACTOR_RANK), held_items.reshape(ITEMS, FACTOR_RANK)
```

```python
import functools
import math

import jax
import jax.numpy as jnp
from jax import lax
from jax.experimental import pallas as pl
from jax.experimental.pallas import tpu as pltpu
from jax.sharding import PartitionSpec as P

STRATUM_STEPS = 4
EPOCHS = 2
ITEM_BLOCKS = 4
SLOTS = 9
HALF_STEPS = 2 * STRATUM_STEPS
LEAD = SLOTS - HALF_STEPS + 1

ROW_BY_ROW = (((1,), (1,)), ((), ()))
PLAIN = (((1,), (0,)), ((), ()))


def dot(lhs, rhs, dims):
    return lax.dot_general(lhs, rhs, dims, preferred_element_type=jnp.float32)


def worker_device(worker, n_devs):
    if n_devs != 128:
        return worker * ITEM_BLOCKS
    plane = worker // 16
    place = worker + plane * (31 - 2 * worker)
    y = place // 4
    odd = y % 2
    x = place % 4
    x = x + odd * (3 - 2 * x)
    return ((plane * 4 + y) * 4 + x) * 2 + 1


def worker_of(dev, n_devs):
    if n_devs != 128:
        return dev // ITEM_BLOCKS
    chip = dev // 2
    plane = (chip // 16) % 2
    y = (chip // 4) % 4
    x = chip % 4
    place = y * 4 + x + (y % 2) * (3 - 2 * x)
    return place + plane * (31 - 2 * place)


def is_worker(dev, n_devs):
    if n_devs != 128:
        return dev % ITEM_BLOCKS == 0
    return jnp.logical_and(dev % 2 == 1, dev < 64)


def kernel(n_devs, strata, step_size, weight_decay, ratings, user_init, item_init, user_out, item_out, rated, turned,
           arriving, handed, handed_bf, leaving, user, user_bf, item, item_bf, user_start,
           block_send, block_recv, start_send, user_recv, item_recv, hop_send, hop_recv, end_send, end_recv):
    k = ITEM_BLOCKS
    workers = n_devs // k
    items = item_init.shape[0]
    me = lax.axis_index("shard")
    last = k - 1

    def remote(src, dst, send, recv, dev):
        return pltpu.make_async_remote_copy(
            src_ref=src, dst_ref=dst, send_sem=send, recv_sem=recv, device_id={"shard": dev}, device_id_type=pl.DeviceIdType.MESH
        )

    def arrival(like, dst, recv):
        return pltpu.make_async_copy(like, dst, recv)

    def send(src, dst, send_sem, recv_sem, dev):
        @pl.when(dev != me)
        def _():
            remote(src, dst, send_sem, recv_sem, dev).start()

        @pl.when(dev == me)
        def _():
            pltpu.make_async_copy(src, dst, recv_sem).start()

    def wait_sent(src, dst, send_sem, recv_sem, dev):
        @pl.when(dev != me)
        def _():
            remote(src, dst, send_sem, recv_sem, dev).wait_send()

    home = worker_device(me // k, n_devs)
    user_copy = (user_init, user_start.at[me % k], start_send.at[0], user_recv.at[me % k], home)
    item_copy = (item_init, item.at[me % k], start_send.at[1], item_recv.at[me % k], home)
    send(*user_copy)
    send(*item_copy)

    def block_copy(turn):
        worker = (me // k + turn) % workers
        columns = pl.ds(pl.multiple_of(worker * (k * items), 128), k * items)
        return ratings.at[:, columns], rated.at[me], block_send.at[turn], block_recv.at[me], worker_device(worker, n_devs)

    @pl.loop(0, workers)
    def _(turn):
        send(*block_copy(turn))

    @pl.when(is_worker(me, n_devs))
    def _():
        mine = worker_of(me, n_devs)
        first = mine * k
        after = worker_device((mine + 1) % workers, n_devs)

        def wait_block(block):
            arrival(ratings.at[:, pl.ds(0, k * items)], rated.at[block], block_recv.at[block]).wait()

        def hop(stratum):
            slot = (stratum + 1) % n_devs
            return remote(leaving.at[stratum % 2], arriving.at[slot], hop_send.at[stratum % 2], hop_recv.at[slot], after)

        for c in range(k):
            arrival(user_init, user_start.at[c], user_recv.at[c]).wait()
            arrival(item_init, item.at[c], item_recv.at[c]).wait()
            wait_block(first + c)
        for c in range(k):
            if c == 0:
                arriving[0] = user_start[0]
            else:
                handed[c - 1] = user_start[c]
                handed_bf[c - 1] = user_start[c].astype(jnp.bfloat16)
            item_bf[c] = item[c].astype(jnp.bfloat16)

        def slot(work):
            first_product, residual = {}, {}
            for c, half, stratum in work:
                if half == 0:
                    lhs = arriving[stratum % n_devs].astype(jnp.bfloat16) if c == 0 else handed_bf[c - 1]
                else:
                    lhs = user_bf[c]
                if half % 2 == 0:
                    first_product[c] = dot(lhs, item_bf[c], ROW_BY_ROW)
                else:
                    first_product[c] = dot(item_bf[c], lhs, ROW_BY_ROW)
            for c, half, stratum in work:
                if half % 2 == 0:
                    block = (first + c - stratum + 2 * n_devs) % n_devs
                    known = rated[block, :, c * items : (c + 1) * items]
                    if half == 0:
                        turned[c] = known.T
                else:
                    known = turned[c]
                residual[c] = jnp.where(known != known, 0.0, first_product[c] - known).astype(jnp.bfloat16)
            for c, half, stratum in work:
                if half % 2 == 0:
                    if half > 0:
                        old = user[c]
                    elif c == 0:
                        old = arriving[stratum % n_devs]
                    else:
                        old = handed[c - 1]
                    grad = dot(residual[c], item_bf[c], PLAIN)
                    new = old - step_size * (grad + weight_decay * old)
                    new_bf = new.astype(jnp.bfloat16)
                    user_bf[c] = new_bf
                    if half < HALF_STEPS - 2:
                        user[c] = new
                    elif c < last:
                        handed[c] = new
                        handed_bf[c] = new_bf
                    else:
                        leaving[stratum % 2] = new
                else:
                    old = item[c]
                    grad = dot(residual[c], user_bf[c], PLAIN)
                    new = old - step_size * (grad + weight_decay * old)
                    item[c] = new
                    item_bf[c] = new.astype(jnp.bfloat16)

        def work_of(s, stratum, first_only=False):
            work = []
            for c in range(k):
                place = s + LEAD * c
                if place < 0 or (first_only and place >= SLOTS):
                    continue
                if place % SLOTS < HALF_STEPS:
                    work.append((c, place % SLOTS, stratum + place // SLOTS))
            return work

        leave_slot = (HALF_STEPS - 1 - LEAD * last) % SLOTS

        def stratum_body(stratum, ends):
            @pl.when(stratum > 0)
            def _():
                slot_in = stratum % n_devs
                arrival(leaving.at[0], arriving.at[slot_in], hop_recv.at[slot_in]).wait()

            @pl.when(jnp.logical_and(stratum > 0, stratum <= n_devs - k))
            def _():
                wait_block((first - stratum + n_devs) % n_devs)

            for s in range(SLOTS):
                if s == leave_slot and not ends:
                    @pl.when(stratum > 0)
                    def _():
                        hop(stratum - 1).wait_send()

                    hop(stratum).start()
                slot(work_of(s, stratum, ends))

        for s in range(-LEAD * last, 0):
            slot(work_of(s, 0))

        @pl.loop(0, strata - 1)
        def _(stratum):
            stratum_body(stratum, False)

        hop(strata - 2).wait_send()
        stratum_body(strata - 1, True)

        def end_copies(c):
            done = handed.at[c] if c < last else leaving.at[(strata - 1) % 2]
            block = first + c
            return (
                (done, user_out, end_send.at[2 * c], end_recv.at[0], (block + 1) % n_devs),
                (item.at[c], item_out, end_send.at[2 * c + 1], end_recv.at[1], block),
            )

        for c in range(k):
            for copy in end_copies(c):
                send(*copy)
        for c in range(k):
            for copy in end_copies(c):
                wait_sent(*copy)

    wait_sent(*user_copy)
    wait_sent(*item_copy)

    @pl.loop(0, workers)
    def _(turn):
        wait_sent(*block_copy(turn))

    arrival(user_init, user_out, end_recv.at[0]).wait()
    arrival(item_init, item_out, end_recv.at[1]).wait()


def solution(mesh):
    n_devs = mesh.shape["shard"]
    row_spec = P(("rep", "shard"), None)
    k = ITEM_BLOCKS
    workers = n_devs // k

    def local(ratings, observed, user_init, item_init):
        users, rank = user_init.shape
        items = item_init.shape[0]
        step_scale = (users + items + rank) / math.sqrt(rank)
        step_size = 0.5 / step_scale
        weight_decay = 0.03 * math.sqrt(users * items / rank)
        masked = jnp.where(observed != 0, ratings, jnp.nan)
        dma = pltpu.SemaphoreType.DMA
        return pl.pallas_call(
            functools.partial(kernel, n_devs, EPOCHS * n_devs, step_size, weight_decay),
            out_shape=(jax.ShapeDtypeStruct((users, rank), jnp.float32), jax.ShapeDtypeStruct((items, rank), jnp.float32)),
            in_specs=[
                pl.BlockSpec(memory_space=pl.ANY),
                pl.BlockSpec(memory_space=pltpu.VMEM),
                pl.BlockSpec(memory_space=pltpu.VMEM),
            ],
            out_specs=(pl.BlockSpec(memory_space=pltpu.VMEM), pl.BlockSpec(memory_space=pltpu.VMEM)),
            scratch_shapes=[
                pltpu.VMEM((n_devs, users, k * items), jnp.float32),
                pltpu.VMEM((k, items, users), jnp.float32),
                pltpu.VMEM((n_devs, users, rank), jnp.float32),
                pltpu.VMEM((k - 1, users, rank), jnp.float32),
                pltpu.VMEM((k - 1, users, rank), jnp.bfloat16),
                pltpu.VMEM((2, users, rank), jnp.float32),
                pltpu.VMEM((k, users, rank), jnp.float32),
                pltpu.VMEM((k, users, rank), jnp.bfloat16),
                pltpu.VMEM((k, items, rank), jnp.float32),
                pltpu.VMEM((k, items, rank), jnp.bfloat16),
                pltpu.VMEM((k, users, rank), jnp.float32),
                dma((workers,)),
                dma((n_devs,)),
                dma((2,)),
                dma((k,)),
                dma((k,)),
                dma((2,)),
                dma((n_devs,)),
                dma((2 * k,)),
                dma((2,)),
            ],
            compiler_params=pltpu.CompilerParams(has_side_effects=True, vmem_limit_bytes=60 * 2**20),
            name="strata",
        )(masked, user_init, item_init)

    return jax.shard_map(local, mesh=mesh, in_specs=(row_spec,) * 4, out_specs=(row_spec, row_spec), check_vma=False)
```

```python
import functools
import math

import jax
import jax.numpy as jnp
from jax import lax
from jax.experimental import pallas as pl
from jax.experimental.pallas import tpu as pltpu
from jax.sharding import PartitionSpec as P

STRATUM_STEPS = 4
EPOCHS = 2
ITEM_BLOCKS = 4
SLOTS = 9
AHEAD = 8
HALF_STEPS = 2 * STRATUM_STEPS
LEAD = SLOTS - HALF_STEPS + 1

ROW_BY_ROW = (((1,), (1,)), ((), ()))
PLAIN = (((1,), (0,)), ((), ()))


def dot(lhs, rhs, dims):
    return lax.dot_general(lhs, rhs, dims, preferred_element_type=jnp.float32)


def worker_device(worker, n_devs):
    if n_devs != 128:
        return worker * ITEM_BLOCKS
    plane = worker // 16
    place = worker + plane * (31 - 2 * worker)
    y = place // 4
    odd = y % 2
    x = place % 4
    x = x + odd * (3 - 2 * x)
    return ((plane * 4 + y) * 4 + x) * 2 + 1


def worker_of(dev, n_devs):
    if n_devs != 128:
        return dev // ITEM_BLOCKS
    chip = dev // 2
    plane = (chip // 16) % 2
    y = (chip // 4) % 4
    x = chip % 4
    place = y * 4 + x + (y % 2) * (3 - 2 * x)
    return place + plane * (31 - 2 * place)


def is_worker(dev, n_devs):
    if n_devs != 128:
        return dev % ITEM_BLOCKS == 0
    return jnp.logical_and(dev % 2 == 1, dev < 64)


def kernel(n_devs, strata, step_size, weight_decay, ratings, user_init, item_init, user_out, item_out, rated, turned,
           arriving, handed, handed_bf, leaving, user, user_bf, item, item_bf, user_start,
           go, block_send, block_recv, start_send, user_recv, item_recv, hop_send, hop_recv, end_send, end_recv):
    k = ITEM_BLOCKS
    workers = n_devs // k
    items = item_init.shape[0]
    me = lax.axis_index("shard")
    last = k - 1

    def remote(src, dst, send, recv, dev):
        return pltpu.make_async_remote_copy(
            src_ref=src, dst_ref=dst, send_sem=send, recv_sem=recv, device_id={"shard": dev}, device_id_type=pl.DeviceIdType.MESH
        )

    def arrival(like, dst, recv):
        return pltpu.make_async_copy(like, dst, recv)

    def send(src, dst, send_sem, recv_sem, dev):
        @pl.when(dev != me)
        def _():
            remote(src, dst, send_sem, recv_sem, dev).start()

        @pl.when(dev == me)
        def _():
            pltpu.make_async_copy(src, dst, recv_sem).start()

    def wait_sent(src, dst, send_sem, recv_sem, dev):
        @pl.when(dev != me)
        def _():
            remote(src, dst, send_sem, recv_sem, dev).wait_send()

    home = worker_device(me // k, n_devs)
    user_copy = (user_init, user_start.at[me % k], start_send.at[0], user_recv.at[me % k], home)
    item_copy = (item_init, item.at[me % k], start_send.at[1], item_recv.at[me % k], home)
    send(*user_copy)
    send(*item_copy)

    def block_copy(turn):
        worker = (me // k + turn) % workers
        columns = pl.ds(pl.multiple_of(worker * (k * items), 128), k * items)
        return ratings.at[:, columns], rated.at[me], block_send.at[turn], block_recv.at[me], worker_device(worker, n_devs)

    free_turns = jnp.minimum((AHEAD + me % k) // k + 1, workers)

    @pl.loop(0, free_turns)
    def _(turn):
        send(*block_copy(turn))

    @pl.when(jnp.logical_not(is_worker(me, n_devs)))
    def _():
        @pl.loop(free_turns, workers)
        def _(turn):
            pl.semaphore_wait(go, 1)
            send(*block_copy(turn))

    @pl.when(is_worker(me, n_devs))
    def _():
        mine = worker_of(me, n_devs)
        first = mine * k
        after = worker_device((mine + 1) % workers, n_devs)

        def wait_block(block):
            arrival(ratings.at[:, pl.ds(0, k * items)], rated.at[block], block_recv.at[block]).wait()

        def hop(stratum):
            slot = (stratum + 1) % n_devs
            return remote(leaving.at[stratum % 2], arriving.at[slot], hop_send.at[stratum % 2], hop_recv.at[slot], after)

        for c in range(k):
            arrival(user_init, user_start.at[c], user_recv.at[c]).wait()
            arrival(item_init, item.at[c], item_recv.at[c]).wait()
            wait_block(first + c)
        for c in range(k):
            if c == 0:
                arriving[0] = user_start[0]
            else:
                handed[c - 1] = user_start[c]
                handed_bf[c - 1] = user_start[c].astype(jnp.bfloat16)
            item_bf[c] = item[c].astype(jnp.bfloat16)

        def slot(work):
            first_product, residual = {}, {}
            for c, half, stratum in work:
                if half == 0:
                    lhs = arriving[stratum % n_devs].astype(jnp.bfloat16) if c == 0 else handed_bf[c - 1]
                else:
                    lhs = user_bf[c]
                if half % 2 == 0:
                    first_product[c] = dot(lhs, item_bf[c], ROW_BY_ROW)
                else:
                    first_product[c] = dot(item_bf[c], lhs, ROW_BY_ROW)
            for c, half, stratum in work:
                if half % 2 == 0:
                    block = (first + c - stratum + 2 * n_devs) % n_devs
                    known = rated[block, :, c * items : (c + 1) * items]
                    if half == 0:
                        turned[c] = known.T
                else:
                    known = turned[c]
                residual[c] = jnp.where(known != known, 0.0, first_product[c] - known).astype(jnp.bfloat16)
            for c, half, stratum in work:
                if half % 2 == 0:
                    if half > 0:
                        old = user[c]
                    elif c == 0:
                        old = arriving[stratum % n_devs]
                    else:
                        old = handed[c - 1]
                    grad = dot(residual[c], item_bf[c], PLAIN)
                    new = old - step_size * (grad + weight_decay * old)
                    new_bf = new.astype(jnp.bfloat16)
                    user_bf[c] = new_bf
                    if half < HALF_STEPS - 2:
                        user[c] = new
                    elif c < last:
                        handed[c] = new
                        handed_bf[c] = new_bf
                    else:
                        leaving[stratum % 2] = new
                else:
                    old = item[c]
                    grad = dot(residual[c], user_bf[c], PLAIN)
                    new = old - step_size * (grad + weight_decay * old)
                    item[c] = new
                    item_bf[c] = new.astype(jnp.bfloat16)

        def work_of(s, stratum, first_only=False):
            work = []
            for c in range(k):
                place = s + LEAD * c
                if place < 0 or (first_only and place >= SLOTS):
                    continue
                if place % SLOTS < HALF_STEPS:
                    work.append((c, place % SLOTS, stratum + place // SLOTS))
            return work

        leave_slot = (HALF_STEPS - 1 - LEAD * last) % SLOTS

        def stratum_body(stratum, ends):
            @pl.when(stratum > 0)
            def _():
                slot_in = stratum % n_devs
                arrival(leaving.at[0], arriving.at[slot_in], hop_recv.at[slot_in]).wait()

            @pl.when(jnp.logical_and(stratum > 0, stratum <= n_devs - k))
            def _():
                wait_block((first - stratum + n_devs) % n_devs)

            if not ends:
                asked = stratum + AHEAD
                source = (first - asked + 2 * n_devs) % n_devs

                @pl.when(jnp.logical_and(stratum > 0, jnp.logical_and(asked <= n_devs - k, jnp.logical_not(is_worker(source, n_devs)))))
                def _():
                    pl.semaphore_signal(go, inc=1, device_id={"shard": source}, device_id_type=pl.DeviceIdType.MESH)

                turn = (asked + me % k) // k

                @pl.when(jnp.logical_and(jnp.logical_and(turn >= free_turns, turn < workers), (asked + me % k) % k == 0))
                def _():
                    send(*block_copy(turn))

            for s in range(SLOTS):
                if s == leave_slot and not ends:
                    @pl.when(stratum > 0)
                    def _():
                        hop(stratum - 1).wait_send()

                    hop(stratum).start()
                slot(work_of(s, stratum, ends))

        for s in range(-LEAD * last, 0):
            slot(work_of(s, 0))

        @pl.loop(0, strata - 1)
        def _(stratum):
            stratum_body(stratum, False)

        hop(strata - 2).wait_send()
        stratum_body(strata - 1, True)

        def end_copies(c):
            done = handed.at[c] if c < last else leaving.at[(strata - 1) % 2]
            block = first + c
            return (
                (done, user_out, end_send.at[2 * c], end_recv.at[0], (block + 1) % n_devs),
                (item.at[c], item_out, end_send.at[2 * c + 1], end_recv.at[1], block),
            )

        for c in range(k):
            for copy in end_copies(c):
                send(*copy)
        for c in range(k):
            for copy in end_copies(c):
                wait_sent(*copy)

    wait_sent(*user_copy)
    wait_sent(*item_copy)

    @pl.loop(0, workers)
    def _(turn):
        wait_sent(*block_copy(turn))

    arrival(user_init, user_out, end_recv.at[0]).wait()
    arrival(item_init, item_out, end_recv.at[1]).wait()


def solution(mesh):
    n_devs = mesh.shape["shard"]
    row_spec = P(("rep", "shard"), None)
    k = ITEM_BLOCKS
    workers = n_devs // k

    def local(ratings, observed, user_init, item_init):
        users, rank = user_init.shape
        items = item_init.shape[0]
        step_scale = (users + items + rank) / math.sqrt(rank)
        step_size = 0.5 / step_scale
        weight_decay = 0.03 * math.sqrt(users * items / rank)
        masked = jnp.where(observed != 0, ratings, jnp.nan)
        dma = pltpu.SemaphoreType.DMA
        return pl.pallas_call(
            functools.partial(kernel, n_devs, EPOCHS * n_devs, step_size, weight_decay),
            out_shape=(jax.ShapeDtypeStruct((users, rank), jnp.float32), jax.ShapeDtypeStruct((items, rank), jnp.float32)),
            in_specs=[
                pl.BlockSpec(memory_space=pl.ANY),
                pl.BlockSpec(memory_space=pltpu.VMEM),
                pl.BlockSpec(memory_space=pltpu.VMEM),
            ],
            out_specs=(pl.BlockSpec(memory_space=pltpu.VMEM), pl.BlockSpec(memory_space=pltpu.VMEM)),
            scratch_shapes=[
                pltpu.VMEM((n_devs, users, k * items), jnp.float32),
                pltpu.VMEM((k, items, users), jnp.float32),
                pltpu.VMEM((n_devs, users, rank), jnp.float32),
                pltpu.VMEM((k - 1, users, rank), jnp.float32),
                pltpu.VMEM((k - 1, users, rank), jnp.bfloat16),
                pltpu.VMEM((2, users, rank), jnp.float32),
                pltpu.VMEM((k, users, rank), jnp.float32),
                pltpu.VMEM((k, users, rank), jnp.bfloat16),
                pltpu.VMEM((k, items, rank), jnp.float32),
                pltpu.VMEM((k, items, rank), jnp.bfloat16),
                pltpu.VMEM((k, users, rank), jnp.float32),
                pltpu.SemaphoreType.REGULAR,
                dma((workers,)),
                dma((n_devs,)),
                dma((2,)),
                dma((k,)),
                dma((k,)),
                dma((2,)),
                dma((n_devs,)),
                dma((2 * k,)),
                dma((2,)),
            ],
            compiler_params=pltpu.CompilerParams(has_side_effects=True, vmem_limit_bytes=60 * 2**20),
            name="strata",
        )(masked, user_init, item_init)

    return jax.shard_map(local, mesh=mesh, in_specs=(row_spec,) * 4, out_specs=(row_spec, row_spec), check_vma=False)
```

```python
import functools
import math

import jax
import jax.numpy as jnp
from jax import lax
from jax.experimental import pallas as pl
from jax.experimental.pallas import tpu as pltpu
from jax.sharding import PartitionSpec as P

STRATUM_STEPS = 4
EPOCHS = 2
ITEM_BLOCKS = 4
SLOTS = 9
HALF_STEPS = 2 * STRATUM_STEPS
LEAD = SLOTS - HALF_STEPS + 1

ROW_BY_ROW = (((1,), (1,)), ((), ()))
PLAIN = (((1,), (0,)), ((), ()))


def dot(lhs, rhs, dims):
    return lax.dot_general(lhs, rhs, dims, preferred_element_type=jnp.float32)


def worker_device(worker, n_devs):
    if n_devs != 128:
        return worker * ITEM_BLOCKS
    plane = worker // 16
    place = worker + plane * (31 - 2 * worker)
    y = place // 4
    odd = y % 2
    x = place % 4
    x = x + odd * (3 - 2 * x)
    return ((x * 4 + y) * 4 + plane) * 2 + 1


def worker_of(dev, n_devs):
    if n_devs != 128:
        return dev // ITEM_BLOCKS
    chip = dev // 2
    plane = chip % 2
    y = (chip // 4) % 4
    x = chip // 16
    place = y * 4 + x + (y % 2) * (3 - 2 * x)
    return place + plane * (31 - 2 * place)


def is_worker(dev, n_devs):
    if n_devs != 128:
        return dev % ITEM_BLOCKS == 0
    return jnp.logical_and(dev % 2 == 1, dev % 8 < 4)


def kernel(n_devs, strata, step_size, weight_decay, ratings, user_init, item_init, user_out, item_out, rated, turned,
           arriving, handed, handed_bf, leaving, user, user_bf, item, item_bf, user_start,
           block_send, block_recv, start_send, user_recv, item_recv, hop_send, hop_recv, end_send, end_recv):
    k = ITEM_BLOCKS
    workers = n_devs // k
    items = item_init.shape[0]
    me = lax.axis_index("shard")
    last = k - 1

    def remote(src, dst, send, recv, dev):
        return pltpu.make_async_remote_copy(
            src_ref=src, dst_ref=dst, send_sem=send, recv_sem=recv, device_id={"shard": dev}, device_id_type=pl.DeviceIdType.MESH
        )

    def arrival(like, dst, recv):
        return pltpu.make_async_copy(like, dst, recv)

    def send(src, dst, send_sem, recv_sem, dev):
        @pl.when(dev != me)
        def _():
            remote(src, dst, send_sem, recv_sem, dev).start()

        @pl.when(dev == me)
        def _():
            pltpu.make_async_copy(src, dst, recv_sem).start()

    def wait_sent(src, dst, send_sem, recv_sem, dev):
        @pl.when(dev != me)
        def _():
            remote(src, dst, send_sem, recv_sem, dev).wait_send()

    home = worker_device(me // k, n_devs)
    user_copy = (user_init, user_start.at[me % k], start_send.at[0], user_recv.at[me % k], home)
    item_copy = (item_init, item.at[me % k], start_send.at[1], item_recv.at[me % k], home)
    send(*user_copy)
    send(*item_copy)

    def block_copy(turn):
        worker = (me // k + turn) % workers
        columns = pl.ds(pl.multiple_of(worker * (k * items), 128), k * items)
        return ratings.at[:, columns], rated.at[me], block_send.at[turn], block_recv.at[me], worker_device(worker, n_devs)

    @pl.loop(0, workers)
    def _(turn):
        send(*block_copy(turn))

    @pl.when(is_worker(me, n_devs))
    def _():
        mine = worker_of(me, n_devs)
        first = mine * k
        after = worker_device((mine + 1) % workers, n_devs)

        def wait_block(block):
            arrival(ratings.at[:, pl.ds(0, k * items)], rated.at[block], block_recv.at[block]).wait()

        def hop(stratum):
            slot = (stratum + 1) % n_devs
            return remote(leaving.at[stratum % 2], arriving.at[slot], hop_send.at[stratum % 2], hop_recv.at[slot], after)

        for c in range(k):
            arrival(user_init, user_start.at[c], user_recv.at[c]).wait()
            arrival(item_init, item.at[c], item_recv.at[c]).wait()
            wait_block(first + c)
        for c in range(k):
            if c == 0:
                arriving[0] = user_start[0]
            else:
                handed[c - 1] = user_start[c]
                handed_bf[c - 1] = user_start[c].astype(jnp.bfloat16)
            item_bf[c] = item[c].astype(jnp.bfloat16)

        def slot(work):
            first_product, residual = {}, {}
            for c, half, stratum in work:
                if half == 0:
                    lhs = arriving[stratum % n_devs].astype(jnp.bfloat16) if c == 0 else handed_bf[c - 1]
                else:
                    lhs = user_bf[c]
                if half % 2 == 0:
                    first_product[c] = dot(lhs, item_bf[c], ROW_BY_ROW)
                else:
                    first_product[c] = dot(item_bf[c], lhs, ROW_BY_ROW)
            for c, half, stratum in work:
                if half % 2 == 0:
                    block = (first + c - stratum + 2 * n_devs) % n_devs
                    known = rated[block, :, c * items : (c + 1) * items]
                    if half == 0:
                        turned[c] = known.T
                else:
                    known = turned[c]
                residual[c] = jnp.where(known != known, 0.0, first_product[c] - known).astype(jnp.bfloat16)
            for c, half, stratum in work:
                if half % 2 == 0:
                    if half > 0:
                        old = user[c]
                    elif c == 0:
                        old = arriving[stratum % n_devs]
                    else:
                        old = handed[c - 1]
                    grad = dot(residual[c], item_bf[c], PLAIN)
                    new = old - step_size * (grad + weight_decay * old)
                    new_bf = new.astype(jnp.bfloat16)
                    user_bf[c] = new_bf
                    if half < HALF_STEPS - 2:
                        user[c] = new
                    elif c < last:
                        handed[c] = new
                        handed_bf[c] = new_bf
                    else:
                        leaving[stratum % 2] = new
                else:
                    old = item[c]
                    grad = dot(residual[c], user_bf[c], PLAIN)
                    new = old - step_size * (grad + weight_decay * old)
                    item[c] = new
                    item_bf[c] = new.astype(jnp.bfloat16)

        def work_of(s, stratum, first_only=False):
            work = []
            for c in range(k):
                place = s + LEAD * c
                if place < 0 or (first_only and place >= SLOTS):
                    continue
                if place % SLOTS < HALF_STEPS:
                    work.append((c, place % SLOTS, stratum + place // SLOTS))
            return work

        leave_slot = (HALF_STEPS - 1 - LEAD * last) % SLOTS

        def stratum_body(stratum, ends):
            @pl.when(stratum > 0)
            def _():
                slot_in = stratum % n_devs
                arrival(leaving.at[0], arriving.at[slot_in], hop_recv.at[slot_in]).wait()

            @pl.when(jnp.logical_and(stratum > 0, stratum <= n_devs - k))
            def _():
                wait_block((first - stratum + n_devs) % n_devs)

            for s in range(SLOTS):
                if s == leave_slot and not ends:
                    @pl.when(stratum > 0)
                    def _():
                        hop(stratum - 1).wait_send()

                    hop(stratum).start()
                slot(work_of(s, stratum, ends))

        for s in range(-LEAD * last, 0):
            slot(work_of(s, 0))

        @pl.loop(0, strata - 1)
        def _(stratum):
            stratum_body(stratum, False)

        hop(strata - 2).wait_send()
        stratum_body(strata - 1, True)

        def end_copies(c):
            done = handed.at[c] if c < last else leaving.at[(strata - 1) % 2]
            block = first + c
            return (
                (done, user_out, end_send.at[2 * c], end_recv.at[0], (block + 1) % n_devs),
                (item.at[c], item_out, end_send.at[2 * c + 1], end_recv.at[1], block),
            )

        for c in range(k):
            for copy in end_copies(c):
                send(*copy)
        for c in range(k):
            for copy in end_copies(c):
                wait_sent(*copy)

    wait_sent(*user_copy)
    wait_sent(*item_copy)

    @pl.loop(0, workers)
    def _(turn):
        wait_sent(*block_copy(turn))

    arrival(user_init, user_out, end_recv.at[0]).wait()
    arrival(item_init, item_out, end_recv.at[1]).wait()


def solution(mesh):
    n_devs = mesh.shape["shard"]
    row_spec = P(("rep", "shard"), None)
    k = ITEM_BLOCKS
    workers = n_devs // k

    def local(ratings, observed, user_init, item_init):
        users, rank = user_init.shape
        items = item_init.shape[0]
        step_scale = (users + items + rank) / math.sqrt(rank)
        step_size = 0.5 / step_scale
        weight_decay = 0.03 * math.sqrt(users * items / rank)
        masked = jnp.where(observed != 0, ratings, jnp.nan)
        dma = pltpu.SemaphoreType.DMA
        return pl.pallas_call(
            functools.partial(kernel, n_devs, EPOCHS * n_devs, step_size, weight_decay),
            out_shape=(jax.ShapeDtypeStruct((users, rank), jnp.float32), jax.ShapeDtypeStruct((items, rank), jnp.float32)),
            in_specs=[
                pl.BlockSpec(memory_space=pl.ANY),
                pl.BlockSpec(memory_space=pltpu.VMEM),
                pl.BlockSpec(memory_space=pltpu.VMEM),
            ],
            out_specs=(pl.BlockSpec(memory_space=pltpu.VMEM), pl.BlockSpec(memory_space=pltpu.VMEM)),
            scratch_shapes=[
                pltpu.VMEM((n_devs, users, k * items), jnp.float32),
                pltpu.VMEM((k, items, users), jnp.float32),
                pltpu.VMEM((n_devs, users, rank), jnp.float32),
                pltpu.VMEM((k - 1, users, rank), jnp.float32),
                pltpu.VMEM((k - 1, users, rank), jnp.bfloat16),
                pltpu.VMEM((2, users, rank), jnp.float32),
                pltpu.VMEM((k, users, rank), jnp.float32),
                pltpu.VMEM((k, users, rank), jnp.bfloat16),
                pltpu.VMEM((k, items, rank), jnp.float32),
                pltpu.VMEM((k, items, rank), jnp.bfloat16),
                pltpu.VMEM((k, users, rank), jnp.float32),
                dma((workers,)),
                dma((n_devs,)),
                dma((2,)),
                dma((k,)),
                dma((k,)),
                dma((2,)),
                dma((n_devs,)),
                dma((2 * k,)),
                dma((2,)),
            ],
            compiler_params=pltpu.CompilerParams(has_side_effects=True, vmem_limit_bytes=60 * 2**20),
            name="strata",
        )(masked, user_init, item_init)

    return jax.shard_map(local, mesh=mesh, in_specs=(row_spec,) * 4, out_specs=(row_spec, row_spec), check_vma=False)
```

```python
import functools
import math

import jax
import jax.numpy as jnp
from jax import lax
from jax.experimental import pallas as pl
from jax.experimental.pallas import tpu as pltpu
from jax.sharding import PartitionSpec as P

STRATUM_STEPS = 4
EPOCHS = 2
ITEM_BLOCKS = 4
SLOTS = 9
HALF_STEPS = 2 * STRATUM_STEPS
LEAD = SLOTS - HALF_STEPS + 1

ROW_BY_ROW = (((1,), (1,)), ((), ()))
PLAIN = (((1,), (0,)), ((), ()))


def dot(lhs, rhs, dims):
    return lax.dot_general(lhs, rhs, dims, preferred_element_type=jnp.float32)


def worker_device(worker, n_devs):
    if n_devs != 128:
        return worker * ITEM_BLOCKS
    plane = worker // 16
    place = worker + plane * (31 - 2 * worker)
    y = place // 4
    odd = y % 2
    x = place % 4
    x = x + odd * (3 - 2 * x)
    return ((plane * 8 + y) * 4 + x) * 2 + 1


def worker_of(dev, n_devs):
    if n_devs != 128:
        return dev // ITEM_BLOCKS
    chip = dev // 2
    plane = (chip // 32) % 2
    y = (chip // 4) % 4
    x = chip % 4
    place = y * 4 + x + (y % 2) * (3 - 2 * x)
    return place + plane * (31 - 2 * place)


def is_worker(dev, n_devs):
    if n_devs != 128:
        return dev % ITEM_BLOCKS == 0
    return jnp.logical_and(dev % 2 == 1, (dev // 32) % 2 == 0)


def partner(dev):
    return dev + 1 - 2 * (dev % 2)


def kernel(n_devs, strata, step_size, weight_decay, ratings, user_init, item_init, user_out, item_out, rated, turned,
           arriving, handed, handed_bf, leaving, user, user_bf, item, item_bf, user_start,
           relay_send, block_send, block_recv, start_send, user_recv, item_recv, hop_send, hop_recv, end_send, end_recv):
    k = ITEM_BLOCKS
    workers = n_devs // k
    items = item_init.shape[0]
    me = lax.axis_index("shard")
    last = k - 1
    other = partner(me)

    def remote(src, dst, send, recv, dev):
        return pltpu.make_async_remote_copy(
            src_ref=src, dst_ref=dst, send_sem=send, recv_sem=recv, device_id={"shard": dev}, device_id_type=pl.DeviceIdType.MESH
        )

    def arrival(like, dst, recv):
        return pltpu.make_async_copy(like, dst, recv)

    def send(src, dst, send_sem, recv_sem, dev):
        @pl.when(dev != me)
        def _():
            remote(src, dst, send_sem, recv_sem, dev).start()

        @pl.when(dev == me)
        def _():
            pltpu.make_async_copy(src, dst, recv_sem).start()

    def wait_sent(src, dst, send_sem, recv_sem, dev):
        @pl.when(dev != me)
        def _():
            remote(src, dst, send_sem, recv_sem, dev).wait_send()

    home = worker_device(me // k, n_devs)
    user_copy = (user_init, user_start.at[me % k], start_send.at[0], user_recv.at[me % k], home)
    item_copy = (item_init, item.at[me % k], start_send.at[1], item_recv.at[me % k], home)
    send(*user_copy)
    send(*item_copy)

    def columns_of(dev, turn):
        worker = (dev // k + turn) % workers
        return worker_device(worker, n_devs), pl.ds(pl.multiple_of(worker * (k * items), 128), k * items)

    def block_copy(turn):
        to, columns = columns_of(me, turn)
        return remote(ratings.at[:, columns], rated.at[me], block_send.at[turn], block_recv.at[me], to)

    def aside_copy(turn):
        _, columns = columns_of(me, turn)
        return remote(ratings.at[:, columns], rated.at[turn], block_send.at[turn], block_recv.at[turn], other)

    def relay_copy(turn):
        to, _ = columns_of(other, turn)
        return remote(rated.at[turn], rated.at[other], relay_send.at[turn], block_recv.at[other], to)

    def own_columns():
        return ratings.at[:, pl.ds(pl.multiple_of(worker_of(me, n_devs) * (k * items), 128), k * items)]

    working = is_worker(me, n_devs)
    relaying = is_worker(other, n_devs)

    @pl.when(working)
    def _():
        pltpu.make_async_copy(own_columns(), rated.at[me], block_recv.at[me]).start()

        @pl.loop(0, workers)
        def _(turn):
            to, _ = columns_of(me, turn)

            @pl.when(to != me)
            def _():
                aside_copy(turn).start()

    @pl.when(jnp.logical_not(working))
    def _():
        @pl.loop(0, workers)
        def _(turn):
            @pl.when(relaying)
            def _():
                to, _ = columns_of(other, turn)

                @pl.when(to != other)
                def _():
                    arrival(ratings.at[:, pl.ds(0, k * items)], rated.at[turn], block_recv.at[turn]).wait()
                    relay_copy(turn).start()

            block_copy(turn).start()

    @pl.when(working)
    def _():
        mine = worker_of(me, n_devs)
        first = mine * k
        after = worker_device((mine + 1) % workers, n_devs)

        def wait_block(block):
            arrival(ratings.at[:, pl.ds(0, k * items)], rated.at[block], block_recv.at[block]).wait()

        def hop(stratum):
            slot = (stratum + 1) % n_devs
            return remote(leaving.at[stratum % 2], arriving.at[slot], hop_send.at[stratum % 2], hop_recv.at[slot], after)

        for c in range(k):
            arrival(user_init, user_start.at[c], user_recv.at[c]).wait()
            arrival(item_init, item.at[c], item_recv.at[c]).wait()
            wait_block(first + c)
        for c in range(k):
            if c == 0:
                arriving[0] = user_start[0]
            else:
                handed[c - 1] = user_start[c]
                handed_bf[c - 1] = user_start[c].astype(jnp.bfloat16)
            item_bf[c] = item[c].astype(jnp.bfloat16)

        def slot(work):
            first_product, residual = {}, {}
            for c, half, stratum in work:
                if half == 0:
                    lhs = arriving[stratum % n_devs].astype(jnp.bfloat16) if c == 0 else handed_bf[c - 1]
                else:
                    lhs = user_bf[c]
                if half % 2 == 0:
                    first_product[c] = dot(lhs, item_bf[c], ROW_BY_ROW)
                else:
                    first_product[c] = dot(item_bf[c], lhs, ROW_BY_ROW)
            for c, half, stratum in work:
                if half % 2 == 0:
                    block = (first + c - stratum + 2 * n_devs) % n_devs
                    known = rated[block, :, c * items : (c + 1) * items]
                    if half == 0:
                        turned[c] = known.T
                else:
                    known = turned[c]
                residual[c] = jnp.where(known != known, 0.0, first_product[c] - known).astype(jnp.bfloat16)
            for c, half, stratum in work:
                if half % 2 == 0:
                    if half > 0:
                        old = user[c]
                    elif c == 0:
                        old = arriving[stratum % n_devs]
                    else:
                        old = handed[c - 1]
                    grad = dot(residual[c], item_bf[c], PLAIN)
                    new = old - step_size * (grad + weight_decay * old)
                    new_bf = new.astype(jnp.bfloat16)
                    user_bf[c] = new_bf
                    if half < HALF_STEPS - 2:
                        user[c] = new
                    elif c < last:
                        handed[c] = new
                        handed_bf[c] = new_bf
                    else:
                        leaving[stratum % 2] = new
                else:
                    old = item[c]
                    grad = dot(residual[c], user_bf[c], PLAIN)
                    new = old - step_size * (grad + weight_decay * old)
                    item[c] = new
                    item_bf[c] = new.astype(jnp.bfloat16)

        def work_of(s, stratum, first_only=False):
            work = []
            for c in range(k):
                place = s + LEAD * c
                if place < 0 or (first_only and place >= SLOTS):
                    continue
                if place % SLOTS < HALF_STEPS:
                    work.append((c, place % SLOTS, stratum + place // SLOTS))
            return work

        leave_slot = (HALF_STEPS - 1 - LEAD * last) % SLOTS

        def stratum_body(stratum, ends):
            @pl.when(stratum > 0)
            def _():
                slot_in = stratum % n_devs
                arrival(leaving.at[0], arriving.at[slot_in], hop_recv.at[slot_in]).wait()

            @pl.when(jnp.logical_and(stratum > 0, stratum <= n_devs - k))
            def _():
                wait_block((first - stratum + n_devs) % n_devs)

            for s in range(SLOTS):
                if s == leave_slot and not ends:
                    @pl.when(stratum > 0)
                    def _():
                        hop(stratum - 1).wait_send()

                    hop(stratum).start()
                slot(work_of(s, stratum, ends))

        for s in range(-LEAD * last, 0):
            slot(work_of(s, 0))

        @pl.loop(0, strata - 1)
        def _(stratum):
            stratum_body(stratum, False)

        hop(strata - 2).wait_send()
        stratum_body(strata - 1, True)

        def end_copies(c):
            done = handed.at[c] if c < last else leaving.at[(strata - 1) % 2]
            block = first + c
            return (
                (done, user_out, end_send.at[2 * c], end_recv.at[0], (block + 1) % n_devs),
                (item.at[c], item_out, end_send.at[2 * c + 1], end_recv.at[1], block),
            )

        for c in range(k):
            for copy in end_copies(c):
                send(*copy)
        for c in range(k):
            for copy in end_copies(c):
                wait_sent(*copy)

    wait_sent(*user_copy)
    wait_sent(*item_copy)

    @pl.loop(0, workers)
    def _(turn):
        @pl.when(working)
        def _():
            to, _ = columns_of(me, turn)

            @pl.when(to != me)
            def _():
                aside_copy(turn).wait_send()

        @pl.when(jnp.logical_not(working))
        def _():
            block_copy(turn).wait_send()

            @pl.when(relaying)
            def _():
                to, _ = columns_of(other, turn)

                @pl.when(to != other)
                def _():
                    relay_copy(turn).wait_send()

    arrival(user_init, user_out, end_recv.at[0]).wait()
    arrival(item_init, item_out, end_recv.at[1]).wait()


def solution(mesh):
    n_devs = mesh.shape["shard"]
    row_spec = P(("rep", "shard"), None)
    k = ITEM_BLOCKS
    workers = n_devs // k

    def local(ratings, observed, user_init, item_init):
        users, rank = user_init.shape
        items = item_init.shape[0]
        step_scale = (users + items + rank) / math.sqrt(rank)
        step_size = 0.5 / step_scale
        weight_decay = 0.03 * math.sqrt(users * items / rank)
        masked = jnp.where(observed != 0, ratings, jnp.nan)
        dma = pltpu.SemaphoreType.DMA
        return pl.pallas_call(
            functools.partial(kernel, n_devs, EPOCHS * n_devs, step_size, weight_decay),
            out_shape=(jax.ShapeDtypeStruct((users, rank), jnp.float32), jax.ShapeDtypeStruct((items, rank), jnp.float32)),
            in_specs=[
                pl.BlockSpec(memory_space=pl.ANY),
                pl.BlockSpec(memory_space=pltpu.VMEM),
                pl.BlockSpec(memory_space=pltpu.VMEM),
            ],
            out_specs=(pl.BlockSpec(memory_space=pltpu.VMEM), pl.BlockSpec(memory_space=pltpu.VMEM)),
            scratch_shapes=[
                pltpu.VMEM((n_devs, users, k * items), jnp.float32),
                pltpu.VMEM((k, items, users), jnp.float32),
                pltpu.VMEM((n_devs, users, rank), jnp.float32),
                pltpu.VMEM((k - 1, users, rank), jnp.float32),
                pltpu.VMEM((k - 1, users, rank), jnp.bfloat16),
                pltpu.VMEM((2, users, rank), jnp.float32),
                pltpu.VMEM((k, users, rank), jnp.float32),
                pltpu.VMEM((k, users, rank), jnp.bfloat16),
                pltpu.VMEM((k, items, rank), jnp.float32),
                pltpu.VMEM((k, items, rank), jnp.bfloat16),
                pltpu.VMEM((k, users, rank), jnp.float32),
                dma((workers,)),
                dma((workers,)),
                dma((n_devs,)),
                dma((2,)),
                dma((k,)),
                dma((k,)),
                dma((2,)),
                dma((n_devs,)),
                dma((2 * k,)),
                dma((2,)),
            ],
            compiler_params=pltpu.CompilerParams(has_side_effects=True, vmem_limit_bytes=60 * 2**20),
            name="strata",
        )(masked, user_init, item_init)

    return jax.shard_map(local, mesh=mesh, in_specs=(row_spec,) * 4, out_specs=(row_spec, row_spec), check_vma=False)
```

```python
import functools
import math

import jax
import jax.numpy as jnp
from jax import lax
from jax.experimental import pallas as pl
from jax.experimental.pallas import tpu as pltpu
from jax.sharding import PartitionSpec as P

STRATUM_STEPS = 4
EPOCHS = 2
ITEM_BLOCKS = 4
SLOTS = 9
SOON = 2
HALF_STEPS = 2 * STRATUM_STEPS
LEAD = SLOTS - HALF_STEPS + 1

ROW_BY_ROW = (((1,), (1,)), ((), ()))
PLAIN = (((1,), (0,)), ((), ()))


def dot(lhs, rhs, dims):
    return lax.dot_general(lhs, rhs, dims, preferred_element_type=jnp.float32)


def worker_device(worker, n_devs):
    if n_devs != 128:
        return worker * ITEM_BLOCKS
    plane = worker // 16
    place = worker + plane * (31 - 2 * worker)
    y = place // 4
    odd = y % 2
    x = place % 4
    x = x + odd * (3 - 2 * x)
    return ((plane * 4 + y) * 4 + x) * 2 + 1


def worker_of(dev, n_devs):
    if n_devs != 128:
        return dev // ITEM_BLOCKS
    chip = dev // 2
    plane = (chip // 16) % 2
    y = (chip // 4) % 4
    x = chip % 4
    place = y * 4 + x + (y % 2) * (3 - 2 * x)
    return place + plane * (31 - 2 * place)


def is_worker(dev, n_devs):
    if n_devs != 128:
        return dev % ITEM_BLOCKS == 0
    return jnp.logical_and(dev % 2 == 1, dev < 64)


def kernel(n_devs, strata, step_size, weight_decay, ratings, user_init, item_init, user_out, item_out, rated, turned,
           arriving, handed, handed_bf, leaving, user, user_bf, item, item_bf, user_start,
           block_send, block_recv, start_send, user_recv, item_recv, hop_send, hop_recv, end_send, end_recv):
    k = ITEM_BLOCKS
    workers = n_devs // k
    items = item_init.shape[0]
    me = lax.axis_index("shard")
    last = k - 1

    def remote(src, dst, send, recv, dev):
        return pltpu.make_async_remote_copy(
            src_ref=src, dst_ref=dst, send_sem=send, recv_sem=recv, device_id={"shard": dev}, device_id_type=pl.DeviceIdType.MESH
        )

    def arrival(like, dst, recv):
        return pltpu.make_async_copy(like, dst, recv)

    def send(src, dst, send_sem, recv_sem, dev):
        @pl.when(dev != me)
        def _():
            remote(src, dst, send_sem, recv_sem, dev).start()

        @pl.when(dev == me)
        def _():
            pltpu.make_async_copy(src, dst, recv_sem).start()

    def wait_sent(src, dst, send_sem, recv_sem, dev):
        @pl.when(dev != me)
        def _():
            remote(src, dst, send_sem, recv_sem, dev).wait_send()

    home = worker_device(me // k, n_devs)
    user_copy = (user_init, user_start.at[me % k], start_send.at[0], user_recv.at[me % k], home)
    item_copy = (item_init, item.at[me % k], start_send.at[1], item_recv.at[me % k], home)
    send(*user_copy)
    send(*item_copy)

    def block_copy(turn):
        worker = (me // k + turn) % workers
        columns = pl.ds(pl.multiple_of(worker * (k * items), 128), k * items)
        return ratings.at[:, columns], rated.at[me], block_send.at[turn], block_recv.at[me], worker_device(worker, n_devs)

    working = is_worker(me, n_devs)

    @pl.loop(0, SOON)
    def _(turn):
        send(*block_copy(turn))

    @pl.when(jnp.logical_not(working))
    def _():
        wait_sent(*user_copy)
        wait_sent(*item_copy)
        wait_sent(*block_copy(0))

        @pl.loop(SOON, workers)
        def _(turn):
            send(*block_copy(turn))

    @pl.when(working)
    def _():
        mine = worker_of(me, n_devs)
        first = mine * k
        after = worker_device((mine + 1) % workers, n_devs)

        def wait_block(block):
            arrival(ratings.at[:, pl.ds(0, k * items)], rated.at[block], block_recv.at[block]).wait()

        def hop(stratum):
            slot = (stratum + 1) % n_devs
            return remote(leaving.at[stratum % 2], arriving.at[slot], hop_send.at[stratum % 2], hop_recv.at[slot], after)

        for c in range(k):
            arrival(user_init, user_start.at[c], user_recv.at[c]).wait()
            arrival(item_init, item.at[c], item_recv.at[c]).wait()
            wait_block(first + c)
        for c in range(k):
            if c == 0:
                arriving[0] = user_start[0]
            else:
                handed[c - 1] = user_start[c]
                handed_bf[c - 1] = user_start[c].astype(jnp.bfloat16)
            item_bf[c] = item[c].astype(jnp.bfloat16)

        def slot(work):
            first_product, residual = {}, {}
            for c, half, stratum in work:
                if half == 0:
                    lhs = arriving[stratum % n_devs].astype(jnp.bfloat16) if c == 0 else handed_bf[c - 1]
                else:
                    lhs = user_bf[c]
                if half % 2 == 0:
                    first_product[c] = dot(lhs, item_bf[c], ROW_BY_ROW)
                else:
                    first_product[c] = dot(item_bf[c], lhs, ROW_BY_ROW)
            for c, half, stratum in work:
                if half % 2 == 0:
                    block = (first + c - stratum + 2 * n_devs) % n_devs
                    known = rated[block, :, c * items : (c + 1) * items]
                    if half == 0:
                        turned[c] = known.T
                else:
                    known = turned[c]
                residual[c] = jnp.where(known != known, 0.0, first_product[c] - known).astype(jnp.bfloat16)
            for c, half, stratum in work:
                if half % 2 == 0:
                    if half > 0:
                        old = user[c]
                    elif c == 0:
                        old = arriving[stratum % n_devs]
                    else:
                        old = handed[c - 1]
                    grad = dot(residual[c], item_bf[c], PLAIN)
                    new = old - step_size * (grad + weight_decay * old)
                    new_bf = new.astype(jnp.bfloat16)
                    user_bf[c] = new_bf
                    if half < HALF_STEPS - 2:
                        user[c] = new
                    elif c < last:
                        handed[c] = new
                        handed_bf[c] = new_bf
                    else:
                        leaving[stratum % 2] = new
                else:
                    old = item[c]
                    grad = dot(residual[c], user_bf[c], PLAIN)
                    new = old - step_size * (grad + weight_decay * old)
                    item[c] = new
                    item_bf[c] = new.astype(jnp.bfloat16)

        def work_of(s, stratum, first_only=False):
            work = []
            for c in range(k):
                place = s + LEAD * c
                if place < 0 or (first_only and place >= SLOTS):
                    continue
                if place % SLOTS < HALF_STEPS:
                    work.append((c, place % SLOTS, stratum + place // SLOTS))
            return work

        leave_slot = (HALF_STEPS - 1 - LEAD * last) % SLOTS

        def stratum_body(stratum, ends):
            @pl.when(stratum > 0)
            def _():
                slot_in = stratum % n_devs
                arrival(leaving.at[0], arriving.at[slot_in], hop_recv.at[slot_in]).wait()

            @pl.when(jnp.logical_and(stratum > 0, stratum <= n_devs - k))
            def _():
                wait_block((first - stratum + n_devs) % n_devs)

            for s in range(SLOTS):
                if s == leave_slot and not ends:
                    @pl.when(stratum > 0)
                    def _():
                        hop(stratum - 1).wait_send()

                    hop(stratum).start()

                    @pl.when(stratum + SOON < workers)
                    def _():
                        send(*block_copy(stratum + SOON))

                slot(work_of(s, stratum, ends))

        for s in range(-LEAD * last, 0):
            slot(work_of(s, 0))

        @pl.loop(0, strata - 1)
        def _(stratum):
            stratum_body(stratum, False)

        hop(strata - 2).wait_send()
        stratum_body(strata - 1, True)

        def end_copies(c):
            done = handed.at[c] if c < last else leaving.at[(strata - 1) % 2]
            block = first + c
            return (
                (done, user_out, end_send.at[2 * c], end_recv.at[0], (block + 1) % n_devs),
                (item.at[c], item_out, end_send.at[2 * c + 1], end_recv.at[1], block),
            )

        for c in range(k):
            for copy in end_copies(c):
                send(*copy)
        for c in range(k):
            for copy in end_copies(c):
                wait_sent(*copy)

    @pl.when(working)
    def _():
        wait_sent(*user_copy)
        wait_sent(*item_copy)
        wait_sent(*block_copy(0))

    @pl.loop(1, workers)
    def _(turn):
        wait_sent(*block_copy(turn))

    arrival(user_init, user_out, end_recv.at[0]).wait()
    arrival(item_init, item_out, end_recv.at[1]).wait()


def solution(mesh):
    n_devs = mesh.shape["shard"]
    row_spec = P(("rep", "shard"), None)
    k = ITEM_BLOCKS
    workers = n_devs // k

    def local(ratings, observed, user_init, item_init):
        users, rank = user_init.shape
        items = item_init.shape[0]
        step_scale = (users + items + rank) / math.sqrt(rank)
        step_size = 0.5 / step_scale
        weight_decay = 0.03 * math.sqrt(users * items / rank)
        masked = jnp.where(observed != 0, ratings, jnp.nan)
        dma = pltpu.SemaphoreType.DMA
        return pl.pallas_call(
            functools.partial(kernel, n_devs, EPOCHS * n_devs, step_size, weight_decay),
            out_shape=(jax.ShapeDtypeStruct((users, rank), jnp.float32), jax.ShapeDtypeStruct((items, rank), jnp.float32)),
            in_specs=[
                pl.BlockSpec(memory_space=pl.ANY),
                pl.BlockSpec(memory_space=pltpu.VMEM),
                pl.BlockSpec(memory_space=pltpu.VMEM),
            ],
            out_specs=(pl.BlockSpec(memory_space=pltpu.VMEM), pl.BlockSpec(memory_space=pltpu.VMEM)),
            scratch_shapes=[
                pltpu.VMEM((n_devs, users, k * items), jnp.float32),
                pltpu.VMEM((k, items, users), jnp.float32),
                pltpu.VMEM((n_devs, users, rank), jnp.float32),
                pltpu.VMEM((k - 1, users, rank), jnp.float32),
                pltpu.VMEM((k - 1, users, rank), jnp.bfloat16),
                pltpu.VMEM((2, users, rank), jnp.float32),
                pltpu.VMEM((k, users, rank), jnp.float32),
                pltpu.VMEM((k, users, rank), jnp.bfloat16),
                pltpu.VMEM((k, items, rank), jnp.float32),
                pltpu.VMEM((k, items, rank), jnp.bfloat16),
                pltpu.VMEM((k, users, rank), jnp.float32),
                dma((workers,)),
                dma((n_devs,)),
                dma((2,)),
                dma((k,)),
                dma((k,)),
                dma((2,)),
                dma((n_devs,)),
                dma((2 * k,)),
                dma((2,)),
            ],
            compiler_params=pltpu.CompilerParams(has_side_effects=True, vmem_limit_bytes=60 * 2**20),
            name="strata",
        )(masked, user_init, item_init)

    return jax.shard_map(local, mesh=mesh, in_specs=(row_spec,) * 4, out_specs=(row_spec, row_spec), check_vma=False)
```

```python
import functools
import math

import jax
import jax.numpy as jnp
from jax import lax
from jax.experimental import pallas as pl
from jax.experimental.pallas import tpu as pltpu
from jax.sharding import PartitionSpec as P

STRATUM_STEPS = 4
EPOCHS = 2
ITEM_BLOCKS = 4
SLOTS = 9
AHEAD = 12
SOON = 2
HALF_STEPS = 2 * STRATUM_STEPS
LEAD = SLOTS - HALF_STEPS + 1

ROW_BY_ROW = (((1,), (1,)), ((), ()))
PLAIN = (((1,), (0,)), ((), ()))


def dot(lhs, rhs, dims):
    return lax.dot_general(lhs, rhs, dims, preferred_element_type=jnp.float32)


def worker_device(worker, n_devs):
    if n_devs != 128:
        return worker
    plane = worker // 16
    place = worker + plane * (31 - 2 * worker)
    y = place // 4
    odd = y % 2
    x = place % 4
    x = x + odd * (3 - 2 * x)
    return ((plane * 4 + y) * 4 + x) * 2 + 1


def worker_of(dev, n_devs):
    if n_devs != 128:
        return dev
    chip = dev // 2
    plane = (chip // 16) % 2
    y = (chip // 4) % 4
    x = chip % 4
    place = y * 4 + x + (y % 2) * (3 - 2 * x)
    return place + plane * (31 - 2 * place)


def is_worker(dev, n_devs):
    if n_devs != 128:
        return dev < n_devs // ITEM_BLOCKS
    return jnp.logical_and(dev % 2 == 1, dev < 64)


def is_low(dev, n_devs):
    return dev < n_devs // 2


def mirror(dev, n_devs):
    quarter = n_devs // 4
    return dev + quarter * (3 - 2 * (dev // quarter))


def kernel(n_devs, strata, step_size, weight_decay, ratings, user_init, item_init, user_out, item_out, rated, turned,
           arriving, handed, handed_bf, leaving, user, user_bf, item, item_bf, user_start,
           go, more_own, more_relayed, relay_send, block_send, block_recv, start_send, user_recv, item_recv, hop_send, hop_recv, end_send, end_recv):
    k = ITEM_BLOCKS
    workers = n_devs // k
    items = item_init.shape[0]
    me = lax.axis_index("shard")
    last = k - 1

    def remote(src, dst, send, recv, dev):
        return pltpu.make_async_remote_copy(
            src_ref=src, dst_ref=dst, send_sem=send, recv_sem=recv, device_id={"shard": dev}, device_id_type=pl.DeviceIdType.MESH
        )

    def arrival(like, dst, recv):
        return pltpu.make_async_copy(like, dst, recv)

    def send(src, dst, send_sem, recv_sem, dev):
        @pl.when(dev != me)
        def _():
            remote(src, dst, send_sem, recv_sem, dev).start()

        @pl.when(dev == me)
        def _():
            pltpu.make_async_copy(src, dst, recv_sem).start()

    def wait_sent(src, dst, send_sem, recv_sem, dev):
        @pl.when(dev != me)
        def _():
            remote(src, dst, send_sem, recv_sem, dev).wait_send()

    home = worker_device(me // k, n_devs)
    user_copy = (user_init, user_start.at[me % k], start_send.at[0], user_recv.at[me % k], home)
    item_copy = (item_init, item.at[me % k], start_send.at[1], item_recv.at[me % k], home)
    send(*user_copy)
    send(*item_copy)

    def columns_of(dev, turn):
        worker = (dev // k + turn) % workers
        return worker_device(worker, n_devs), pl.ds(pl.multiple_of(worker * (k * items), 128), k * items)

    def block_copy(turn):
        to, columns = columns_of(me, turn)
        return ratings.at[:, columns], rated.at[me], block_send.at[turn], block_recv.at[me], to

    low = is_low(me, n_devs)
    across = mirror(me, n_devs)

    def up_copy(turn):
        _, columns = columns_of(me, turn)
        return remote(ratings.at[:, columns], rated.at[turn], block_send.at[turn], block_recv.at[turn], across)

    def relay_copy(turn):
        to, _ = columns_of(across, turn)
        return remote(rated.at[turn], rated.at[across], relay_send.at[turn], block_recv.at[across], to)

    def block_out(turn):
        return remote(*block_copy(turn))

    @pl.loop(0, SOON)
    def _(turn):
        send(*block_copy(turn))

    def send_up():
        @pl.loop(SOON, workers)
        def _(turn):
            to, columns = columns_of(me, turn)

            @pl.when(to != me)
            def _():
                up_copy(turn).start()

            @pl.when(to == me)
            def _():
                pltpu.make_async_copy(ratings.at[:, columns], rated.at[me], block_recv.at[me]).start()

    working = is_worker(me, n_devs)

    @pl.when(low)
    def _():
        send_up()

    @pl.when(jnp.logical_not(low))
    def _():
        pl.semaphore_wait(go, 1)

        @pl.loop(SOON, workers)
        def _(turn):
            to, _ = columns_of(across, turn)
            relays = to != across

            @pl.when(turn * k - me % k > AHEAD)
            def _():
                pl.semaphore_wait(more_own, 1)

                @pl.when(relays)
                def _():
                    pl.semaphore_wait(more_relayed, 1)

            block_out(turn).start()

            @pl.when(relays)
            def _():
                arrival(ratings.at[:, pl.ds(0, k * items)], rated.at[turn], block_recv.at[turn]).wait()
                relay_copy(turn).start()

    @pl.when(working)
    def _():
        mine = worker_of(me, n_devs)
        first = mine * k
        after = worker_device((mine + 1) % workers, n_devs)

        def wait_block(block):
            arrival(ratings.at[:, pl.ds(0, k * items)], rated.at[block], block_recv.at[block]).wait()

        def hop(stratum):
            slot = (stratum + 1) % n_devs
            return remote(leaving.at[stratum % 2], arriving.at[slot], hop_send.at[stratum % 2], hop_recv.at[slot], after)

        for c in range(k):
            arrival(user_init, user_start.at[c], user_recv.at[c]).wait()
            arrival(item_init, item.at[c], item_recv.at[c]).wait()
            wait_block(first + c)
        for c in range(k):
            @pl.when(jnp.logical_not(is_low(first + c, n_devs)))
            def _():
                pl.semaphore_signal(go, inc=1, device_id={"shard": first + c}, device_id_type=pl.DeviceIdType.MESH)

        for c in range(k):
            if c == 0:
                arriving[0] = user_start[0]
            else:
                handed[c - 1] = user_start[c]
                handed_bf[c - 1] = user_start[c].astype(jnp.bfloat16)
            item_bf[c] = item[c].astype(jnp.bfloat16)

        def slot(work):
            first_product, residual = {}, {}
            for c, half, stratum in work:
                if half == 0:
                    lhs = arriving[stratum % n_devs].astype(jnp.bfloat16) if c == 0 else handed_bf[c - 1]
                else:
                    lhs = user_bf[c]
                if half % 2 == 0:
                    first_product[c] = dot(lhs, item_bf[c], ROW_BY_ROW)
                else:
                    first_product[c] = dot(item_bf[c], lhs, ROW_BY_ROW)
            for c, half, stratum in work:
                if half % 2 == 0:
                    block = (first + c - stratum + 2 * n_devs) % n_devs
                    known = rated[block, :, c * items : (c + 1) * items]
                    if half == 0:
                        turned[c] = known.T
                else:
                    known = turned[c]
                residual[c] = jnp.where(known != known, 0.0, first_product[c] - known).astype(jnp.bfloat16)
            for c, half, stratum in work:
                if half % 2 == 0:
                    if half > 0:
                        old = user[c]
                    elif c == 0:
                        old = arriving[stratum % n_devs]
                    else:
                        old = handed[c - 1]
                    grad = dot(residual[c], item_bf[c], PLAIN)
                    new = old - step_size * (grad + weight_decay * old)
                    new_bf = new.astype(jnp.bfloat16)
                    user_bf[c] = new_bf
                    if half < HALF_STEPS - 2:
                        user[c] = new
                    elif c < last:
                        handed[c] = new
                        handed_bf[c] = new_bf
                    else:
                        leaving[stratum % 2] = new
                else:
                    old = item[c]
                    grad = dot(residual[c], user_bf[c], PLAIN)
                    new = old - step_size * (grad + weight_decay * old)
                    item[c] = new
                    item_bf[c] = new.astype(jnp.bfloat16)

        def work_of(s, stratum, first_only=False):
            work = []
            for c in range(k):
                place = s + LEAD * c
                if place < 0 or (first_only and place >= SLOTS):
                    continue
                if place % SLOTS < HALF_STEPS:
                    work.append((c, place % SLOTS, stratum + place // SLOTS))
            return work

        leave_slot = (HALF_STEPS - 1 - LEAD * last) % SLOTS

        def stratum_body(stratum, ends):
            @pl.when(stratum > 0)
            def _():
                slot_in = stratum % n_devs
                arrival(leaving.at[0], arriving.at[slot_in], hop_recv.at[slot_in]).wait()

            @pl.when(jnp.logical_and(stratum > 0, stratum <= n_devs - k))
            def _():
                wait_block((first - stratum + n_devs) % n_devs)

            if not ends:
                asked = (first - stratum - AHEAD + 2 * n_devs) % n_devs

                @pl.when(jnp.logical_and(stratum > 0, jnp.logical_and(stratum + AHEAD <= n_devs - k, asked != me)))
                def _():
                    @pl.when(is_low(asked, n_devs))
                    def _():
                        pl.semaphore_signal(more_relayed, inc=1, device_id={"shard": mirror(asked, n_devs)}, device_id_type=pl.DeviceIdType.MESH)

                    @pl.when(jnp.logical_not(is_low(asked, n_devs)))
                    def _():
                        pl.semaphore_signal(more_own, inc=1, device_id={"shard": asked}, device_id_type=pl.DeviceIdType.MESH)

            for s in range(SLOTS):
                if s == leave_slot and not ends:
                    @pl.when(stratum > 0)
                    def _():
                        hop(stratum - 1).wait_send()

                    hop(stratum).start()
                slot(work_of(s, stratum, ends))

        for s in range(-LEAD * last, 0):
            slot(work_of(s, 0))

        @pl.loop(0, strata - 1)
        def _(stratum):
            stratum_body(stratum, False)

        hop(strata - 2).wait_send()
        stratum_body(strata - 1, True)

        def end_copies(c):
            done = handed.at[c] if c < last else leaving.at[(strata - 1) % 2]
            block = first + c
            return (
                (done, user_out, end_send.at[2 * c], end_recv.at[0], (block + 1) % n_devs),
                (item.at[c], item_out, end_send.at[2 * c + 1], end_recv.at[1], block),
            )

        for c in range(k):
            for copy in end_copies(c):
                send(*copy)
        for c in range(k):
            for copy in end_copies(c):
                wait_sent(*copy)

    wait_sent(*user_copy)
    wait_sent(*item_copy)

    @pl.loop(0, SOON)
    def _(turn):
        wait_sent(*block_copy(turn))

    @pl.when(low)
    def _():
        @pl.loop(SOON, workers)
        def _(turn):
            to, _ = columns_of(me, turn)

            @pl.when(to != me)
            def _():
                up_copy(turn).wait_send()

    @pl.when(jnp.logical_not(low))
    def _():
        @pl.loop(SOON, workers)
        def _(turn):
            block_out(turn).wait_send()
            to, _ = columns_of(across, turn)

            @pl.when(to != across)
            def _():
                relay_copy(turn).wait_send()

    arrival(user_init, user_out, end_recv.at[0]).wait()
    arrival(item_init, item_out, end_recv.at[1]).wait()


def solution(mesh):
    n_devs = mesh.shape["shard"]
    row_spec = P(("rep", "shard"), None)
    k = ITEM_BLOCKS
    workers = n_devs // k

    def local(ratings, observed, user_init, item_init):
        users, rank = user_init.shape
        items = item_init.shape[0]
        step_scale = (users + items + rank) / math.sqrt(rank)
        step_size = 0.5 / step_scale
        weight_decay = 0.03 * math.sqrt(users * items / rank)
        masked = jnp.where(observed != 0, ratings, jnp.nan)
        dma = pltpu.SemaphoreType.DMA
        return pl.pallas_call(
            functools.partial(kernel, n_devs, EPOCHS * n_devs, step_size, weight_decay),
            out_shape=(jax.ShapeDtypeStruct((users, rank), jnp.float32), jax.ShapeDtypeStruct((items, rank), jnp.float32)),
            in_specs=[
                pl.BlockSpec(memory_space=pl.ANY),
                pl.BlockSpec(memory_space=pltpu.VMEM),
                pl.BlockSpec(memory_space=pltpu.VMEM),
            ],
            out_specs=(pl.BlockSpec(memory_space=pltpu.VMEM), pl.BlockSpec(memory_space=pltpu.VMEM)),
            scratch_shapes=[
                pltpu.VMEM((n_devs, users, k * items), jnp.float32),
                pltpu.VMEM((k, items, users), jnp.float32),
                pltpu.VMEM((n_devs, users, rank), jnp.float32),
                pltpu.VMEM((k - 1, users, rank), jnp.float32),
                pltpu.VMEM((k - 1, users, rank), jnp.bfloat16),
                pltpu.VMEM((2, users, rank), jnp.float32),
                pltpu.VMEM((k, users, rank), jnp.float32),
                pltpu.VMEM((k, users, rank), jnp.bfloat16),
                pltpu.VMEM((k, items, rank), jnp.float32),
                pltpu.VMEM((k, items, rank), jnp.bfloat16),
                pltpu.VMEM((k, users, rank), jnp.float32),
                pltpu.SemaphoreType.REGULAR,
                pltpu.SemaphoreType.REGULAR,
                pltpu.SemaphoreType.REGULAR,
                dma((workers,)),
                dma((workers,)),
                dma((n_devs,)),
                dma((2,)),
                dma((k,)),
                dma((k,)),
                dma((2,)),
                dma((n_devs,)),
                dma((2 * k,)),
                dma((2,)),
            ],
            compiler_params=pltpu.CompilerParams(has_side_effects=True, vmem_limit_bytes=60 * 2**20),
            name="strata",
        )(masked, user_init, item_init)

    return jax.shard_map(local, mesh=mesh, in_specs=(row_spec,) * 4, out_specs=(row_spec, row_spec), check_vma=False)
```

```python
import functools
import math

import jax
import jax.numpy as jnp
from jax import lax
from jax.experimental import pallas as pl
from jax.experimental.pallas import tpu as pltpu
from jax.sharding import PartitionSpec as P

STRATUM_STEPS = 4
EPOCHS = 2
ITEM_BLOCKS = 4
SLOTS = 9
AHEAD = 12
PHASES = (0.0, 0.5, 0.9)
SHIFTS = (0.0,) * ITEM_BLOCKS
ORDER = (3, 2, 1, 0)
SOON = 2
HALF_STEPS = 2 * STRATUM_STEPS
LEAD = SLOTS - HALF_STEPS + 1

ROW_BY_ROW = (((1,), (1,)), ((), ()))
PLAIN = (((1,), (0,)), ((), ()))


def dot(lhs, rhs, dims):
    return lax.dot_general(lhs, rhs, dims, preferred_element_type=jnp.float32)


def worker_device(worker, n_devs):
    if n_devs != 128:
        return worker
    plane = worker // 16
    place = worker + plane * (31 - 2 * worker)
    y = place // 4
    odd = y % 2
    x = place % 4
    x = x + odd * (3 - 2 * x)
    return ((plane * 4 + y) * 4 + x) * 2 + 1


def worker_of(dev, n_devs):
    if n_devs != 128:
        return dev
    chip = dev // 2
    plane = (chip // 16) % 2
    y = (chip // 4) % 4
    x = chip % 4
    place = y * 4 + x + (y % 2) * (3 - 2 * x)
    return place + plane * (31 - 2 * place)


def is_worker(dev, n_devs):
    if n_devs != 128:
        return dev < n_devs // ITEM_BLOCKS
    return jnp.logical_and(dev % 2 == 1, dev < 64)


def is_low(dev, n_devs):
    return dev < n_devs // 2


def mirror(dev, n_devs):
    quarter = n_devs // 4
    return dev + quarter * (3 - 2 * (dev // quarter))


def kernel(n_devs, strata, step_size, weight_decay, ratings, user_init, item_init, user_out, item_out, rated, turned,
           arriving, handed, handed_bf, leaving, user, user_bf, item, item_bf, user_start,
           go, more_own, more_relayed, relay_send, block_send, block_recv, start_send, user_recv, item_recv, hop_send, hop_recv, end_send, end_recv):
    k = ITEM_BLOCKS
    workers = n_devs // k
    items = item_init.shape[0]
    me = lax.axis_index("shard")
    last = k - 1

    def remote(src, dst, send, recv, dev):
        return pltpu.make_async_remote_copy(
            src_ref=src, dst_ref=dst, send_sem=send, recv_sem=recv, device_id={"shard": dev}, device_id_type=pl.DeviceIdType.MESH
        )

    def arrival(like, dst, recv):
        return pltpu.make_async_copy(like, dst, recv)

    def send(src, dst, send_sem, recv_sem, dev):
        @pl.when(dev != me)
        def _():
            remote(src, dst, send_sem, recv_sem, dev).start()

        @pl.when(dev == me)
        def _():
            pltpu.make_async_copy(src, dst, recv_sem).start()

    def wait_sent(src, dst, send_sem, recv_sem, dev):
        @pl.when(dev != me)
        def _():
            remote(src, dst, send_sem, recv_sem, dev).wait_send()

    home = worker_device(me // k, n_devs)
    user_copy = (user_init, user_start.at[me % k], start_send.at[0], user_recv.at[me % k], home)
    item_copy = (item_init, item.at[me % k], start_send.at[1], item_recv.at[me % k], home)
    send(*user_copy)
    send(*item_copy)

    def columns_of(dev, turn):
        worker = (dev // k + turn) % workers
        return worker_device(worker, n_devs), pl.ds(pl.multiple_of(worker * (k * items), 128), k * items)

    def block_copy(turn):
        to, columns = columns_of(me, turn)
        return ratings.at[:, columns], rated.at[me], block_send.at[turn], block_recv.at[me], to

    low = is_low(me, n_devs)
    across = mirror(me, n_devs)

    def up_copy(turn):
        _, columns = columns_of(me, turn)
        return remote(ratings.at[:, columns], rated.at[turn], block_send.at[turn], block_recv.at[turn], across)

    def relay_copy(turn):
        to, _ = columns_of(across, turn)
        return remote(rated.at[turn], rated.at[across], relay_send.at[turn], block_recv.at[across], to)

    def block_out(turn):
        return remote(*block_copy(turn))

    @pl.loop(0, SOON)
    def _(turn):
        send(*block_copy(turn))

    def send_up():
        @pl.loop(SOON, workers)
        def _(turn):
            to, columns = columns_of(me, turn)

            @pl.when(to != me)
            def _():
                up_copy(turn).start()

            @pl.when(to == me)
            def _():
                pltpu.make_async_copy(ratings.at[:, columns], rated.at[me], block_recv.at[me]).start()

    working = is_worker(me, n_devs)

    @pl.when(low)
    def _():
        send_up()

    @pl.when(jnp.logical_not(low))
    def _():
        pl.semaphore_wait(go, 1)

        @pl.loop(SOON, workers)
        def _(turn):
            to, _ = columns_of(across, turn)
            relays = to != across

            @pl.when(turn * k - me % k > AHEAD)
            def _():
                pl.semaphore_wait(more_own, 1)

                @pl.when(relays)
                def _():
                    pl.semaphore_wait(more_relayed, 1)

            block_out(turn).start()

            @pl.when(relays)
            def _():
                arrival(ratings.at[:, pl.ds(0, k * items)], rated.at[turn], block_recv.at[turn]).wait()
                relay_copy(turn).start()

    @pl.when(working)
    def _():
        mine = worker_of(me, n_devs)
        first = mine * k
        after = worker_device((mine + 1) % workers, n_devs)

        def wait_block(block):
            arrival(ratings.at[:, pl.ds(0, k * items)], rated.at[block], block_recv.at[block]).wait()

        def hop(stratum):
            slot = (stratum + 1) % n_devs
            return remote(leaving.at[stratum % 2], arriving.at[slot], hop_send.at[stratum % 2], hop_recv.at[slot], after)

        for c in range(k):
            arrival(user_init, user_start.at[c], user_recv.at[c]).wait()
            arrival(item_init, item.at[c], item_recv.at[c]).wait()
            wait_block(first + c)
        for c in range(k):
            @pl.when(jnp.logical_not(is_low(first + c, n_devs)))
            def _():
                pl.semaphore_signal(go, inc=1, device_id={"shard": first + c}, device_id_type=pl.DeviceIdType.MESH)

        for c in range(k):
            if c == 0:
                arriving[0] = user_start[0]
            else:
                handed[c - 1] = user_start[c]

        def steps_of(c, half, stratum, send_user):
            kept = {}

            def predict():
                if half == 0:
                    lhs = arriving[stratum % n_devs] if c == 0 else handed[c - 1]
                else:
                    lhs = user[c] if half < HALF_STEPS - 1 else (handed[c] if c < last else leaving[stratum % 2])
                if half % 2 == 0:
                    kept["predicted"] = dot(lhs, item[c], ROW_BY_ROW)
                else:
                    kept["predicted"] = dot(item[c], lhs, ROW_BY_ROW)

            def descend():
                if half % 2 == 0:
                    block = (first + c - stratum + 2 * n_devs) % n_devs
                    known = rated[block, :, c * items : (c + 1) * items]
                    if half == 0:
                        turned[c] = known.T
                else:
                    known = turned[c]
                residual = jnp.where(known != known, 0.0, kept["predicted"] - known)
                kept["grad"] = dot(residual, item[c] if half % 2 == 0 else (user[c] if half < HALF_STEPS - 1 else (handed[c] if c < last else leaving[stratum % 2])), PLAIN)

            def update():
                if half % 2 == 0:
                    if half > 0:
                        old = user[c]
                    elif c == 0:
                        old = arriving[stratum % n_devs]
                    else:
                        old = handed[c - 1]
                else:
                    old = item[c]
                new = old - step_size * (kept["grad"] + weight_decay * old)
                if half % 2 == 1:
                    item[c] = new
                    return
                if half < HALF_STEPS - 2:
                    user[c] = new
                elif c < last:
                    handed[c] = new
                else:
                    leaving[stratum % 2] = new
                    if send_user is not None:
                        send_user(stratum)

            return predict, descend, update

        def run(slots, send_user=None):
            steps = []
            for s, c, half, stratum in slots:
                for phase, step in zip(PHASES, steps_of(c, half, stratum, send_user)):
                    steps.append((s + phase + SHIFTS[c], ORDER[c], step))
            for _, _, step in sorted(steps, key=lambda step: step[:2]):
                step()

        def work_of(s, stratum, first_only=False):
            work = []
            for c in range(k):
                place = s + LEAD * c
                if place < 0 or (first_only and place >= SLOTS):
                    continue
                if place % SLOTS < HALF_STEPS:
                    work.append((s, c, place % SLOTS, stratum + place // SLOTS))
            return work

        sent_next = LEAD * last > HALF_STEPS - 2

        def stratum_body(stratum, ends):
            if sent_next and not ends:
                send_user(stratum)

            @pl.when(stratum > 0)
            def _():
                slot_in = stratum % n_devs
                arrival(leaving.at[0], arriving.at[slot_in], hop_recv.at[slot_in]).wait()

            @pl.when(jnp.logical_and(stratum > 0, stratum <= n_devs - k))
            def _():
                wait_block((first - stratum + n_devs) % n_devs)

            if not ends:
                asked = (first - stratum - AHEAD + 2 * n_devs) % n_devs

                @pl.when(jnp.logical_and(stratum > 0, jnp.logical_and(stratum + AHEAD <= n_devs - k, asked != me)))
                def _():
                    @pl.when(is_low(asked, n_devs))
                    def _():
                        pl.semaphore_signal(more_relayed, inc=1, device_id={"shard": mirror(asked, n_devs)}, device_id_type=pl.DeviceIdType.MESH)

                    @pl.when(jnp.logical_not(is_low(asked, n_devs)))
                    def _():
                        pl.semaphore_signal(more_own, inc=1, device_id={"shard": asked}, device_id_type=pl.DeviceIdType.MESH)

            run([w for s in range(SLOTS) for w in work_of(s, stratum, ends)], None if sent_next or ends else send_user)

        def send_user(stratum):
            hop(stratum).start()

            @pl.when(stratum > 0)
            def _():
                hop(stratum - 1).wait_send()

        run([w for s in range(-LEAD * last, 0) for w in work_of(s, 0)])

        @pl.loop(0, strata - 1)
        def _(stratum):
            stratum_body(stratum, False)

        hop(strata - 2).wait_send()
        stratum_body(strata - 1, True)

        def end_copies(c):
            done = handed.at[c] if c < last else leaving.at[(strata - 1) % 2]
            block = first + c
            return (
                (done, user_out, end_send.at[2 * c], end_recv.at[0], (block + 1) % n_devs),
                (item.at[c], item_out, end_send.at[2 * c + 1], end_recv.at[1], block),
            )

        for c in range(k):
            for copy in end_copies(c):
                send(*copy)
        for c in range(k):
            for copy in end_copies(c):
                wait_sent(*copy)

    wait_sent(*user_copy)
    wait_sent(*item_copy)

    @pl.loop(0, SOON)
    def _(turn):
        wait_sent(*block_copy(turn))

    @pl.when(low)
    def _():
        @pl.loop(SOON, workers)
        def _(turn):
            to, _ = columns_of(me, turn)

            @pl.when(to != me)
            def _():
                up_copy(turn).wait_send()

    @pl.when(jnp.logical_not(low))
    def _():
        @pl.loop(SOON, workers)
        def _(turn):
            block_out(turn).wait_send()
            to, _ = columns_of(across, turn)

            @pl.when(to != across)
            def _():
                relay_copy(turn).wait_send()

    arrival(user_init, user_out, end_recv.at[0]).wait()
    arrival(item_init, item_out, end_recv.at[1]).wait()


def solution(mesh):
    n_devs = mesh.shape["shard"]
    row_spec = P(("rep", "shard"), None)
    k = ITEM_BLOCKS
    workers = n_devs // k

    def local(ratings, observed, user_init, item_init):
        users, rank = user_init.shape
        items = item_init.shape[0]
        step_scale = (users + items + rank) / math.sqrt(rank)
        step_size = 0.5 / step_scale
        weight_decay = 0.03 * math.sqrt(users * items / rank)
        masked = jnp.where(observed != 0, ratings, jnp.nan)
        dma = pltpu.SemaphoreType.DMA
        return pl.pallas_call(
            functools.partial(kernel, n_devs, EPOCHS * n_devs, step_size, weight_decay),
            out_shape=(jax.ShapeDtypeStruct((users, rank), jnp.float32), jax.ShapeDtypeStruct((items, rank), jnp.float32)),
            in_specs=[
                pl.BlockSpec(memory_space=pl.ANY),
                pl.BlockSpec(memory_space=pltpu.VMEM),
                pl.BlockSpec(memory_space=pltpu.VMEM),
            ],
            out_specs=(pl.BlockSpec(memory_space=pltpu.VMEM), pl.BlockSpec(memory_space=pltpu.VMEM)),
            scratch_shapes=[
                pltpu.VMEM((n_devs, users, k * items), jnp.float32),
                pltpu.VMEM((k, items, users), jnp.float32),
                pltpu.VMEM((n_devs, users, rank), jnp.float32),
                pltpu.VMEM((k - 1, users, rank), jnp.float32),
                pltpu.VMEM((k - 1, users, rank), jnp.bfloat16),
                pltpu.VMEM((2, users, rank), jnp.float32),
                pltpu.VMEM((k, users, rank), jnp.float32),
                pltpu.VMEM((k, users, rank), jnp.bfloat16),
                pltpu.VMEM((k, items, rank), jnp.float32),
                pltpu.VMEM((k, items, rank), jnp.bfloat16),
                pltpu.VMEM((k, users, rank), jnp.float32),
                pltpu.SemaphoreType.REGULAR,
                pltpu.SemaphoreType.REGULAR,
                pltpu.SemaphoreType.REGULAR,
                dma((workers,)),
                dma((workers,)),
                dma((n_devs,)),
                dma((2,)),
                dma((k,)),
                dma((k,)),
                dma((2,)),
                dma((n_devs,)),
                dma((2 * k,)),
                dma((2,)),
            ],
            compiler_params=pltpu.CompilerParams(has_side_effects=True, vmem_limit_bytes=60 * 2**20),
            name="strata",
        )(masked, user_init, item_init)

    return jax.shard_map(local, mesh=mesh, in_specs=(row_spec,) * 4, out_specs=(row_spec, row_spec), check_vma=False)
```

```python
import functools
import math

import jax
import jax.numpy as jnp
from jax import lax
from jax.experimental import pallas as pl
from jax.experimental.pallas import tpu as pltpu
from jax.sharding import PartitionSpec as P

STRATUM_STEPS = 4
EPOCHS = 2
ITEM_BLOCKS = 4
SLOTS = 9
AHEAD = 12
PHASES = (0.0, 0.5, 0.9)
SHIFTS = (0.0,) * ITEM_BLOCKS
ORDER = (3, 2, 1, 0)
SOON = 2
HALF_STEPS = 2 * STRATUM_STEPS
LEAD = SLOTS - HALF_STEPS + 1

ROW_BY_ROW = (((1,), (1,)), ((), ()))
PLAIN = (((1,), (0,)), ((), ()))


def dot(lhs, rhs, dims):
    return lax.dot_general(lhs, rhs, dims, preferred_element_type=jnp.float32)


def worker_device(worker, n_devs):
    if n_devs != 128:
        return worker
    plane = worker // 16
    place = worker + plane * (31 - 2 * worker)
    y = place // 4
    odd = y % 2
    x = place % 4
    x = x + odd * (3 - 2 * x)
    return ((plane * 4 + y) * 4 + x) * 2 + 1


def worker_of(dev, n_devs):
    if n_devs != 128:
        return dev
    chip = dev // 2
    plane = (chip // 16) % 2
    y = (chip // 4) % 4
    x = chip % 4
    place = y * 4 + x + (y % 2) * (3 - 2 * x)
    return place + plane * (31 - 2 * place)


def is_worker(dev, n_devs):
    if n_devs != 128:
        return dev < n_devs // ITEM_BLOCKS
    return jnp.logical_and(dev % 2 == 1, dev < 64)


def is_low(dev, n_devs):
    return dev < n_devs // 2


def mirror(dev, n_devs):
    quarter = n_devs // 4
    return dev + quarter * (3 - 2 * (dev // quarter))


def kernel(n_devs, strata, step_size, weight_decay, ratings, user_init, item_init, user_out, item_out, rated, turned,
           arriving, handed, handed_bf, leaving, user, user_bf, item, item_bf, user_start,
           go, more_own, more_relayed, relay_send, block_send, block_recv, start_send, user_recv, item_recv, hop_send, hop_recv, end_send, end_recv):
    k = ITEM_BLOCKS
    workers = n_devs // k
    items = item_init.shape[0]
    me = lax.axis_index("shard")
    last = k - 1

    def remote(src, dst, send, recv, dev):
        return pltpu.make_async_remote_copy(
            src_ref=src, dst_ref=dst, send_sem=send, recv_sem=recv, device_id={"shard": dev}, device_id_type=pl.DeviceIdType.MESH
        )

    def arrival(like, dst, recv):
        return pltpu.make_async_copy(like, dst, recv)

    def send(src, dst, send_sem, recv_sem, dev):
        @pl.when(dev != me)
        def _():
            remote(src, dst, send_sem, recv_sem, dev).start()

        @pl.when(dev == me)
        def _():
            pltpu.make_async_copy(src, dst, recv_sem).start()

    def wait_sent(src, dst, send_sem, recv_sem, dev):
        @pl.when(dev != me)
        def _():
            remote(src, dst, send_sem, recv_sem, dev).wait_send()

    home = worker_device(me // k, n_devs)
    user_copy = (user_init, user_start.at[me % k], start_send.at[0], user_recv.at[me % k], home)
    item_copy = (item_init, item.at[me % k], start_send.at[1], item_recv.at[me % k], home)
    send(*user_copy)
    send(*item_copy)

    def columns_of(dev, turn):
        worker = (dev // k + turn) % workers
        return worker_device(worker, n_devs), pl.ds(pl.multiple_of(worker * (k * items), 128), k * items)

    def block_copy(turn):
        to, columns = columns_of(me, turn)
        return ratings.at[:, columns], rated.at[me], block_send.at[turn], block_recv.at[me], to

    low = is_low(me, n_devs)
    across = mirror(me, n_devs)

    def up_copy(turn):
        _, columns = columns_of(me, turn)
        return remote(ratings.at[:, columns], rated.at[turn], block_send.at[turn], block_recv.at[turn], across)

    def relay_copy(turn):
        to, _ = columns_of(across, turn)
        return remote(rated.at[turn], rated.at[across], relay_send.at[turn], block_recv.at[across], to)

    def block_out(turn):
        return remote(*block_copy(turn))

    @pl.loop(0, SOON)
    def _(turn):
        send(*block_copy(turn))

    def send_up():
        @pl.loop(SOON, workers)
        def _(turn):
            to, columns = columns_of(me, turn)

            @pl.when(to != me)
            def _():
                up_copy(turn).start()

            @pl.when(to == me)
            def _():
                pltpu.make_async_copy(ratings.at[:, columns], rated.at[me], block_recv.at[me]).start()

    working = is_worker(me, n_devs)

    @pl.when(low)
    def _():
        send_up()

    @pl.when(jnp.logical_not(low))
    def _():
        pl.semaphore_wait(go, 1)

        @pl.loop(SOON, workers)
        def _(turn):
            to, _ = columns_of(across, turn)
            relays = to != across

            @pl.when(turn * k - me % k > AHEAD)
            def _():
                pl.semaphore_wait(more_own, 1)

                @pl.when(relays)
                def _():
                    pl.semaphore_wait(more_relayed, 1)

            block_out(turn).start()

            @pl.when(relays)
            def _():
                arrival(ratings.at[:, pl.ds(0, k * items)], rated.at[turn], block_recv.at[turn]).wait()
                relay_copy(turn).start()

    @pl.when(working)
    def _():
        mine = worker_of(me, n_devs)
        first = mine * k
        after = worker_device((mine + 1) % workers, n_devs)

        def wait_block(block):
            arrival(ratings.at[:, pl.ds(0, k * items)], rated.at[block], block_recv.at[block]).wait()

        def hop(stratum):
            slot = (stratum + 1) % n_devs
            return remote(leaving.at[stratum % 2], arriving.at[slot], hop_send.at[stratum % 2], hop_recv.at[slot], after)

        for c in range(k):
            arrival(user_init, user_start.at[c], user_recv.at[c]).wait()
            arrival(item_init, item.at[c], item_recv.at[c]).wait()
            wait_block(first + c)
        for c in range(k):
            @pl.when(jnp.logical_not(is_low(first + c, n_devs)))
            def _():
                pl.semaphore_signal(go, inc=1, device_id={"shard": first + c}, device_id_type=pl.DeviceIdType.MESH)

        for c in range(k):
            if c == 0:
                arriving[0] = user_start[0]
            else:
                handed[c - 1] = user_start[c]
                handed_bf[c - 1] = user_start[c].astype(jnp.bfloat16)
            item_bf[c] = item[c].astype(jnp.bfloat16)

        def steps_of(c, half, stratum, send_user):
            kept = {}

            def predict():
                if half == 0:
                    lhs = arriving[stratum % n_devs].astype(jnp.bfloat16) if c == 0 else handed_bf[c - 1]
                else:
                    lhs = user_bf[c]
                if half % 2 == 0:
                    kept["predicted"] = dot(lhs, item_bf[c], ROW_BY_ROW)
                else:
                    kept["predicted"] = dot(item_bf[c], lhs, ROW_BY_ROW)

            def descend():
                if half % 2 == 0:
                    block = (first + c - stratum + 2 * n_devs) % n_devs
                    known = rated[block, :, c * items : (c + 1) * items]
                    if half == 0:
                        turned[c] = known.T
                else:
                    known = turned[c]
                residual = jnp.where(known != known, 0.0, kept["predicted"] - known).astype(jnp.bfloat16)
                kept["grad"] = dot(residual, item_bf[c] if half % 2 == 0 else user_bf[c], PLAIN)

            def update():
                if half % 2 == 0:
                    if half > 0:
                        old = user[c]
                    elif c == 0:
                        old = arriving[stratum % n_devs]
                    else:
                        old = handed[c - 1]
                else:
                    old = item[c]
                new = old * (1 - step_size * weight_decay) - step_size * kept["grad"]
                new_bf = new.astype(jnp.bfloat16)
                if half % 2 == 1:
                    item[c] = new
                    item_bf[c] = new_bf
                    return
                user_bf[c] = new_bf
                if half < HALF_STEPS - 2:
                    user[c] = new
                elif c < last:
                    handed[c] = new
                    handed_bf[c] = new_bf
                else:
                    leaving[stratum % 2] = new
                    if send_user is not None:
                        send_user(stratum)

            return predict, descend, update

        def run(slots, send_user=None):
            steps = []
            for s, c, half, stratum in slots:
                for phase, step in zip(PHASES, steps_of(c, half, stratum, send_user)):
                    steps.append((s + phase + SHIFTS[c], ORDER[c], step))
            for _, _, step in sorted(steps, key=lambda step: step[:2]):
                step()

        def work_of(s, stratum, first_only=False):
            work = []
            for c in range(k):
                place = s + LEAD * c
                if place < 0 or (first_only and place >= SLOTS):
                    continue
                if place % SLOTS < HALF_STEPS:
                    work.append((s, c, place % SLOTS, stratum + place // SLOTS))
            return work

        sent_next = LEAD * last > HALF_STEPS - 2

        def stratum_body(stratum, ends):
            if sent_next and not ends:
                send_user(stratum)

            @pl.when(stratum > 0)
            def _():
                slot_in = stratum % n_devs
                arrival(leaving.at[0], arriving.at[slot_in], hop_recv.at[slot_in]).wait()

            @pl.when(jnp.logical_and(stratum > 0, stratum <= n_devs - k))
            def _():
                wait_block((first - stratum + n_devs) % n_devs)

            if not ends:
                asked = (first - stratum - AHEAD + 2 * n_devs) % n_devs

                @pl.when(jnp.logical_and(stratum > 0, jnp.logical_and(stratum + AHEAD <= n_devs - k, asked != me)))
                def _():
                    @pl.when(is_low(asked, n_devs))
                    def _():
                        pl.semaphore_signal(more_relayed, inc=1, device_id={"shard": mirror(asked, n_devs)}, device_id_type=pl.DeviceIdType.MESH)

                    @pl.when(jnp.logical_not(is_low(asked, n_devs)))
                    def _():
                        pl.semaphore_signal(more_own, inc=1, device_id={"shard": asked}, device_id_type=pl.DeviceIdType.MESH)

            run([w for s in range(SLOTS) for w in work_of(s, stratum, ends)], None if sent_next or ends else send_user)

        def send_user(stratum):
            hop(stratum).start()

            @pl.when(stratum > 0)
            def _():
                hop(stratum - 1).wait_send()

        run([w for s in range(-LEAD * last, 0) for w in work_of(s, 0)])

        @pl.loop(0, strata - 1)
        def _(stratum):
            stratum_body(stratum, False)

        hop(strata - 2).wait_send()
        stratum_body(strata - 1, True)

        def end_copies(c):
            done = handed.at[c] if c < last else leaving.at[(strata - 1) % 2]
            block = first + c
            return (
                (done, user_out, end_send.at[2 * c], end_recv.at[0], (block + 1) % n_devs),
                (item.at[c], item_out, end_send.at[2 * c + 1], end_recv.at[1], block),
            )

        for c in range(k):
            for copy in end_copies(c):
                send(*copy)
        for c in range(k):
            for copy in end_copies(c):
                wait_sent(*copy)

    wait_sent(*user_copy)
    wait_sent(*item_copy)

    @pl.loop(0, SOON)
    def _(turn):
        wait_sent(*block_copy(turn))

    @pl.when(low)
    def _():
        @pl.loop(SOON, workers)
        def _(turn):
            to, _ = columns_of(me, turn)

            @pl.when(to != me)
            def _():
                up_copy(turn).wait_send()

    @pl.when(jnp.logical_not(low))
    def _():
        @pl.loop(SOON, workers)
        def _(turn):
            block_out(turn).wait_send()
            to, _ = columns_of(across, turn)

            @pl.when(to != across)
            def _():
                relay_copy(turn).wait_send()

    arrival(user_init, user_out, end_recv.at[0]).wait()
    arrival(item_init, item_out, end_recv.at[1]).wait()


def solution(mesh):
    n_devs = mesh.shape["shard"]
    row_spec = P(("rep", "shard"), None)
    k = ITEM_BLOCKS
    workers = n_devs // k

    def local(ratings, observed, user_init, item_init):
        users, rank = user_init.shape
        items = item_init.shape[0]
        step_scale = (users + items + rank) / math.sqrt(rank)
        step_size = 0.5 / step_scale
        weight_decay = 0.03 * math.sqrt(users * items / rank)
        masked = jnp.where(observed != 0, ratings, jnp.nan)
        dma = pltpu.SemaphoreType.DMA
        return pl.pallas_call(
            functools.partial(kernel, n_devs, EPOCHS * n_devs, step_size, weight_decay),
            out_shape=(jax.ShapeDtypeStruct((users, rank), jnp.float32), jax.ShapeDtypeStruct((items, rank), jnp.float32)),
            in_specs=[
                pl.BlockSpec(memory_space=pl.ANY),
                pl.BlockSpec(memory_space=pltpu.VMEM),
                pl.BlockSpec(memory_space=pltpu.VMEM),
            ],
            out_specs=(pl.BlockSpec(memory_space=pltpu.VMEM), pl.BlockSpec(memory_space=pltpu.VMEM)),
            scratch_shapes=[
                pltpu.VMEM((n_devs, users, k * items), jnp.float32),
                pltpu.VMEM((k, items, users), jnp.float32),
                pltpu.VMEM((n_devs, users, rank), jnp.float32),
                pltpu.VMEM((k - 1, users, rank), jnp.float32),
                pltpu.VMEM((k - 1, users, rank), jnp.bfloat16),
                pltpu.VMEM((2, users, rank), jnp.float32),
                pltpu.VMEM((k, users, rank), jnp.float32),
                pltpu.VMEM((k, users, rank), jnp.bfloat16),
                pltpu.VMEM((k, items, rank), jnp.float32),
                pltpu.VMEM((k, items, rank), jnp.bfloat16),
                pltpu.VMEM((k, users, rank), jnp.float32),
                pltpu.SemaphoreType.REGULAR,
                pltpu.SemaphoreType.REGULAR,
                pltpu.SemaphoreType.REGULAR,
                dma((workers,)),
                dma((workers,)),
                dma((n_devs,)),
                dma((2,)),
                dma((k,)),
                dma((k,)),
                dma((2,)),
                dma((n_devs,)),
                dma((2 * k,)),
                dma((2,)),
            ],
            compiler_params=pltpu.CompilerParams(has_side_effects=True, vmem_limit_bytes=60 * 2**20),
            name="strata",
        )(masked, user_init, item_init)

    return jax.shard_map(local, mesh=mesh, in_specs=(row_spec,) * 4, out_specs=(row_spec, row_spec), check_vma=False)
```

```python
import functools
import math

import jax
import jax.numpy as jnp
from jax import lax
from jax.experimental import pallas as pl
from jax.experimental.pallas import tpu as pltpu
from jax.sharding import PartitionSpec as P

STRATUM_STEPS = 4
EPOCHS = 2
ITEM_BLOCKS = 4
SLOTS = 9
AHEAD = 12
SOON = 2
HALF_STEPS = 2 * STRATUM_STEPS
LEAD = SLOTS - HALF_STEPS + 1

ROW_BY_ROW = (((1,), (1,)), ((), ()))
PLAIN = (((1,), (0,)), ((), ()))


def dot(lhs, rhs, dims):
    return lax.dot_general(lhs, rhs, dims, preferred_element_type=jnp.float32)


def worker_device(worker, n_devs):
    if n_devs != 128:
        return worker
    plane = worker // 16
    place = worker + plane * (31 - 2 * worker)
    y = place // 4
    odd = y % 2
    x = place % 4
    x = x + odd * (3 - 2 * x)
    return ((plane * 4 + y) * 4 + x) * 2 + 1


def worker_of(dev, n_devs):
    if n_devs != 128:
        return dev
    chip = dev // 2
    plane = (chip // 16) % 2
    y = (chip // 4) % 4
    x = chip % 4
    place = y * 4 + x + (y % 2) * (3 - 2 * x)
    return place + plane * (31 - 2 * place)


def is_worker(dev, n_devs):
    if n_devs != 128:
        return dev < n_devs // ITEM_BLOCKS
    return jnp.logical_and(dev % 2 == 1, dev < 64)


def is_low(dev, n_devs):
    return dev < n_devs // 2


def mirror(dev, n_devs):
    quarter = n_devs // 4
    return dev + quarter * (3 - 2 * (dev // quarter))


def kernel(n_devs, strata, step_size, weight_decay, ratings, observed, user_init, item_init, user_out, item_out,
           masked, seen, rated, turned,
           arriving, handed, handed_bf, leaving, user, user_bf, item, item_bf, user_start, item_start,
           ratings_here, seen_here, go, more_own, more_relayed, relay_send, first_send, first_recv, block_send, block_recv,
           start_send, user_recv, item_recv, hop_send, hop_recv, end_send, end_recv):
    k = ITEM_BLOCKS
    workers = n_devs // k
    items = item_init.shape[1]
    wide = k * items
    me = lax.axis_index("shard")
    last = k - 1

    def remote(src, dst, send, recv, dev):
        return pltpu.make_async_remote_copy(
            src_ref=src, dst_ref=dst, send_sem=send, recv_sem=recv, device_id={"shard": dev}, device_id_type=pl.DeviceIdType.MESH
        )

    def arrival(like, dst, recv):
        return pltpu.make_async_copy(like, dst, recv)

    def send(src, dst, send_sem, recv_sem, dev):
        @pl.when(dev != me)
        def _():
            remote(src, dst, send_sem, recv_sem, dev).start()

        @pl.when(dev == me)
        def _():
            pltpu.make_async_copy(src, dst, recv_sem).start()

    def wait_sent(src, dst, send_sem, recv_sem, dev):
        @pl.when(dev != me)
        def _():
            remote(src, dst, send_sem, recv_sem, dev).wait_send()

    low = is_low(me, n_devs)
    across = mirror(me, n_devs)
    pair_here = me % k
    home = worker_device(me // k, n_devs)

    def columns_of(dev, turn):
        worker = (dev // k + turn) % workers
        return worker_device(worker, n_devs), pl.ds(pl.multiple_of(worker * wide, 128), wide)

    def fetch(turn):
        _, columns = columns_of(me, turn)
        return (
            pltpu.make_async_copy(ratings.at[:, columns], masked.at[:, columns], ratings_here.at[turn]),
            pltpu.make_async_copy(observed.at[:, columns], seen.at[:, columns], seen_here.at[turn]),
        )

    def mask(turn):
        for copy in fetch(turn):
            copy.wait()
        _, columns = columns_of(me, turn)
        masked[:, columns] = jnp.where(seen[:, columns] != 0, masked[:, columns], jnp.nan)

    for copy in fetch(0):
        copy.start()
    user_copy = (user_init, user_start.at[pair_here], start_send.at[0], user_recv.at[pair_here], home)
    item_copy = (item_init, item_start.at[pair_here], start_send.at[1], item_recv.at[pair_here], home)
    send(*user_copy)
    send(*item_copy)

    @pl.loop(1, workers)
    def _(turn):
        for copy in fetch(turn):
            copy.start()

    def part_copy(ahead):
        pair = (pair_here + ahead) % k
        here = pl.ds(pl.multiple_of((me // k) * wide + pair * items, 128), items)
        there = pl.ds(pl.multiple_of(pair * items, 128), items)
        sent, received = (first_send, first_recv.at[pair]) if ahead == 0 else (block_send.at[0], block_recv.at[me])
        return masked.at[:, here], rated.at[me, :, there], sent, received, home

    mask(0)
    for ahead in range(k):
        send(*part_copy(ahead))

    def block_copy(turn):
        to, columns = columns_of(me, turn)
        return masked.at[:, columns], rated.at[me], block_send.at[turn], block_recv.at[me], to

    def up_copy(turn):
        _, columns = columns_of(me, turn)
        return remote(masked.at[:, columns], rated.at[turn], block_send.at[turn], block_recv.at[turn], across)

    def relay_copy(turn):
        to, _ = columns_of(across, turn)
        return remote(rated.at[turn], rated.at[across], relay_send.at[turn], block_recv.at[across], to)

    def block_out(turn):
        return remote(*block_copy(turn))

    @pl.loop(1, SOON)
    def _(turn):
        mask(turn)
        send(*block_copy(turn))

    def send_up():
        @pl.loop(SOON, workers)
        def _(turn):
            mask(turn)
            to, _ = columns_of(me, turn)

            @pl.when(to != me)
            def _():
                up_copy(turn).start()

            @pl.when(to == me)
            def _():
                source, target, _, received, _ = block_copy(turn)
                pltpu.make_async_copy(source, target, received).start()

    working = is_worker(me, n_devs)

    @pl.when(low)
    def _():
        send_up()

    @pl.when(jnp.logical_not(low))
    def _():
        @pl.loop(SOON, workers)
        def _(turn):
            mask(turn)

        pl.semaphore_wait(go, 1)

        @pl.loop(SOON, workers)
        def _(turn):
            to, _ = columns_of(across, turn)
            relays = to != across

            @pl.when(turn * k - me % k > AHEAD)
            def _():
                pl.semaphore_wait(more_own, 1)

                @pl.when(relays)
                def _():
                    pl.semaphore_wait(more_relayed, 1)

            block_out(turn).start()

            @pl.when(relays)
            def _():
                arrival(rated.at[turn], rated.at[turn], block_recv.at[turn]).wait()
                relay_copy(turn).start()

    @pl.when(working)
    def _():
        mine = worker_of(me, n_devs)
        first = mine * k
        after = worker_device((mine + 1) % workers, n_devs)

        def wait_block(block):
            arrival(rated.at[block], rated.at[block], block_recv.at[block]).wait()

        def hop(stratum):
            slot = (stratum + 1) % n_devs
            return remote(leaving.at[stratum % 2], arriving.at[slot], hop_send.at[stratum % 2], hop_recv.at[slot], after)

        for c in range(k):
            arrival(user_init, user_start.at[c], user_recv.at[c]).wait()
            arrival(item_init, item_start.at[c], item_recv.at[c]).wait()
            part = rated.at[first + c, :, c * items : (c + 1) * items]
            arrival(part, part, first_recv.at[c]).wait()
        for c in range(k):
            @pl.when(jnp.logical_not(is_low(first + c, n_devs)))
            def _():
                pl.semaphore_signal(go, inc=1, device_id={"shard": first + c}, device_id_type=pl.DeviceIdType.MESH)

        for c in range(k):
            if c == 0:
                arriving[0] = user_start[0]
            else:
                handed[c - 1] = user_start[c]
                handed_bf[c - 1] = user_start[c].astype(jnp.bfloat16)
            item[c] = item_start[c].T
            item_bf[c] = item[c].astype(jnp.bfloat16)

        def steps_of(c, half, stratum, send_user):
            kept = {}

            def predict():
                if half == 0:
                    lhs = arriving[stratum % n_devs].astype(jnp.bfloat16) if c == 0 else handed_bf[c - 1]
                else:
                    lhs = user_bf[c]
                if half % 2 == 0:
                    kept["predicted"] = dot(lhs, item_bf[c], ROW_BY_ROW)
                else:
                    kept["predicted"] = dot(item_bf[c], lhs, ROW_BY_ROW)

            def descend():
                if half % 2 == 0:
                    block = (first + c - stratum + 2 * n_devs) % n_devs
                    known = rated[block, :, c * items : (c + 1) * items]
                    if half == 0:
                        turned[c] = known.T
                else:
                    known = turned[c]
                residual = jnp.where(known != known, 0.0, kept["predicted"] - known).astype(jnp.bfloat16)
                kept["grad"] = dot(residual, item_bf[c] if half % 2 == 0 else user_bf[c], PLAIN)

            def update():
                if half % 2 == 0:
                    if half > 0:
                        old = user[c]
                    elif c == 0:
                        old = arriving[stratum % n_devs]
                    else:
                        old = handed[c - 1]
                else:
                    old = item[c]
                new = old * (1 - step_size * weight_decay) - step_size * kept["grad"]
                new_bf = new.astype(jnp.bfloat16)
                if half % 2 == 1:
                    item[c] = new
                    item_bf[c] = new_bf
                    return
                user_bf[c] = new_bf
                if half < HALF_STEPS - 2:
                    user[c] = new
                elif c < last:
                    handed[c] = new
                    handed_bf[c] = new_bf
                else:
                    leaving[stratum % 2] = new
                    if send_user is not None:
                        send_user(stratum)

            return predict, descend, update

        def slot(work, send_user=None):
            steps = [steps_of(c, half, stratum, send_user) for c, half, stratum in reversed(work)]
            for step in zip(*steps):
                for of_pair in step:
                    of_pair()

        def work_of(s, stratum, first_only=False):
            work = []
            for c in range(k):
                place = s + LEAD * c
                if place < 0 or (first_only and place >= SLOTS):
                    continue
                if place % SLOTS < HALF_STEPS:
                    work.append((c, place % SLOTS, stratum + place // SLOTS))
            return work

        def stratum_body(stratum, ends):
            @pl.when(stratum > 0)
            def _():
                slot_in = stratum % n_devs
                arrival(leaving.at[0], arriving.at[slot_in], hop_recv.at[slot_in]).wait()

            @pl.when(jnp.logical_and(stratum > 0, stratum <= n_devs - k))
            def _():
                wait_block((first - stratum + n_devs) % n_devs)

            if not ends:
                asked = (first - stratum - AHEAD + 2 * n_devs) % n_devs

                @pl.when(jnp.logical_and(stratum > 0, jnp.logical_and(stratum + AHEAD <= n_devs - k, asked != me)))
                def _():
                    @pl.when(is_low(asked, n_devs))
                    def _():
                        pl.semaphore_signal(more_relayed, inc=1, device_id={"shard": mirror(asked, n_devs)}, device_id_type=pl.DeviceIdType.MESH)

                    @pl.when(jnp.logical_not(is_low(asked, n_devs)))
                    def _():
                        pl.semaphore_signal(more_own, inc=1, device_id={"shard": asked}, device_id_type=pl.DeviceIdType.MESH)

            for s in range(SLOTS):
                slot(work_of(s, stratum, ends), None if ends else send_user)

        def send_user(stratum):
            hop(stratum).start()

            @pl.when(stratum > 0)
            def _():
                hop(stratum - 1).wait_send()

        for s in range(-LEAD * last, 0):
            slot(work_of(s, 0))

        for c in range(k):
            some = rated.at[first + c, :, pl.ds(0, last * items)]
            arrival(some, some, block_recv.at[first + c]).wait()

        @pl.loop(0, strata - 1)
        def _(stratum):
            stratum_body(stratum, False)

        hop(strata - 2).wait_send()
        stratum_body(strata - 1, True)

        def end_copies(c):
            done = handed.at[c] if c < last else leaving.at[(strata - 1) % 2]
            block = first + c
            return (
                (done, user_out, end_send.at[2 * c], end_recv.at[0], (block + 1) % n_devs),
                (item_start.at[c], item_out, end_send.at[2 * c + 1], end_recv.at[1], block),
            )

        for c in range(k):
            item_start[c] = item[c].T
        for c in range(k):
            for copy in end_copies(c):
                send(*copy)
        for c in range(k):
            for copy in end_copies(c):
                wait_sent(*copy)

    wait_sent(*user_copy)
    wait_sent(*item_copy)

    wait_sent(*part_copy(0))

    @pl.when(home != me)
    def _():
        some = rated.at[me, :, pl.ds(0, last * items)]
        arrival(some, some, block_send.at[0]).wait()

    @pl.loop(1, SOON)
    def _(turn):
        wait_sent(*block_copy(turn))

    @pl.when(low)
    def _():
        @pl.loop(SOON, workers)
        def _(turn):
            to, _ = columns_of(me, turn)

            @pl.when(to != me)
            def _():
                up_copy(turn).wait_send()

    @pl.when(jnp.logical_not(low))
    def _():
        @pl.loop(SOON, workers)
        def _(turn):
            block_out(turn).wait_send()
            to, _ = columns_of(across, turn)

            @pl.when(to != across)
            def _():
                relay_copy(turn).wait_send()

    arrival(user_init, user_out, end_recv.at[0]).wait()
    arrival(item_init, item_out, end_recv.at[1]).wait()


def solution(mesh):
    n_devs = mesh.shape["shard"]
    row_spec = P(("rep", "shard"), None)
    k = ITEM_BLOCKS
    workers = n_devs // k

    def local(ratings, observed, user_init, item_init):
        users, rank = user_init.shape
        items = item_init.shape[0]
        wide = k * items
        step_scale = (users + items + rank) / math.sqrt(rank)
        step_size = 0.5 / step_scale
        weight_decay = 0.03 * math.sqrt(users * items / rank)
        dma = pltpu.SemaphoreType.DMA
        user_new, item_new = pl.pallas_call(
            functools.partial(kernel, n_devs, EPOCHS * n_devs, step_size, weight_decay),
            out_shape=(jax.ShapeDtypeStruct((users, rank), jnp.float32), jax.ShapeDtypeStruct((rank, items), jnp.float32)),
            in_specs=[pl.BlockSpec(memory_space=pl.ANY)] * 4,
            out_specs=(pl.BlockSpec(memory_space=pl.ANY),) * 2,
            scratch_shapes=[
                pltpu.VMEM((users, n_devs * items), jnp.float32),
                pltpu.VMEM((users, n_devs * items), jnp.int32),
                pltpu.VMEM((n_devs, users, wide), jnp.float32),
                pltpu.VMEM((k, items, users), jnp.float32),
                pltpu.VMEM((n_devs, users, rank), jnp.float32),
                pltpu.VMEM((k - 1, users, rank), jnp.float32),
                pltpu.VMEM((k - 1, users, rank), jnp.bfloat16),
                pltpu.VMEM((2, users, rank), jnp.float32),
                pltpu.VMEM((k, users, rank), jnp.float32),
                pltpu.VMEM((k, users, rank), jnp.bfloat16),
                pltpu.VMEM((k, items, rank), jnp.float32),
                pltpu.VMEM((k, items, rank), jnp.bfloat16),
                pltpu.VMEM((k, users, rank), jnp.float32),
                pltpu.VMEM((k, rank, items), jnp.float32),
                dma((workers,)),
                dma((workers,)),
                pltpu.SemaphoreType.REGULAR,
                pltpu.SemaphoreType.REGULAR,
                pltpu.SemaphoreType.REGULAR,
                dma((workers,)),
                dma,
                dma((k,)),
                dma((workers,)),
                dma((n_devs,)),
                dma((2,)),
                dma((k,)),
                dma((k,)),
                dma((2,)),
                dma((n_devs,)),
                dma((2 * k,)),
                dma((2,)),
            ],
            compiler_params=pltpu.CompilerParams(has_side_effects=True, vmem_limit_bytes=60 * 2**20),
            name="strata",
        )(ratings, observed, user_init, item_init.T)
        return user_new, item_new.T

    return jax.shard_map(local, mesh=mesh, in_specs=(row_spec,) * 4, out_specs=(row_spec, row_spec), check_vma=False)
```

```python
import functools
import math

import jax
import jax.numpy as jnp
from jax import lax
from jax.experimental import pallas as pl
from jax.experimental.pallas import tpu as pltpu
from jax.sharding import PartitionSpec as P

STRATUM_STEPS = 4
EPOCHS = 2
ITEM_BLOCKS = 4
SLOTS = 9
AHEAD = 12
SOON = 2
HALF_STEPS = 2 * STRATUM_STEPS
LEAD = SLOTS - HALF_STEPS + 1

ROW_BY_ROW = (((1,), (1,)), ((), ()))
PLAIN = (((1,), (0,)), ((), ()))


def dot(lhs, rhs, dims):
    return lax.dot_general(lhs, rhs, dims, preferred_element_type=jnp.float32)


def worker_device(worker, n_devs):
    if n_devs != 128:
        return worker
    plane = worker // 16
    place = worker + plane * (31 - 2 * worker)
    y = place // 4
    odd = y % 2
    x = place % 4
    x = x + odd * (3 - 2 * x)
    return ((plane * 4 + y) * 4 + x) * 2 + 1


def worker_of(dev, n_devs):
    if n_devs != 128:
        return dev
    chip = dev // 2
    plane = (chip // 16) % 2
    y = (chip // 4) % 4
    x = chip % 4
    place = y * 4 + x + (y % 2) * (3 - 2 * x)
    return place + plane * (31 - 2 * place)


def is_worker(dev, n_devs):
    if n_devs != 128:
        return dev < n_devs // ITEM_BLOCKS
    return jnp.logical_and(dev % 2 == 1, dev < 64)


def is_low(dev, n_devs):
    return dev < n_devs // 2


def mirror(dev, n_devs):
    quarter = n_devs // 4
    return dev + quarter * (3 - 2 * (dev // quarter))


def kernel(n_devs, strata, step_size, weight_decay, ratings, observed, user_init, item_init, user_out, item_out,
           masked, seen, rated, turned,
           arriving, handed, handed_bf, leaving, user, user_bf, item, item_bf, user_start, item_start,
           ratings_here, seen_here, go, more_own, more_relayed, relay_send, first_send, first_recv, block_send, block_recv,
           start_send, user_recv, item_recv, hop_send, hop_recv, end_send, end_recv):
    k = ITEM_BLOCKS
    workers = n_devs // k
    items = item_init.shape[1]
    wide = k * items
    me = lax.axis_index("shard")
    last = k - 1

    def remote(src, dst, send, recv, dev):
        return pltpu.make_async_remote_copy(
            src_ref=src, dst_ref=dst, send_sem=send, recv_sem=recv, device_id={"shard": dev}, device_id_type=pl.DeviceIdType.MESH
        )

    def arrival(like, dst, recv):
        return pltpu.make_async_copy(like, dst, recv)

    def send(src, dst, send_sem, recv_sem, dev):
        @pl.when(dev != me)
        def _():
            remote(src, dst, send_sem, recv_sem, dev).start()

        @pl.when(dev == me)
        def _():
            pltpu.make_async_copy(src, dst, recv_sem).start()

    def wait_sent(src, dst, send_sem, recv_sem, dev):
        @pl.when(dev != me)
        def _():
            remote(src, dst, send_sem, recv_sem, dev).wait_send()

    low = is_low(me, n_devs)
    across = mirror(me, n_devs)
    pair_here = me % k
    home = worker_device(me // k, n_devs)

    def columns_of(dev, turn):
        worker = (dev // k + turn) % workers
        return worker_device(worker, n_devs), pl.ds(pl.multiple_of(worker * wide, 128), wide)

    def fetch(turn):
        _, columns = columns_of(me, turn)
        return (
            pltpu.make_async_copy(ratings.at[:, columns], masked.at[:, columns], ratings_here.at[turn]),
            pltpu.make_async_copy(observed.at[:, columns], seen.at[:, columns], seen_here.at[turn]),
        )

    def mask(turn):
        for copy in fetch(turn):
            copy.wait()
        _, columns = columns_of(me, turn)
        masked[:, columns] = jnp.where(seen[:, columns] != 0, masked[:, columns], jnp.nan)

    for copy in fetch(0):
        copy.start()
    user_copy = (user_init, user_start.at[pair_here], start_send.at[0], user_recv.at[pair_here], home)
    item_copy = (item_init, item_start.at[pair_here], start_send.at[1], item_recv.at[pair_here], home)
    send(*user_copy)
    send(*item_copy)

    @pl.loop(1, workers)
    def _(turn):
        for copy in fetch(turn):
            copy.start()

    def part_copy(ahead):
        pair = (pair_here + ahead) % k
        here = pl.ds(pl.multiple_of((me // k) * wide + pair * items, 128), items)
        there = pl.ds(pl.multiple_of(pair * items, 128), items)
        sent, received = (first_send, first_recv.at[pair]) if ahead == 0 else (block_send.at[0], block_recv.at[me])
        return masked.at[:, here], rated.at[me, :, there], sent, received, home

    mask(0)
    for ahead in range(k):
        send(*part_copy(ahead))

    def block_copy(turn):
        to, columns = columns_of(me, turn)
        return masked.at[:, columns], rated.at[me], block_send.at[turn], block_recv.at[me], to

    def up_copy(turn):
        _, columns = columns_of(me, turn)
        return remote(masked.at[:, columns], rated.at[turn], block_send.at[turn], block_recv.at[turn], across)

    def relay_copy(turn):
        to, _ = columns_of(across, turn)
        return remote(rated.at[turn], rated.at[across], relay_send.at[turn], block_recv.at[across], to)

    def block_out(turn):
        return remote(*block_copy(turn))

    @pl.loop(1, SOON)
    def _(turn):
        mask(turn)

    wait_sent(*user_copy)
    wait_sent(*item_copy)
    wait_sent(*part_copy(0))

    @pl.loop(1, SOON)
    def _(turn):
        send(*block_copy(turn))

    def send_up():
        @pl.loop(SOON, workers)
        def _(turn):
            mask(turn)
            to, _ = columns_of(me, turn)

            @pl.when(to != me)
            def _():
                up_copy(turn).start()

            @pl.when(to == me)
            def _():
                source, target, _, received, _ = block_copy(turn)
                pltpu.make_async_copy(source, target, received).start()

    working = is_worker(me, n_devs)

    @pl.when(low)
    def _():
        send_up()

    @pl.when(jnp.logical_not(low))
    def _():
        @pl.loop(SOON, workers)
        def _(turn):
            mask(turn)

        pl.semaphore_wait(go, 1)

        @pl.loop(SOON, workers)
        def _(turn):
            to, _ = columns_of(across, turn)
            relays = to != across

            @pl.when(turn * k - me % k > AHEAD)
            def _():
                pl.semaphore_wait(more_own, 1)

                @pl.when(relays)
                def _():
                    pl.semaphore_wait(more_relayed, 1)

            block_out(turn).start()

            @pl.when(relays)
            def _():
                arrival(rated.at[turn], rated.at[turn], block_recv.at[turn]).wait()
                relay_copy(turn).start()

    @pl.when(working)
    def _():
        mine = worker_of(me, n_devs)
        first = mine * k
        after = worker_device((mine + 1) % workers, n_devs)

        def wait_block(block):
            arrival(rated.at[block], rated.at[block], block_recv.at[block]).wait()

        def hop(stratum):
            slot = (stratum + 1) % n_devs
            return remote(leaving.at[stratum % 2], arriving.at[slot], hop_send.at[stratum % 2], hop_recv.at[slot], after)

        for c in range(k):
            arrival(user_init, user_start.at[c], user_recv.at[c]).wait()
            arrival(item_init, item_start.at[c], item_recv.at[c]).wait()
            part = rated.at[first + c, :, c * items : (c + 1) * items]
            arrival(part, part, first_recv.at[c]).wait()
        for c in range(k):
            @pl.when(jnp.logical_not(is_low(first + c, n_devs)))
            def _():
                pl.semaphore_signal(go, inc=1, device_id={"shard": first + c}, device_id_type=pl.DeviceIdType.MESH)

        for c in range(k):
            if c == 0:
                arriving[0] = user_start[0]
            else:
                handed[c - 1] = user_start[c]
                handed_bf[c - 1] = user_start[c].astype(jnp.bfloat16)
            item[c] = item_start[c].T
            item_bf[c] = item[c].astype(jnp.bfloat16)

        def steps_of(c, half, stratum, send_user):
            kept = {}

            def predict():
                if half == 0:
                    lhs = arriving[stratum % n_devs].astype(jnp.bfloat16) if c == 0 else handed_bf[c - 1]
                else:
                    lhs = user_bf[c]
                if half % 2 == 0:
                    kept["predicted"] = dot(lhs, item_bf[c], ROW_BY_ROW)
                else:
                    kept["predicted"] = dot(item_bf[c], lhs, ROW_BY_ROW)

            def descend():
                if half % 2 == 0:
                    block = (first + c - stratum + 2 * n_devs) % n_devs
                    known = rated[block, :, c * items : (c + 1) * items]
                    if half == 0:
                        turned[c] = known.T
                else:
                    known = turned[c]
                residual = jnp.where(known != known, 0.0, kept["predicted"] - known).astype(jnp.bfloat16)
                kept["grad"] = dot(residual, item_bf[c] if half % 2 == 0 else user_bf[c], PLAIN)

            def update():
                if half % 2 == 0:
                    if half > 0:
                        old = user[c]
                    elif c == 0:
                        old = arriving[stratum % n_devs]
                    else:
                        old = handed[c - 1]
                else:
                    old = item[c]
                new = old * (1 - step_size * weight_decay) - step_size * kept["grad"]
                new_bf = new.astype(jnp.bfloat16)
                if half % 2 == 1:
                    item[c] = new
                    item_bf[c] = new_bf
                    return
                user_bf[c] = new_bf
                if half < HALF_STEPS - 2:
                    user[c] = new
                elif c < last:
                    handed[c] = new
                    handed_bf[c] = new_bf
                else:
                    leaving[stratum % 2] = new
                    if send_user is not None:
                        send_user(stratum)

            return predict, descend, update

        def slot(work, send_user=None):
            steps = [steps_of(c, half, stratum, send_user) for c, half, stratum in reversed(work)]
            for step in zip(*steps):
                for of_pair in step:
                    of_pair()

        def work_of(s, stratum, first_only=False):
            work = []
            for c in range(k):
                place = s + LEAD * c
                if place < 0 or (first_only and place >= SLOTS):
                    continue
                if place % SLOTS < HALF_STEPS:
                    work.append((c, place % SLOTS, stratum + place // SLOTS))
            return work

        def ask(stratum):
            asked = (first - stratum + 2 * n_devs) % n_devs

            @pl.when(jnp.logical_and(stratum <= n_devs - k, asked != me))
            def _():
                @pl.when(is_low(asked, n_devs))
                def _():
                    pl.semaphore_signal(more_relayed, inc=1, device_id={"shard": mirror(asked, n_devs)}, device_id_type=pl.DeviceIdType.MESH)

                @pl.when(jnp.logical_not(is_low(asked, n_devs)))
                def _():
                    pl.semaphore_signal(more_own, inc=1, device_id={"shard": asked}, device_id_type=pl.DeviceIdType.MESH)

        def stratum_body(stratum, begins=False, moving=False, ends=False):
            if not begins:
                slot_in = stratum % n_devs
                arrival(leaving.at[0], arriving.at[slot_in], hop_recv.at[slot_in]).wait()
            if moving:
                wait_block((first - stratum + n_devs) % n_devs)
                ask(stratum + AHEAD)

            for s in range(SLOTS):
                slot(work_of(s, stratum, ends), None if ends else functools.partial(send_user, begins))

        def send_user(begins, stratum):
            hop(stratum).start()
            if not begins:
                hop(stratum - 1).wait_send()

        for s in range(-LEAD * last, 0):
            slot(work_of(s, 0))

        for c in range(k):
            some = rated.at[first + c, :, pl.ds(0, last * items)]
            arrival(some, some, block_recv.at[first + c]).wait()

        stratum_body(0, begins=True)

        @pl.loop(1, n_devs - k + 1)
        def _(stratum):
            stratum_body(stratum, moving=True)

        @pl.loop(n_devs - k + 1, strata - 1)
        def _(stratum):
            stratum_body(stratum)

        hop(strata - 2).wait_send()
        stratum_body(strata - 1, ends=True)

        def end_copies(c):
            done = handed.at[c] if c < last else leaving.at[(strata - 1) % 2]
            block = first + c
            return (
                (done, user_out, end_send.at[2 * c], end_recv.at[0], (block + 1) % n_devs),
                (item_start.at[c], item_out, end_send.at[2 * c + 1], end_recv.at[1], block),
            )

        for c in range(k):
            item_start[c] = item[c].T
        for c in range(k):
            for copy in end_copies(c):
                send(*copy)
        for c in range(k):
            for copy in end_copies(c):
                wait_sent(*copy)


    @pl.when(home != me)
    def _():
        some = rated.at[me, :, pl.ds(0, last * items)]
        arrival(some, some, block_send.at[0]).wait()

    @pl.loop(1, SOON)
    def _(turn):
        wait_sent(*block_copy(turn))

    @pl.when(low)
    def _():
        @pl.loop(SOON, workers)
        def _(turn):
            to, _ = columns_of(me, turn)

            @pl.when(to != me)
            def _():
                up_copy(turn).wait_send()

    @pl.when(jnp.logical_not(low))
    def _():
        @pl.loop(SOON, workers)
        def _(turn):
            block_out(turn).wait_send()
            to, _ = columns_of(across, turn)

            @pl.when(to != across)
            def _():
                relay_copy(turn).wait_send()

    arrival(user_init, user_out, end_recv.at[0]).wait()
    arrival(item_init, item_out, end_recv.at[1]).wait()


def solution(mesh):
    n_devs = mesh.shape["shard"]
    row_spec = P(("rep", "shard"), None)
    k = ITEM_BLOCKS
    workers = n_devs // k

    def local(ratings, observed, user_init, item_init):
        users, rank = user_init.shape
        items = item_init.shape[0]
        wide = k * items
        step_scale = (users + items + rank) / math.sqrt(rank)
        step_size = 0.5 / step_scale
        weight_decay = 0.03 * math.sqrt(users * items / rank)
        dma = pltpu.SemaphoreType.DMA
        user_new, item_new = pl.pallas_call(
            functools.partial(kernel, n_devs, EPOCHS * n_devs, step_size, weight_decay),
            out_shape=(jax.ShapeDtypeStruct((users, rank), jnp.float32), jax.ShapeDtypeStruct((rank, items), jnp.float32)),
            in_specs=[pl.BlockSpec(memory_space=pl.ANY)] * 4,
            out_specs=(pl.BlockSpec(memory_space=pl.ANY),) * 2,
            scratch_shapes=[
                pltpu.VMEM((users, n_devs * items), jnp.float32),
                pltpu.VMEM((users, n_devs * items), jnp.int32),
                pltpu.VMEM((n_devs, users, wide), jnp.float32),
                pltpu.VMEM((k, items, users), jnp.float32),
                pltpu.VMEM((n_devs, users, rank), jnp.float32),
                pltpu.VMEM((k - 1, users, rank), jnp.float32),
                pltpu.VMEM((k - 1, users, rank), jnp.bfloat16),
                pltpu.VMEM((2, users, rank), jnp.float32),
                pltpu.VMEM((k, users, rank), jnp.float32),
                pltpu.VMEM((k, users, rank), jnp.bfloat16),
                pltpu.VMEM((k, items, rank), jnp.float32),
                pltpu.VMEM((k, items, rank), jnp.bfloat16),
                pltpu.VMEM((k, users, rank), jnp.float32),
                pltpu.VMEM((k, rank, items), jnp.float32),
                dma((workers,)),
                dma((workers,)),
                pltpu.SemaphoreType.REGULAR,
                pltpu.SemaphoreType.REGULAR,
                pltpu.SemaphoreType.REGULAR,
                dma((workers,)),
                dma,
                dma((k,)),
                dma((workers,)),
                dma((n_devs,)),
                dma((2,)),
                dma((k,)),
                dma((k,)),
                dma((2,)),
                dma((n_devs,)),
                dma((2 * k,)),
                dma((2,)),
            ],
            compiler_params=pltpu.CompilerParams(has_side_effects=True, vmem_limit_bytes=60 * 2**20),
            name="strata",
        )(ratings, observed, user_init, item_init.T)
        return user_new, item_new.T

    return jax.shard_map(local, mesh=mesh, in_specs=(row_spec,) * 4, out_specs=(row_spec, row_spec), check_vma=False)
```

```python
import functools
import math

import jax
import jax.numpy as jnp
from jax import lax
from jax.experimental import pallas as pl
from jax.experimental.pallas import tpu as pltpu
from jax.sharding import PartitionSpec as P

STRATUM_STEPS = 4
EPOCHS = 2
ITEM_BLOCKS = 4
SLOTS = 9
AHEAD = 12
SOON = 2
HALF_STEPS = 2 * STRATUM_STEPS
LEAD = SLOTS - HALF_STEPS + 1

ROW_BY_ROW = (((1,), (1,)), ((), ()))
PLAIN = (((1,), (0,)), ((), ()))


LANES = 128


def rounded(first, second, pair):
    return jnp.concatenate([first[pair], second[pair]], axis=1)


def keep_rounded(first, second, pair, values):
    values = values.astype(jnp.bfloat16)
    first[pair] = values[:, :LANES]
    second[pair] = values[:, LANES:]


def dot(lhs, rhs, dims):
    return lax.dot_general(lhs, rhs, dims, preferred_element_type=jnp.float32)


def worker_device(worker, n_devs):
    if n_devs != 128:
        return worker
    plane = worker // 16
    place = worker + plane * (31 - 2 * worker)
    y = place // 4
    odd = y % 2
    x = place % 4
    x = x + odd * (3 - 2 * x)
    return ((plane * 4 + y) * 4 + x) * 2 + 1


def worker_of(dev, n_devs):
    if n_devs != 128:
        return dev
    chip = dev // 2
    plane = (chip // 16) % 2
    y = (chip // 4) % 4
    x = chip % 4
    place = y * 4 + x + (y % 2) * (3 - 2 * x)
    return place + plane * (31 - 2 * place)


def is_worker(dev, n_devs):
    if n_devs != 128:
        return dev < n_devs // ITEM_BLOCKS
    return jnp.logical_and(dev % 2 == 1, dev < 64)


def is_low(dev, n_devs):
    return dev < n_devs // 2


def mirror(dev, n_devs):
    quarter = n_devs // 4
    return dev + quarter * (3 - 2 * (dev // quarter))


def kernel(n_devs, strata, step_size, weight_decay, ratings, observed, user_init, item_init, user_out, item_out,
           masked, seen, rated, turned,
           arriving, handed, handed_bf, handed_bf_2, leaving, user, user_bf, user_bf_2, item, item_bf, item_bf_2, user_start, item_start,
           ratings_here, seen_here, go, more_own, more_relayed, relay_send, first_send, first_recv, block_send, block_recv,
           start_send, user_recv, item_recv, hop_send, hop_recv, end_send, end_recv):
    k = ITEM_BLOCKS
    workers = n_devs // k
    items = item_init.shape[1]
    wide = k * items
    me = lax.axis_index("shard")
    last = k - 1

    def remote(src, dst, send, recv, dev):
        return pltpu.make_async_remote_copy(
            src_ref=src, dst_ref=dst, send_sem=send, recv_sem=recv, device_id={"shard": dev}, device_id_type=pl.DeviceIdType.MESH
        )

    def arrival(like, dst, recv):
        return pltpu.make_async_copy(like, dst, recv)

    def send(src, dst, send_sem, recv_sem, dev):
        @pl.when(dev != me)
        def _():
            remote(src, dst, send_sem, recv_sem, dev).start()

        @pl.when(dev == me)
        def _():
            pltpu.make_async_copy(src, dst, recv_sem).start()

    def wait_sent(src, dst, send_sem, recv_sem, dev):
        @pl.when(dev != me)
        def _():
            remote(src, dst, send_sem, recv_sem, dev).wait_send()

    low = is_low(me, n_devs)
    across = mirror(me, n_devs)
    pair_here = me % k
    home = worker_device(me // k, n_devs)

    def columns_of(dev, turn):
        worker = (dev // k + turn) % workers
        return worker_device(worker, n_devs), pl.ds(pl.multiple_of(worker * wide, 128), wide)

    def fetch(turn):
        _, columns = columns_of(me, turn)
        return (
            pltpu.make_async_copy(ratings.at[:, columns], masked.at[:, columns], ratings_here.at[turn]),
            pltpu.make_async_copy(observed.at[:, columns], seen.at[:, columns], seen_here.at[turn]),
        )

    def mask(turn):
        for copy in fetch(turn):
            copy.wait()
        _, columns = columns_of(me, turn)
        masked[:, columns] = jnp.where(seen[:, columns] != 0, masked[:, columns], jnp.nan)

    for copy in fetch(0):
        copy.start()
    user_copy = (user_init, user_start.at[pair_here], start_send.at[0], user_recv.at[pair_here], home)
    item_copy = (item_init, item_start.at[pair_here], start_send.at[1], item_recv.at[pair_here], home)
    send(*user_copy)
    send(*item_copy)

    @pl.loop(1, workers)
    def _(turn):
        for copy in fetch(turn):
            copy.start()

    def part_copy(ahead):
        pair = (pair_here + ahead) % k
        here = pl.ds(pl.multiple_of((me // k) * wide + pair * items, 128), items)
        there = pl.ds(pl.multiple_of(pair * items, 128), items)
        sent, received = (first_send, first_recv.at[pair]) if ahead == 0 else (block_send.at[0], block_recv.at[me])
        return masked.at[:, here], rated.at[me, :, there], sent, received, home

    mask(0)
    for ahead in range(k):
        send(*part_copy(ahead))

    def block_copy(turn):
        to, columns = columns_of(me, turn)
        return masked.at[:, columns], rated.at[me], block_send.at[turn], block_recv.at[me], to

    def up_copy(turn):
        _, columns = columns_of(me, turn)
        return remote(masked.at[:, columns], rated.at[turn], block_send.at[turn], block_recv.at[turn], across)

    def relay_copy(turn):
        to, _ = columns_of(across, turn)
        return remote(rated.at[turn], rated.at[across], relay_send.at[turn], block_recv.at[across], to)

    def block_out(turn):
        return remote(*block_copy(turn))

    @pl.loop(1, SOON)
    def _(turn):
        mask(turn)
        send(*block_copy(turn))

    def send_up():
        @pl.loop(SOON, workers)
        def _(turn):
            mask(turn)
            to, _ = columns_of(me, turn)

            @pl.when(to != me)
            def _():
                up_copy(turn).start()

            @pl.when(to == me)
            def _():
                source, target, _, received, _ = block_copy(turn)
                pltpu.make_async_copy(source, target, received).start()

    working = is_worker(me, n_devs)

    @pl.when(low)
    def _():
        send_up()

    @pl.when(jnp.logical_not(low))
    def _():
        @pl.loop(SOON, workers)
        def _(turn):
            mask(turn)

        pl.semaphore_wait(go, 1)

        @pl.loop(SOON, workers)
        def _(turn):
            to, _ = columns_of(across, turn)
            relays = to != across

            @pl.when(turn * k - me % k > AHEAD)
            def _():
                pl.semaphore_wait(more_own, 1)

                @pl.when(relays)
                def _():
                    pl.semaphore_wait(more_relayed, 1)

            block_out(turn).start()

            @pl.when(relays)
            def _():
                arrival(rated.at[turn], rated.at[turn], block_recv.at[turn]).wait()
                relay_copy(turn).start()

    @pl.when(working)
    def _():
        mine = worker_of(me, n_devs)
        first = mine * k
        after = worker_device((mine + 1) % workers, n_devs)

        def wait_block(block):
            arrival(rated.at[block], rated.at[block], block_recv.at[block]).wait()

        def hop(stratum):
            slot = (stratum + 1) % n_devs
            return remote(leaving.at[stratum % 2], arriving.at[slot], hop_send.at[stratum % 2], hop_recv.at[slot], after)

        for c in range(k):
            arrival(user_init, user_start.at[c], user_recv.at[c]).wait()
            arrival(item_init, item_start.at[c], item_recv.at[c]).wait()
            part = rated.at[first + c, :, c * items : (c + 1) * items]
            arrival(part, part, first_recv.at[c]).wait()
        for c in range(k):
            @pl.when(jnp.logical_not(is_low(first + c, n_devs)))
            def _():
                pl.semaphore_signal(go, inc=1, device_id={"shard": first + c}, device_id_type=pl.DeviceIdType.MESH)

        for c in range(k):
            if c == 0:
                arriving[0] = user_start[0]
            else:
                handed[c - 1] = user_start[c]
                keep_rounded(handed_bf, handed_bf_2, c - 1, user_start[c])
            item[c] = item_start[c].T
            keep_rounded(item_bf, item_bf_2, c, item_start[c].T)

        def steps_of(c, half, stratum, send_user):
            kept = {}

            def predict():
                if half == 0:
                    lhs = arriving[stratum % n_devs].astype(jnp.bfloat16) if c == 0 else rounded(handed_bf, handed_bf_2, c - 1)
                else:
                    lhs = rounded(user_bf, user_bf_2, c)
                if half % 2 == 0:
                    kept["predicted"] = dot(lhs, rounded(item_bf, item_bf_2, c), ROW_BY_ROW)
                else:
                    kept["predicted"] = dot(rounded(item_bf, item_bf_2, c), lhs, ROW_BY_ROW)

            def descend():
                if half % 2 == 0:
                    block = (first + c - stratum + 2 * n_devs) % n_devs
                    known = rated[block, :, c * items : (c + 1) * items]
                    if half == 0:
                        turned[c] = known.T
                else:
                    known = turned[c]
                residual = jnp.where(known != known, 0.0, kept["predicted"] - known).astype(jnp.bfloat16)
                kept["grad"] = dot(
                    residual,
                    rounded(item_bf, item_bf_2, c) if half % 2 == 0 else rounded(user_bf, user_bf_2, c),
                    PLAIN,
                )

            def update():
                if half % 2 == 0:
                    if half > 0:
                        old = user[c]
                    elif c == 0:
                        old = arriving[stratum % n_devs]
                    else:
                        old = handed[c - 1]
                else:
                    old = item[c]
                new = old * (1 - step_size * weight_decay) - step_size * kept["grad"]
                if half % 2 == 1:
                    item[c] = new
                    keep_rounded(item_bf, item_bf_2, c, new)
                    return
                keep_rounded(user_bf, user_bf_2, c, new)
                if half < HALF_STEPS - 2:
                    user[c] = new
                elif c < last:
                    handed[c] = new
                    keep_rounded(handed_bf, handed_bf_2, c, new)
                else:
                    leaving[stratum % 2] = new
                    if send_user is not None:
                        send_user(stratum)

            return predict, descend, update

        def slot(work, send_user=None):
            steps = [steps_of(c, half, stratum, send_user) for c, half, stratum in reversed(work)]
            for step in zip(*steps):
                for of_pair in step:
                    of_pair()

        def work_of(s, stratum, first_only=False):
            work = []
            for c in range(k):
                place = s + LEAD * c
                if place < 0 or (first_only and place >= SLOTS):
                    continue
                if place % SLOTS < HALF_STEPS:
                    work.append((c, place % SLOTS, stratum + place // SLOTS))
            return work

        def ask(stratum):
            asked = (first - stratum + 2 * n_devs) % n_devs

            @pl.when(jnp.logical_and(stratum <= n_devs - k, asked != me))
            def _():
                @pl.when(is_low(asked, n_devs))
                def _():
                    pl.semaphore_signal(more_relayed, inc=1, device_id={"shard": mirror(asked, n_devs)}, device_id_type=pl.DeviceIdType.MESH)

                @pl.when(jnp.logical_not(is_low(asked, n_devs)))
                def _():
                    pl.semaphore_signal(more_own, inc=1, device_id={"shard": asked}, device_id_type=pl.DeviceIdType.MESH)

        def stratum_body(stratum, begins=False, moving=False, ends=False):
            if not begins:
                slot_in = stratum % n_devs
                arrival(leaving.at[0], arriving.at[slot_in], hop_recv.at[slot_in]).wait()
            if moving:
                wait_block((first - stratum + n_devs) % n_devs)
                ask(stratum + AHEAD)

            for s in range(SLOTS):
                slot(work_of(s, stratum, ends), None if ends else functools.partial(send_user, begins))

        def send_user(begins, stratum):
            hop(stratum).start()
            if not begins:
                hop(stratum - 1).wait_send()

        for s in range(-LEAD * last, 0):
            slot(work_of(s, 0))

        for c in range(k):
            some = rated.at[first + c, :, pl.ds(0, last * items)]
            arrival(some, some, block_recv.at[first + c]).wait()

        stratum_body(0, begins=True)

        @pl.loop(1, n_devs - k + 1)
        def _(stratum):
            stratum_body(stratum, moving=True)

        @pl.loop(n_devs - k + 1, strata - 1)
        def _(stratum):
            stratum_body(stratum)

        hop(strata - 2).wait_send()
        stratum_body(strata - 1, ends=True)

        def end_copies(c):
            done = handed.at[c] if c < last else leaving.at[(strata - 1) % 2]
            block = first + c
            return (
                (done, user_out, end_send.at[2 * c], end_recv.at[0], (block + 1) % n_devs),
                (item_start.at[c], item_out, end_send.at[2 * c + 1], end_recv.at[1], block),
            )

        for c in range(k):
            item_start[c] = item[c].T
        for c in range(k):
            for copy in end_copies(c):
                send(*copy)
        for c in range(k):
            for copy in end_copies(c):
                wait_sent(*copy)


    wait_sent(*user_copy)
    wait_sent(*item_copy)
    wait_sent(*part_copy(0))

    @pl.when(home != me)
    def _():
        some = rated.at[me, :, pl.ds(0, last * items)]
        arrival(some, some, block_send.at[0]).wait()

    @pl.loop(1, SOON)
    def _(turn):
        wait_sent(*block_copy(turn))

    @pl.when(low)
    def _():
        @pl.loop(SOON, workers)
        def _(turn):
            to, _ = columns_of(me, turn)

            @pl.when(to != me)
            def _():
                up_copy(turn).wait_send()

    @pl.when(jnp.logical_not(low))
    def _():
        @pl.loop(SOON, workers)
        def _(turn):
            block_out(turn).wait_send()
            to, _ = columns_of(across, turn)

            @pl.when(to != across)
            def _():
                relay_copy(turn).wait_send()

    arrival(user_init, user_out, end_recv.at[0]).wait()
    arrival(item_init, item_out, end_recv.at[1]).wait()


def solution(mesh):
    n_devs = mesh.shape["shard"]
    row_spec = P(("rep", "shard"), None)
    k = ITEM_BLOCKS
    workers = n_devs // k

    def local(ratings, observed, user_init, item_init):
        users, rank = user_init.shape
        items = item_init.shape[0]
        wide = k * items
        step_scale = (users + items + rank) / math.sqrt(rank)
        step_size = 0.5 / step_scale
        weight_decay = 0.03 * math.sqrt(users * items / rank)
        dma = pltpu.SemaphoreType.DMA
        user_new, item_new = pl.pallas_call(
            functools.partial(kernel, n_devs, EPOCHS * n_devs, step_size, weight_decay),
            out_shape=(jax.ShapeDtypeStruct((users, rank), jnp.float32), jax.ShapeDtypeStruct((rank, items), jnp.float32)),
            in_specs=[pl.BlockSpec(memory_space=pl.ANY)] * 4,
            out_specs=(pl.BlockSpec(memory_space=pl.ANY),) * 2,
            scratch_shapes=[
                pltpu.VMEM((users, n_devs * items), jnp.float32),
                pltpu.VMEM((users, n_devs * items), jnp.int32),
                pltpu.VMEM((n_devs, users, wide), jnp.float32),
                pltpu.VMEM((k, items, users), jnp.float32),
                pltpu.VMEM((n_devs, users, rank), jnp.float32),
                pltpu.VMEM((k - 1, users, rank), jnp.float32),
                pltpu.VMEM((k - 1, users, LANES), jnp.bfloat16),
                pltpu.VMEM((k - 1, users, rank - LANES), jnp.bfloat16),
                pltpu.VMEM((2, users, rank), jnp.float32),
                pltpu.VMEM((k, users, rank), jnp.float32),
                pltpu.VMEM((k, users, LANES), jnp.bfloat16),
                pltpu.VMEM((k, users, rank - LANES), jnp.bfloat16),
                pltpu.VMEM((k, items, rank), jnp.float32),
                pltpu.VMEM((k, items, LANES), jnp.bfloat16),
                pltpu.VMEM((k, items, rank - LANES), jnp.bfloat16),
                pltpu.VMEM((k, users, rank), jnp.float32),
                pltpu.VMEM((k, rank, items), jnp.float32),
                dma((workers,)),
                dma((workers,)),
                pltpu.SemaphoreType.REGULAR,
                pltpu.SemaphoreType.REGULAR,
                pltpu.SemaphoreType.REGULAR,
                dma((workers,)),
                dma,
                dma((k,)),
                dma((workers,)),
                dma((n_devs,)),
                dma((2,)),
                dma((k,)),
                dma((k,)),
                dma((2,)),
                dma((n_devs,)),
                dma((2 * k,)),
                dma((2,)),
            ],
            compiler_params=pltpu.CompilerParams(has_side_effects=True, vmem_limit_bytes=60 * 2**20),
            name="strata",
        )(ratings, observed, user_init, item_init.T)
        return user_new, item_new.T

    return jax.shard_map(local, mesh=mesh, in_specs=(row_spec,) * 4, out_specs=(row_spec, row_spec), check_vma=False)
```

```python
import functools
import math

import jax
import jax.numpy as jnp
from jax import lax
from jax.experimental import pallas as pl
from jax.experimental.pallas import tpu as pltpu
from jax.sharding import PartitionSpec as P

STRATUM_STEPS = 4
EPOCHS = 2
ITEM_BLOCKS = 4
SLOTS = 9
UNASKED = 8
AHEAD = 12
SOON = 2
HALF_STEPS = 2 * STRATUM_STEPS
LEAD = SLOTS - HALF_STEPS + 1

ROW_BY_ROW = (((1,), (1,)), ((), ()))
PLAIN = (((1,), (0,)), ((), ()))


def dot(lhs, rhs, dims):
    return lax.dot_general(lhs, rhs, dims, preferred_element_type=jnp.float32)


def worker_device(worker, n_devs):
    if n_devs != 128:
        return worker
    plane = worker // 16
    place = worker + plane * (31 - 2 * worker)
    y = place // 4
    odd = y % 2
    x = place % 4
    x = x + odd * (3 - 2 * x)
    return ((plane * 4 + y) * 4 + x) * 2 + 1


def worker_of(dev, n_devs):
    if n_devs != 128:
        return dev
    chip = dev // 2
    plane = (chip // 16) % 2
    y = (chip // 4) % 4
    x = chip % 4
    place = y * 4 + x + (y % 2) * (3 - 2 * x)
    return place + plane * (31 - 2 * place)


def is_worker(dev, n_devs):
    if n_devs != 128:
        return dev < n_devs // ITEM_BLOCKS
    return jnp.logical_and(dev % 2 == 1, dev < 64)


def is_low(dev, n_devs):
    return dev < n_devs // 2


def mirror(dev, n_devs):
    quarter = n_devs // 4
    return dev + quarter * (3 - 2 * (dev // quarter))


def kernel(n_devs, strata, step_size, weight_decay, ratings, observed, user_init, item_init, user_out, item_out,
           masked, seen, rated, turned,
           arriving, handed, handed_bf, leaving, user, user_bf, item, item_bf, user_start, item_start,
           ratings_here, seen_here, more_own, more_relayed, relay_send, first_send, first_recv, block_send, block_recv,
           start_send, user_recv, item_recv, hop_send, hop_recv, end_send, end_recv):
    k = ITEM_BLOCKS
    workers = n_devs // k
    items = item_init.shape[1]
    wide = k * items
    me = lax.axis_index("shard")
    last = k - 1

    def remote(src, dst, send, recv, dev):
        return pltpu.make_async_remote_copy(
            src_ref=src, dst_ref=dst, send_sem=send, recv_sem=recv, device_id={"shard": dev}, device_id_type=pl.DeviceIdType.MESH
        )

    def arrival(like, dst, recv):
        return pltpu.make_async_copy(like, dst, recv)

    def send(src, dst, send_sem, recv_sem, dev):
        @pl.when(dev != me)
        def _():
            remote(src, dst, send_sem, recv_sem, dev).start()

        @pl.when(dev == me)
        def _():
            pltpu.make_async_copy(src, dst, recv_sem).start()

    def wait_sent(src, dst, send_sem, recv_sem, dev):
        @pl.when(dev != me)
        def _():
            remote(src, dst, send_sem, recv_sem, dev).wait_send()

    low = is_low(me, n_devs)
    across = mirror(me, n_devs)
    pair_here = me % k
    home = worker_device(me // k, n_devs)

    def columns_of(dev, turn):
        worker = (dev // k + turn) % workers
        return worker_device(worker, n_devs), pl.ds(pl.multiple_of(worker * wide, 128), wide)

    def fetch(turn):
        _, columns = columns_of(me, turn)
        return (
            pltpu.make_async_copy(ratings.at[:, columns], masked.at[:, columns], ratings_here.at[turn]),
            pltpu.make_async_copy(observed.at[:, columns], seen.at[:, columns], seen_here.at[turn]),
        )

    def mask(turn):
        for copy in fetch(turn):
            copy.wait()
        _, columns = columns_of(me, turn)
        masked[:, columns] = jnp.where(seen[:, columns] != 0, masked[:, columns], jnp.nan)

    for copy in fetch(0):
        copy.start()
    user_copy = (user_init, user_start.at[pair_here], start_send.at[0], user_recv.at[pair_here], home)
    item_copy = (item_init, item_start.at[pair_here], start_send.at[1], item_recv.at[pair_here], home)
    send(*user_copy)
    send(*item_copy)

    @pl.loop(1, workers)
    def _(turn):
        for copy in fetch(turn):
            copy.start()

    def part_copy(ahead):
        pair = (pair_here + ahead) % k
        here = pl.ds(pl.multiple_of((me // k) * wide + pair * items, 128), items)
        there = pl.ds(pl.multiple_of(pair * items, 128), items)
        sent, received = (first_send, first_recv.at[pair]) if ahead == 0 else (block_send.at[0], block_recv.at[me])
        return masked.at[:, here], rated.at[me, :, there], sent, received, home

    mask(0)
    for ahead in range(k):
        send(*part_copy(ahead))

    def block_copy(turn):
        to, columns = columns_of(me, turn)
        return masked.at[:, columns], rated.at[me], block_send.at[turn], block_recv.at[me], to

    def up_copy(turn):
        _, columns = columns_of(me, turn)
        return remote(masked.at[:, columns], rated.at[turn], block_send.at[turn], block_recv.at[turn], across)

    def relay_copy(turn):
        to, _ = columns_of(across, turn)
        return remote(rated.at[turn], rated.at[across], relay_send.at[turn], block_recv.at[across], to)

    def block_out(turn):
        return remote(*block_copy(turn))

    @pl.loop(1, SOON)
    def _(turn):
        mask(turn)

    wait_sent(*user_copy)
    wait_sent(*item_copy)
    wait_sent(*part_copy(0))

    @pl.loop(1, SOON)
    def _(turn):
        send(*block_copy(turn))

    def send_up():
        @pl.loop(SOON, workers)
        def _(turn):
            mask(turn)
            to, _ = columns_of(me, turn)

            @pl.when(to != me)
            def _():
                up_copy(turn).start()

            @pl.when(to == me)
            def _():
                source, target, _, received, _ = block_copy(turn)
                pltpu.make_async_copy(source, target, received).start()

    working = is_worker(me, n_devs)

    @pl.when(low)
    def _():
        send_up()

    @pl.when(jnp.logical_not(low))
    def _():
        @pl.loop(SOON, workers)
        def _(turn):
            mask(turn)

        @pl.loop(1, SOON)
        def _(turn):
            wait_sent(*block_copy(turn))

        @pl.loop(SOON, workers)
        def _(turn):
            to, _ = columns_of(across, turn)
            relays = to != across

            @pl.when(turn * k - me % k > UNASKED)
            def _():
                pl.semaphore_wait(more_own, 1)

                @pl.when(relays)
                def _():
                    pl.semaphore_wait(more_relayed, 1)

            block_out(turn).start()

            @pl.when(relays)
            def _():
                arrival(rated.at[turn], rated.at[turn], block_recv.at[turn]).wait()
                relay_copy(turn).start()

    @pl.when(working)
    def _():
        mine = worker_of(me, n_devs)
        first = mine * k
        after = worker_device((mine + 1) % workers, n_devs)

        def wait_block(block):
            arrival(rated.at[block], rated.at[block], block_recv.at[block]).wait()

        def hop(stratum):
            slot = (stratum + 1) % n_devs
            return remote(leaving.at[stratum % 2], arriving.at[slot], hop_send.at[stratum % 2], hop_recv.at[slot], after)

        for c in range(k):
            arrival(user_init, user_start.at[c], user_recv.at[c]).wait()
            arrival(item_init, item_start.at[c], item_recv.at[c]).wait()
            part = rated.at[first + c, :, c * items : (c + 1) * items]
            arrival(part, part, first_recv.at[c]).wait()
        def ask(stratum):
            asked = (first - stratum + 2 * n_devs) % n_devs

            @pl.when(jnp.logical_and(stratum <= n_devs - k, asked != me))
            def _():
                @pl.when(is_low(asked, n_devs))
                def _():
                    pl.semaphore_signal(more_relayed, inc=1, device_id={"shard": mirror(asked, n_devs)}, device_id_type=pl.DeviceIdType.MESH)

                @pl.when(jnp.logical_not(is_low(asked, n_devs)))
                def _():
                    pl.semaphore_signal(more_own, inc=1, device_id={"shard": asked}, device_id_type=pl.DeviceIdType.MESH)

        for stratum in range(UNASKED + 1, AHEAD + 1):
            ask(stratum)
        for c in range(k):
            if c == 0:
                arriving[0] = user_start[0]
            else:
                handed[c - 1] = user_start[c]
                handed_bf[c - 1] = user_start[c].astype(jnp.bfloat16)
            item[c] = item_start[c].T
            item_bf[c] = item[c].astype(jnp.bfloat16)

        def steps_of(c, half, stratum, send_user):
            kept = {}

            def predict():
                if half == 0:
                    lhs = arriving[stratum % n_devs].astype(jnp.bfloat16) if c == 0 else handed_bf[c - 1]
                else:
                    lhs = user_bf[c]
                if half % 2 == 0:
                    kept["predicted"] = dot(lhs, item_bf[c], ROW_BY_ROW)
                else:
                    kept["predicted"] = dot(item_bf[c], lhs, ROW_BY_ROW)

            def descend():
                if half % 2 == 0:
                    block = (first + c - stratum + 2 * n_devs) % n_devs
                    known = rated[block, :, c * items : (c + 1) * items]
                    if half == 0:
                        turned[c] = known.T
                else:
                    known = turned[c]
                residual = jnp.where(known != known, 0.0, kept["predicted"] - known).astype(jnp.bfloat16)
                kept["grad"] = dot(residual, item_bf[c] if half % 2 == 0 else user_bf[c], PLAIN)

            def update():
                if half % 2 == 0:
                    if half > 0:
                        old = user[c]
                    elif c == 0:
                        old = arriving[stratum % n_devs]
                    else:
                        old = handed[c - 1]
                else:
                    old = item[c]
                new = old * (1 - step_size * weight_decay) - step_size * kept["grad"]
                new_bf = new.astype(jnp.bfloat16)
                if half % 2 == 1:
                    item[c] = new
                    item_bf[c] = new_bf
                    return
                user_bf[c] = new_bf
                if half < HALF_STEPS - 2:
                    user[c] = new
                elif c < last:
                    handed[c] = new
                    handed_bf[c] = new_bf
                else:
                    leaving[stratum % 2] = new
                    if send_user is not None:
                        send_user(stratum)

            return predict, descend, update

        def slot(work, send_user=None):
            steps = [steps_of(c, half, stratum, send_user) for c, half, stratum in reversed(work)]
            for step in zip(*steps):
                for of_pair in step:
                    of_pair()

        def work_of(s, stratum, first_only=False):
            work = []
            for c in range(k):
                place = s + LEAD * c
                if place < 0 or (first_only and place >= SLOTS):
                    continue
                if place % SLOTS < HALF_STEPS:
                    work.append((c, place % SLOTS, stratum + place // SLOTS))
            return work

        def stratum_body(stratum, begins=False, moving=False, ends=False):
            if not begins:
                slot_in = stratum % n_devs
                arrival(leaving.at[0], arriving.at[slot_in], hop_recv.at[slot_in]).wait()
            if moving:
                wait_block((first - stratum + n_devs) % n_devs)
                ask(stratum + AHEAD)

            for s in range(SLOTS):
                slot(work_of(s, stratum, ends), None if ends else functools.partial(send_user, begins))

        def send_user(begins, stratum):
            hop(stratum).start()
            if not begins:
                hop(stratum - 1).wait_send()

        for s in range(-LEAD * last, 0):
            slot(work_of(s, 0))

        for c in range(k):
            some = rated.at[first + c, :, pl.ds(0, last * items)]
            arrival(some, some, block_recv.at[first + c]).wait()

        stratum_body(0, begins=True)

        @pl.loop(1, n_devs - k + 1)
        def _(stratum):
            stratum_body(stratum, moving=True)

        @pl.loop(n_devs - k + 1, strata - 1)
        def _(stratum):
            stratum_body(stratum)

        hop(strata - 2).wait_send()
        stratum_body(strata - 1, ends=True)

        def end_copies(c):
            done = handed.at[c] if c < last else leaving.at[(strata - 1) % 2]
            block = first + c
            return (
                (done, user_out, end_send.at[2 * c], end_recv.at[0], (block + 1) % n_devs),
                (item_start.at[c], item_out, end_send.at[2 * c + 1], end_recv.at[1], block),
            )

        for c in range(k):
            item_start[c] = item[c].T
        for c in range(k):
            for copy in end_copies(c):
                send(*copy)
        for c in range(k):
            for copy in end_copies(c):
                wait_sent(*copy)


    @pl.when(home != me)
    def _():
        some = rated.at[me, :, pl.ds(0, last * items)]
        arrival(some, some, block_send.at[0]).wait()

    @pl.when(low)
    def _():
        @pl.loop(1, SOON)
        def _(turn):
            wait_sent(*block_copy(turn))

        @pl.loop(SOON, workers)
        def _(turn):
            to, _ = columns_of(me, turn)

            @pl.when(to != me)
            def _():
                up_copy(turn).wait_send()

    @pl.when(jnp.logical_not(low))
    def _():
        @pl.loop(SOON, workers)
        def _(turn):
            block_out(turn).wait_send()
            to, _ = columns_of(across, turn)

            @pl.when(to != across)
            def _():
                relay_copy(turn).wait_send()

    arrival(user_init, user_out, end_recv.at[0]).wait()
    arrival(item_init, item_out, end_recv.at[1]).wait()


def solution(mesh):
    n_devs = mesh.shape["shard"]
    row_spec = P(("rep", "shard"), None)
    k = ITEM_BLOCKS
    workers = n_devs // k

    def local(ratings, observed, user_init, item_init):
        users, rank = user_init.shape
        items = item_init.shape[0]
        wide = k * items
        step_scale = (users + items + rank) / math.sqrt(rank)
        step_size = 0.5 / step_scale
        weight_decay = 0.03 * math.sqrt(users * items / rank)
        dma = pltpu.SemaphoreType.DMA
        user_new, item_new = pl.pallas_call(
            functools.partial(kernel, n_devs, EPOCHS * n_devs, step_size, weight_decay),
            out_shape=(jax.ShapeDtypeStruct((users, rank), jnp.float32), jax.ShapeDtypeStruct((rank, items), jnp.float32)),
            in_specs=[pl.BlockSpec(memory_space=pl.ANY)] * 4,
            out_specs=(pl.BlockSpec(memory_space=pl.ANY),) * 2,
            scratch_shapes=[
                pltpu.VMEM((users, n_devs * items), jnp.float32),
                pltpu.VMEM((users, n_devs * items), jnp.int32),
                pltpu.VMEM((n_devs, users, wide), jnp.float32),
                pltpu.VMEM((k, items, users), jnp.float32),
                pltpu.VMEM((n_devs, users, rank), jnp.float32),
                pltpu.VMEM((k - 1, users, rank), jnp.float32),
                pltpu.VMEM((k - 1, users, rank), jnp.bfloat16),
                pltpu.VMEM((2, users, rank), jnp.float32),
                pltpu.VMEM((k, users, rank), jnp.float32),
                pltpu.VMEM((k, users, rank), jnp.bfloat16),
                pltpu.VMEM((k, items, rank), jnp.float32),
                pltpu.VMEM((k, items, rank), jnp.bfloat16),
                pltpu.VMEM((k, users, rank), jnp.float32),
                pltpu.VMEM((k, rank, items), jnp.float32),
                dma((workers,)),
                dma((workers,)),
                pltpu.SemaphoreType.REGULAR,
                pltpu.SemaphoreType.REGULAR,
                dma((workers,)),
                dma,
                dma((k,)),
                dma((workers,)),
                dma((n_devs,)),
                dma((2,)),
                dma((k,)),
                dma((k,)),
                dma((2,)),
                dma((n_devs,)),
                dma((2 * k,)),
                dma((2,)),
            ],
            compiler_params=pltpu.CompilerParams(has_side_effects=True, vmem_limit_bytes=60 * 2**20),
            name="strata",
        )(ratings, observed, user_init, item_init.T)
        return user_new, item_new.T

    return jax.shard_map(local, mesh=mesh, in_specs=(row_spec,) * 4, out_specs=(row_spec, row_spec), check_vma=False)
```

```python
import functools
import math

import jax
import jax.numpy as jnp
from jax import lax
from jax.experimental import pallas as pl
from jax.experimental.pallas import tpu as pltpu
from jax.sharding import PartitionSpec as P

STRATUM_STEPS = 4
EPOCHS = 2
ITEM_BLOCKS = 4
SLOTS = 9
UNASKED = 8
AHEAD = 12
SOON = 2
HALF_STEPS = 2 * STRATUM_STEPS
LEAD = SLOTS - HALF_STEPS + 1

ROW_BY_ROW = (((1,), (1,)), ((), ()))
PLAIN = (((1,), (0,)), ((), ()))


def dot(lhs, rhs, dims):
    return lax.dot_general(lhs, rhs, dims, preferred_element_type=jnp.float32)


def worker_device(worker, n_devs):
    if n_devs != 128:
        return worker
    plane = worker // 16
    place = worker + plane * (31 - 2 * worker)
    y = place // 4
    odd = y % 2
    x = place % 4
    x = x + odd * (3 - 2 * x)
    return ((plane * 4 + y) * 4 + x) * 2 + 1


def worker_of(dev, n_devs):
    if n_devs != 128:
        return dev
    chip = dev // 2
    plane = (chip // 16) % 2
    y = (chip // 4) % 4
    x = chip % 4
    place = y * 4 + x + (y % 2) * (3 - 2 * x)
    return place + plane * (31 - 2 * place)


def is_worker(dev, n_devs):
    if n_devs != 128:
        return dev < n_devs // ITEM_BLOCKS
    return jnp.logical_and(dev % 2 == 1, dev < 64)


def is_low(dev, n_devs):
    return dev < n_devs // 2


def mirror(dev, n_devs):
    quarter = n_devs // 4
    return dev + quarter * (3 - 2 * (dev // quarter))


def kernel(n_devs, strata, step_size, weight_decay, ratings, observed, user_init, item_init, user_out, item_out,
           masked, seen, rated, turned,
           arriving, handed, handed_bf, leaving, user, user_bf, item, item_bf, user_start, item_start,
           ratings_here, seen_here, more_own, more_relayed, relay_send, first_send, first_recv, block_send, block_recv,
           start_send, user_recv, item_recv, hop_send, hop_recv, end_send, end_recv):
    k = ITEM_BLOCKS
    workers = n_devs // k
    items = item_init.shape[1]
    wide = k * items
    me = lax.axis_index("shard")
    last = k - 1

    def remote(src, dst, send, recv, dev):
        return pltpu.make_async_remote_copy(
            src_ref=src, dst_ref=dst, send_sem=send, recv_sem=recv, device_id={"shard": dev}, device_id_type=pl.DeviceIdType.MESH
        )

    def arrival(like, dst, recv):
        return pltpu.make_async_copy(like, dst, recv)

    def send(src, dst, send_sem, recv_sem, dev):
        @pl.when(dev != me)
        def _():
            remote(src, dst, send_sem, recv_sem, dev).start()

        @pl.when(dev == me)
        def _():
            pltpu.make_async_copy(src, dst, recv_sem).start()

    def wait_sent(src, dst, send_sem, recv_sem, dev):
        @pl.when(dev != me)
        def _():
            remote(src, dst, send_sem, recv_sem, dev).wait_send()

    low = is_low(me, n_devs)
    across = mirror(me, n_devs)
    pair_here = me % k
    home = worker_device(me // k, n_devs)

    def columns_of(dev, turn):
        worker = (dev // k + turn) % workers
        return worker_device(worker, n_devs), pl.ds(pl.multiple_of(worker * wide, 128), wide)

    def fetch(turn):
        _, columns = columns_of(me, turn)
        return (
            pltpu.make_async_copy(ratings.at[:, columns], masked.at[:, columns], ratings_here.at[turn]),
            pltpu.make_async_copy(observed.at[:, columns], seen.at[:, columns], seen_here.at[turn]),
        )

    def mask(turn):
        for copy in fetch(turn):
            copy.wait()
        _, columns = columns_of(me, turn)
        masked[:, columns] = jnp.where(seen[:, columns] != 0, masked[:, columns], jnp.nan)

    for copy in fetch(0):
        copy.start()
    user_copy = (user_init, user_start.at[pair_here], start_send.at[0], user_recv.at[pair_here], home)
    item_copy = (item_init, item_start.at[pair_here], start_send.at[1], item_recv.at[pair_here], home)
    send(*user_copy)
    send(*item_copy)

    @pl.loop(1, workers)
    def _(turn):
        for copy in fetch(turn):
            copy.start()

    def part_copy(ahead):
        pair = (pair_here + ahead) % k
        here = pl.ds(pl.multiple_of((me // k) * wide + pair * items, 128), items)
        there = pl.ds(pl.multiple_of(pair * items, 128), items)
        sent, received = (first_send, first_recv.at[pair]) if ahead == 0 else (block_send.at[0], block_recv.at[me])
        return masked.at[:, here], rated.at[me, :, there], sent, received, home

    mask(0)
    for ahead in range(k):
        send(*part_copy(ahead))

    def block_copy(turn):
        to, columns = columns_of(me, turn)
        return masked.at[:, columns], rated.at[me], block_send.at[turn], block_recv.at[me], to

    def up_copy(turn):
        _, columns = columns_of(me, turn)
        return remote(masked.at[:, columns], rated.at[turn], block_send.at[turn], block_recv.at[turn], across)

    def relay_copy(turn):
        to, _ = columns_of(across, turn)
        return remote(rated.at[turn], rated.at[across], relay_send.at[turn], block_recv.at[across], to)

    def block_out(turn):
        return remote(*block_copy(turn))

    @pl.loop(1, SOON)
    def _(turn):
        mask(turn)

    wait_sent(*user_copy)
    wait_sent(*item_copy)
    wait_sent(*part_copy(0))

    @pl.loop(1, SOON)
    def _(turn):
        send(*block_copy(turn))

    def send_up():
        @pl.loop(SOON, workers)
        def _(turn):
            mask(turn)
            to, _ = columns_of(me, turn)

            @pl.when(to != me)
            def _():
                up_copy(turn).start()

            @pl.when(to == me)
            def _():
                source, target, _, received, _ = block_copy(turn)
                pltpu.make_async_copy(source, target, received).start()

    working = is_worker(me, n_devs)

    @pl.when(low)
    def _():
        send_up()

    @pl.when(jnp.logical_not(low))
    def _():
        @pl.loop(SOON, workers)
        def _(turn):
            mask(turn)

        @pl.loop(1, SOON)
        def _(turn):
            wait_sent(*block_copy(turn))

        @pl.loop(SOON, workers)
        def _(turn):
            to, _ = columns_of(across, turn)
            relays = to != across

            @pl.when(turn * k - me % k > UNASKED)
            def _():
                pl.semaphore_wait(more_own, 1)

                @pl.when(relays)
                def _():
                    pl.semaphore_wait(more_relayed, 1)

            block_out(turn).start()

            @pl.when(relays)
            def _():
                arrival(rated.at[turn], rated.at[turn], block_recv.at[turn]).wait()
                relay_copy(turn).start()

    @pl.when(working)
    def _():
        mine = worker_of(me, n_devs)
        first = mine * k
        after = worker_device((mine + 1) % workers, n_devs)

        def wait_block(block):
            arrival(rated.at[block], rated.at[block], block_recv.at[block]).wait()

        def hop(stratum):
            slot = (stratum + 1) % n_devs
            return remote(leaving.at[stratum % 2], arriving.at[slot], hop_send.at[stratum % 2], hop_recv.at[slot], after)

        for c in range(k):
            arrival(user_init, user_start.at[c], user_recv.at[c]).wait()
            arrival(item_init, item_start.at[c], item_recv.at[c]).wait()
            part = rated.at[first + c, :, c * items : (c + 1) * items]
            arrival(part, part, first_recv.at[c]).wait()
        def ask(stratum):
            asked = (first - stratum + 2 * n_devs) % n_devs

            @pl.when(jnp.logical_and(stratum <= n_devs - k, asked != me))
            def _():
                @pl.when(is_low(asked, n_devs))
                def _():
                    pl.semaphore_signal(more_relayed, inc=1, device_id={"shard": mirror(asked, n_devs)}, device_id_type=pl.DeviceIdType.MESH)

                @pl.when(jnp.logical_not(is_low(asked, n_devs)))
                def _():
                    pl.semaphore_signal(more_own, inc=1, device_id={"shard": asked}, device_id_type=pl.DeviceIdType.MESH)

        for stratum in range(UNASKED + 1, AHEAD + 1):
            ask(stratum)
        for c in range(k):
            if c == 0:
                arriving[0] = user_start[0]
            else:
                handed[c - 1] = user_start[c]
                handed_bf[c - 1] = user_start[c].astype(jnp.bfloat16)
            item[c] = item_start[c].T
            item_bf[c] = item[c].astype(jnp.bfloat16)

        def steps_of(c, half, stratum, send_user):
            kept = {}

            def predict():
                if half == 0:
                    lhs = arriving[stratum % n_devs].astype(jnp.bfloat16) if c == 0 else handed_bf[c - 1]
                else:
                    lhs = user_bf[c]
                if half % 2 == 0:
                    kept["predicted"] = dot(lhs, item_bf[c], ROW_BY_ROW)
                else:
                    kept["predicted"] = dot(item_bf[c], lhs, ROW_BY_ROW)

            def descend():
                if half % 2 == 0:
                    block = (first + c - stratum + 2 * n_devs) % n_devs
                    known = rated[block, :, c * items : (c + 1) * items]
                    if half == 0:
                        turned[c] = known.T
                else:
                    known = turned[c]
                residual = jnp.where(known != known, 0.0, kept["predicted"] - known).astype(jnp.bfloat16)
                kept["grad"] = dot(residual, item_bf[c] if half % 2 == 0 else user_bf[c], PLAIN)

            def update():
                if half % 2 == 0:
                    if half > 0:
                        old = user[c]
                    elif c == 0:
                        old = arriving[stratum % n_devs]
                    else:
                        old = handed[c - 1]
                else:
                    old = item[c]
                new = old * (1 - step_size * weight_decay) - step_size * kept["grad"]
                new_bf = new.astype(jnp.bfloat16)
                if half % 2 == 1:
                    item[c] = new
                    item_bf[c] = new_bf
                    return
                user_bf[c] = new_bf
                if half < HALF_STEPS - 2:
                    user[c] = new
                elif c < last:
                    handed[c] = new
                    handed_bf[c] = new_bf
                else:
                    leaving[stratum % 2] = new
                    if send_user is not None:
                        send_user(stratum)

            return predict, descend, update

        def slot(work, send_user=None):
            steps = [steps_of(c, half, stratum, send_user) for c, half, stratum in reversed(work)]
            for step in zip(*steps):
                for of_pair in step:
                    of_pair()

        def work_of(s, stratum, first_only=False):
            work = []
            for c in range(k):
                place = s + LEAD * c
                if place < 0 or (first_only and place >= SLOTS):
                    continue
                if place % SLOTS < HALF_STEPS:
                    work.append((c, place % SLOTS, stratum + place // SLOTS))
            return work

        def stratum_body(stratum, begins=False, moving=False, ends=False):
            if not begins:
                slot_in = stratum % n_devs
                arrival(leaving.at[0], arriving.at[slot_in], hop_recv.at[slot_in]).wait()
                hop(stratum - 1).wait_send()
            if moving:
                wait_block((first - stratum + n_devs) % n_devs)
                ask(stratum + AHEAD)

            for s in range(SLOTS):
                slot(work_of(s, stratum, ends), None if ends else send_user)

        def send_user(stratum):
            hop(stratum).start()

        for s in range(-LEAD * last, 0):
            slot(work_of(s, 0))

        for c in range(k):
            some = rated.at[first + c, :, pl.ds(0, last * items)]
            arrival(some, some, block_recv.at[first + c]).wait()

        stratum_body(0, begins=True)

        @pl.loop(1, n_devs - k + 1)
        def _(stratum):
            stratum_body(stratum, moving=True)

        @pl.loop(n_devs - k + 1, strata - 1)
        def _(stratum):
            stratum_body(stratum)

        stratum_body(strata - 1, ends=True)

        def end_copies(c):
            done = handed.at[c] if c < last else leaving.at[(strata - 1) % 2]
            block = first + c
            return (
                (done, user_out, end_send.at[2 * c], end_recv.at[0], (block + 1) % n_devs),
                (item_start.at[c], item_out, end_send.at[2 * c + 1], end_recv.at[1], block),
            )

        for c in range(k):
            item_start[c] = item[c].T
        for c in range(k):
            for copy in end_copies(c):
                send(*copy)
        for c in range(k):
            for copy in end_copies(c):
                wait_sent(*copy)


    @pl.when(home != me)
    def _():
        some = rated.at[me, :, pl.ds(0, last * items)]
        arrival(some, some, block_send.at[0]).wait()

    @pl.when(low)
    def _():
        @pl.loop(1, SOON)
        def _(turn):
            wait_sent(*block_copy(turn))

        @pl.loop(SOON, workers)
        def _(turn):
            to, _ = columns_of(me, turn)

            @pl.when(to != me)
            def _():
                up_copy(turn).wait_send()

    @pl.when(jnp.logical_not(low))
    def _():
        @pl.loop(SOON, workers)
        def _(turn):
            block_out(turn).wait_send()
            to, _ = columns_of(across, turn)

            @pl.when(to != across)
            def _():
                relay_copy(turn).wait_send()

    arrival(user_init, user_out, end_recv.at[0]).wait()
    arrival(item_init, item_out, end_recv.at[1]).wait()


def solution(mesh):
    n_devs = mesh.shape["shard"]
    row_spec = P(("rep", "shard"), None)
    k = ITEM_BLOCKS
    workers = n_devs // k

    def local(ratings, observed, user_init, item_init):
        users, rank = user_init.shape
        items = item_init.shape[0]
        wide = k * items
        step_scale = (users + items + rank) / math.sqrt(rank)
        step_size = 0.5 / step_scale
        weight_decay = 0.03 * math.sqrt(users * items / rank)
        dma = pltpu.SemaphoreType.DMA
        user_new, item_new = pl.pallas_call(
            functools.partial(kernel, n_devs, EPOCHS * n_devs, step_size, weight_decay),
            out_shape=(jax.ShapeDtypeStruct((users, rank), jnp.float32), jax.ShapeDtypeStruct((rank, items), jnp.float32)),
            in_specs=[pl.BlockSpec(memory_space=pl.ANY)] * 4,
            out_specs=(pl.BlockSpec(memory_space=pl.ANY),) * 2,
            scratch_shapes=[
                pltpu.VMEM((users, n_devs * items), jnp.float32),
                pltpu.VMEM((users, n_devs * items), jnp.int32),
                pltpu.VMEM((n_devs, users, wide), jnp.float32),
                pltpu.VMEM((k, items, users), jnp.float32),
                pltpu.VMEM((n_devs, users, rank), jnp.float32),
                pltpu.VMEM((k - 1, users, rank), jnp.float32),
                pltpu.VMEM((k - 1, users, rank), jnp.bfloat16),
                pltpu.VMEM((2, users, rank), jnp.float32),
                pltpu.VMEM((k, users, rank), jnp.float32),
                pltpu.VMEM((k, users, rank), jnp.bfloat16),
                pltpu.VMEM((k, items, rank), jnp.float32),
                pltpu.VMEM((k, items, rank), jnp.bfloat16),
                pltpu.VMEM((k, users, rank), jnp.float32),
                pltpu.VMEM((k, rank, items), jnp.float32),
                dma((workers,)),
                dma((workers,)),
                pltpu.SemaphoreType.REGULAR,
                pltpu.SemaphoreType.REGULAR,
                dma((workers,)),
                dma,
                dma((k,)),
                dma((workers,)),
                dma((n_devs,)),
                dma((2,)),
                dma((k,)),
                dma((k,)),
                dma((2,)),
                dma((n_devs,)),
                dma((2 * k,)),
                dma((2,)),
            ],
            compiler_params=pltpu.CompilerParams(has_side_effects=True, vmem_limit_bytes=60 * 2**20),
            name="strata",
        )(ratings, observed, user_init, item_init.T)
        return user_new, item_new.T

    return jax.shard_map(local, mesh=mesh, in_specs=(row_spec,) * 4, out_specs=(row_spec, row_spec), check_vma=False)
```

```python
import functools
import math

import jax
import jax.numpy as jnp
from jax import lax
from jax.experimental import pallas as pl
from jax.experimental.pallas import tpu as pltpu
from jax.sharding import PartitionSpec as P

STRATUM_STEPS = 4
EPOCHS = 2
ITEM_BLOCKS = 4
SLOTS = 9
UNASKED = 8
AHEAD = 12
SOON = 2
HALF_STEPS = 2 * STRATUM_STEPS
LEAD = SLOTS - HALF_STEPS + 1

ROW_BY_ROW = (((1,), (1,)), ((), ()))
PLAIN = (((1,), (0,)), ((), ()))


def dot(lhs, rhs, dims):
    return lax.dot_general(lhs, rhs, dims, preferred_element_type=jnp.float32)


def worker_device(worker, n_devs):
    if n_devs != 128:
        return worker
    plane = worker // 16
    place = worker + plane * (31 - 2 * worker)
    y = place // 4
    odd = y % 2
    x = place % 4
    x = x + odd * (3 - 2 * x)
    return ((plane * 4 + y) * 4 + x) * 2 + 1


def worker_of(dev, n_devs):
    if n_devs != 128:
        return dev
    chip = dev // 2
    plane = (chip // 16) % 2
    y = (chip // 4) % 4
    x = chip % 4
    place = y * 4 + x + (y % 2) * (3 - 2 * x)
    return place + plane * (31 - 2 * place)


def is_worker(dev, n_devs):
    if n_devs != 128:
        return dev < n_devs // ITEM_BLOCKS
    return jnp.logical_and(dev % 2 == 1, dev < 64)


def is_low(dev, n_devs):
    return dev < n_devs // 2


def mirror(dev, n_devs):
    quarter = n_devs // 4
    return dev + quarter * (3 - 2 * (dev // quarter))


def kernel(n_devs, strata, step_size, weight_decay, ratings, observed, user_init, item_init, user_out, item_out,
           masked, seen, rated, turned,
           arriving, handed, handed_bf, leaving, user, user_bf, item, item_bf, user_start, item_start,
           ratings_here, seen_here, more_own, more_relayed, relay_send, first_send, first_recv, block_send, block_recv,
           start_send, user_recv, item_recv, hop_send, hop_recv, end_send, end_recv):
    k = ITEM_BLOCKS
    workers = n_devs // k
    items = item_init.shape[1]
    wide = k * items
    me = lax.axis_index("shard")
    last = k - 1

    def remote(src, dst, send, recv, dev):
        return pltpu.make_async_remote_copy(
            src_ref=src, dst_ref=dst, send_sem=send, recv_sem=recv, device_id={"shard": dev}, device_id_type=pl.DeviceIdType.MESH
        )

    def arrival(like, dst, recv):
        return pltpu.make_async_copy(like, dst, recv)

    def send(src, dst, send_sem, recv_sem, dev):
        @pl.when(dev != me)
        def _():
            remote(src, dst, send_sem, recv_sem, dev).start()

        @pl.when(dev == me)
        def _():
            pltpu.make_async_copy(src, dst, recv_sem).start()

    def wait_sent(src, dst, send_sem, recv_sem, dev):
        @pl.when(dev != me)
        def _():
            remote(src, dst, send_sem, recv_sem, dev).wait_send()

    low = is_low(me, n_devs)
    across = mirror(me, n_devs)
    pair_here = me % k
    home = worker_device(me // k, n_devs)

    def columns_of(dev, turn):
        worker = (dev // k + turn) % workers
        return worker_device(worker, n_devs), pl.ds(pl.multiple_of(worker * wide, 128), wide)

    def fetch(turn):
        _, columns = columns_of(me, turn)
        return (
            pltpu.make_async_copy(ratings.at[:, columns], masked.at[:, columns], ratings_here.at[turn]),
            pltpu.make_async_copy(observed.at[:, columns], seen.at[:, columns], seen_here.at[turn]),
        )

    def mask(turn):
        for copy in fetch(turn):
            copy.wait()
        _, columns = columns_of(me, turn)
        masked[:, columns] = jnp.where(seen[:, columns] != 0, masked[:, columns], jnp.nan)

    for copy in fetch(0):
        copy.start()
    user_copy = (user_init, user_start.at[pair_here], start_send.at[0], user_recv.at[pair_here], home)
    item_copy = (item_init, item_start.at[pair_here], start_send.at[1], item_recv.at[pair_here], home)
    send(*user_copy)
    send(*item_copy)

    @pl.loop(1, workers)
    def _(turn):
        for copy in fetch(turn):
            copy.start()

    def part_copy(ahead):
        pair = (pair_here + ahead) % k
        here = pl.ds(pl.multiple_of((me // k) * wide + pair * items, 128), items)
        there = pl.ds(pl.multiple_of(pair * items, 128), items)
        sent, received = (first_send, first_recv.at[pair]) if ahead == 0 else (block_send.at[0], block_recv.at[me])
        return masked.at[:, here], rated.at[me, :, there], sent, received, home

    mask(0)
    for ahead in range(k):
        send(*part_copy(ahead))

    def block_copy(turn):
        to, columns = columns_of(me, turn)
        return masked.at[:, columns], rated.at[me], block_send.at[turn], block_recv.at[me], to

    def up_copy(turn):
        _, columns = columns_of(me, turn)
        return remote(masked.at[:, columns], rated.at[turn], block_send.at[turn], block_recv.at[turn], across)

    def relay_copy(turn):
        to, _ = columns_of(across, turn)
        return remote(rated.at[turn], rated.at[across], relay_send.at[turn], block_recv.at[across], to)

    def block_out(turn):
        return remote(*block_copy(turn))

    @pl.loop(1, SOON)
    def _(turn):
        mask(turn)

    wait_sent(*user_copy)
    wait_sent(*item_copy)
    wait_sent(*part_copy(0))

    @pl.loop(1, SOON)
    def _(turn):
        send(*block_copy(turn))

    def send_up():
        @pl.loop(SOON, workers)
        def _(turn):
            mask(turn)
            to, _ = columns_of(me, turn)

            @pl.when(to != me)
            def _():
                up_copy(turn).start()

            @pl.when(to == me)
            def _():
                source, target, _, received, _ = block_copy(turn)
                pltpu.make_async_copy(source, target, received).start()

    working = is_worker(me, n_devs)

    @pl.when(low)
    def _():
        send_up()

    @pl.when(jnp.logical_not(low))
    def _():
        @pl.loop(SOON, workers)
        def _(turn):
            mask(turn)

        @pl.loop(1, SOON)
        def _(turn):
            wait_sent(*block_copy(turn))

        @pl.loop(SOON, workers)
        def _(turn):
            to, _ = columns_of(across, turn)
            relays = to != across

            @pl.when(turn * k - me % k > UNASKED)
            def _():
                pl.semaphore_wait(more_own, 1)

                @pl.when(relays)
                def _():
                    pl.semaphore_wait(more_relayed, 1)

            block_out(turn).start()

            @pl.when(relays)
            def _():
                arrival(rated.at[turn], rated.at[turn], block_recv.at[turn]).wait()
                relay_copy(turn).start()

    @pl.when(working)
    def _():
        mine = worker_of(me, n_devs)
        first = mine * k
        after = worker_device((mine + 1) % workers, n_devs)

        def wait_block(block):
            arrival(rated.at[block], rated.at[block], block_recv.at[block]).wait()

        def hop(stratum):
            slot = (stratum + 1) % n_devs
            return remote(leaving.at[stratum % 2], arriving.at[slot], hop_send.at[stratum % 2], hop_recv.at[slot], after)

        for c in range(k):
            arrival(user_init, user_start.at[c], user_recv.at[c]).wait()
            arrival(item_init, item_start.at[c], item_recv.at[c]).wait()
            part = rated.at[first + c, :, c * items : (c + 1) * items]
            arrival(part, part, first_recv.at[c]).wait()
        def ask(stratum):
            asked = (first - stratum + 2 * n_devs) % n_devs

            @pl.when(jnp.logical_and(stratum <= n_devs - k, asked != me))
            def _():
                @pl.when(is_low(asked, n_devs))
                def _():
                    pl.semaphore_signal(more_relayed, inc=1, device_id={"shard": mirror(asked, n_devs)}, device_id_type=pl.DeviceIdType.MESH)

                @pl.when(jnp.logical_not(is_low(asked, n_devs)))
                def _():
                    pl.semaphore_signal(more_own, inc=1, device_id={"shard": asked}, device_id_type=pl.DeviceIdType.MESH)

        for stratum in range(UNASKED + 1, AHEAD + 1):
            ask(stratum)
        for c in range(k):
            if c == 0:
                arriving[0] = user_start[0]
            else:
                handed[c - 1] = user_start[c]
                handed_bf[c - 1] = user_start[c].astype(jnp.bfloat16)
            item[c] = item_start[c].T
            item_bf[c] = item[c].astype(jnp.bfloat16)

        def steps_of(c, half, stratum, send_user):
            kept = {}

            def predict():
                items_now = fresh.pop(("item", c)) if ("item", c) in fresh else item_bf[c]
                if half == 0 and c == 0:
                    users_now = arriving[stratum % n_devs].astype(jnp.bfloat16)
                elif half == 0:
                    users_now = fresh.pop(("handed", c)) if ("handed", c) in fresh else handed_bf[c - 1]
                else:
                    users_now = fresh.pop(("user", c)) if ("user", c) in fresh else user_bf[c]
                if half % 2 == 0:
                    kept["predicted"] = dot(users_now, items_now, ROW_BY_ROW)
                else:
                    kept["predicted"] = dot(items_now, users_now, ROW_BY_ROW)

            def descend():
                if half % 2 == 0:
                    block = (first + c - stratum + 2 * n_devs) % n_devs
                    known = rated[block, :, c * items : (c + 1) * items]
                    if half == 0:
                        turned[c] = known.T
                else:
                    known = turned[c]
                residual = jnp.where(known != known, 0.0, kept["predicted"] - known).astype(jnp.bfloat16)
                kept["grad"] = dot(residual, item_bf[c] if half % 2 == 0 else user_bf[c], PLAIN)

            def update():
                if half % 2 == 0:
                    if half > 0:
                        old = user[c]
                    elif c == 0:
                        old = arriving[stratum % n_devs]
                    else:
                        old = handed[c - 1]
                else:
                    old = item[c]
                new = old * (1 - step_size * weight_decay) - step_size * kept["grad"]
                new_bf = new.astype(jnp.bfloat16)
                if half % 2 == 1:
                    item[c] = new
                    item_bf[c] = new_bf
                    fresh["item", c] = new_bf
                    return
                user_bf[c] = new_bf
                fresh["user", c] = new_bf
                if half < HALF_STEPS - 2:
                    user[c] = new
                elif c < last:
                    handed[c] = new
                    handed_bf[c] = new_bf
                    fresh["handed", c + 1] = new_bf
                else:
                    leaving[stratum % 2] = new
                    if send_user is not None:
                        send_user(stratum)

            return predict, descend, update

        fresh = {}

        def slot(work, send_user=None):
            steps = [steps_of(c, half, stratum, send_user) for c, half, stratum in reversed(work)]
            for step in zip(*steps):
                for of_pair in step:
                    of_pair()

        def work_of(s, stratum, first_only=False):
            work = []
            for c in range(k):
                place = s + LEAD * c
                if place < 0 or (first_only and place >= SLOTS):
                    continue
                if place % SLOTS < HALF_STEPS:
                    work.append((c, place % SLOTS, stratum + place // SLOTS))
            return work

        def stratum_body(stratum, begins=False, moving=False, ends=False):
            if not begins:
                slot_in = stratum % n_devs
                arrival(leaving.at[0], arriving.at[slot_in], hop_recv.at[slot_in]).wait()
                hop(stratum - 1).wait_send()
            if moving:
                wait_block((first - stratum + n_devs) % n_devs)
                ask(stratum + AHEAD)

            fresh.clear()
            for s in range(SLOTS):
                slot(work_of(s, stratum, ends), None if ends else send_user)
            fresh.clear()

        def send_user(stratum):
            hop(stratum).start()

        for s in range(-LEAD * last, 0):
            slot(work_of(s, 0))

        for c in range(k):
            some = rated.at[first + c, :, pl.ds(0, last * items)]
            arrival(some, some, block_recv.at[first + c]).wait()

        stratum_body(0, begins=True)

        @pl.loop(1, n_devs - k + 1)
        def _(stratum):
            stratum_body(stratum, moving=True)

        @pl.loop(n_devs - k + 1, strata - 1)
        def _(stratum):
            stratum_body(stratum)

        stratum_body(strata - 1, ends=True)

        def end_copies(c):
            done = handed.at[c] if c < last else leaving.at[(strata - 1) % 2]
            block = first + c
            return (
                (done, user_out, end_send.at[2 * c], end_recv.at[0], (block + 1) % n_devs),
                (item_start.at[c], item_out, end_send.at[2 * c + 1], end_recv.at[1], block),
            )

        for c in range(k):
            item_start[c] = item[c].T
        for c in range(k):
            for copy in end_copies(c):
                send(*copy)
        for c in range(k):
            for copy in end_copies(c):
                wait_sent(*copy)


    @pl.when(home != me)
    def _():
        some = rated.at[me, :, pl.ds(0, last * items)]
        arrival(some, some, block_send.at[0]).wait()

    @pl.when(low)
    def _():
        @pl.loop(1, SOON)
        def _(turn):
            wait_sent(*block_copy(turn))

        @pl.loop(SOON, workers)
        def _(turn):
            to, _ = columns_of(me, turn)

            @pl.when(to != me)
            def _():
                up_copy(turn).wait_send()

    @pl.when(jnp.logical_not(low))
    def _():
        @pl.loop(SOON, workers)
        def _(turn):
            block_out(turn).wait_send()
            to, _ = columns_of(across, turn)

            @pl.when(to != across)
            def _():
                relay_copy(turn).wait_send()

    arrival(user_init, user_out, end_recv.at[0]).wait()
    arrival(item_init, item_out, end_recv.at[1]).wait()


def solution(mesh):
    n_devs = mesh.shape["shard"]
    row_spec = P(("rep", "shard"), None)
    k = ITEM_BLOCKS
    workers = n_devs // k

    def local(ratings, observed, user_init, item_init):
        users, rank = user_init.shape
        items = item_init.shape[0]
        wide = k * items
        step_scale = (users + items + rank) / math.sqrt(rank)
        step_size = 0.5 / step_scale
        weight_decay = 0.03 * math.sqrt(users * items / rank)
        dma = pltpu.SemaphoreType.DMA
        user_new, item_new = pl.pallas_call(
            functools.partial(kernel, n_devs, EPOCHS * n_devs, step_size, weight_decay),
            out_shape=(jax.ShapeDtypeStruct((users, rank), jnp.float32), jax.ShapeDtypeStruct((rank, items), jnp.float32)),
            in_specs=[pl.BlockSpec(memory_space=pl.ANY)] * 4,
            out_specs=(pl.BlockSpec(memory_space=pl.ANY),) * 2,
            scratch_shapes=[
                pltpu.VMEM((users, n_devs * items), jnp.float32),
                pltpu.VMEM((users, n_devs * items), jnp.int32),
                pltpu.VMEM((n_devs, users, wide), jnp.float32),
                pltpu.VMEM((k, items, users), jnp.float32),
                pltpu.VMEM((n_devs, users, rank), jnp.float32),
                pltpu.VMEM((k - 1, users, rank), jnp.float32),
                pltpu.VMEM((k - 1, users, rank), jnp.bfloat16),
                pltpu.VMEM((2, users, rank), jnp.float32),
                pltpu.VMEM((k, users, rank), jnp.float32),
                pltpu.VMEM((k, users, rank), jnp.bfloat16),
                pltpu.VMEM((k, items, rank), jnp.float32),
                pltpu.VMEM((k, items, rank), jnp.bfloat16),
                pltpu.VMEM((k, users, rank), jnp.float32),
                pltpu.VMEM((k, rank, items), jnp.float32),
                dma((workers,)),
                dma((workers,)),
                pltpu.SemaphoreType.REGULAR,
                pltpu.SemaphoreType.REGULAR,
                dma((workers,)),
                dma,
                dma((k,)),
                dma((workers,)),
                dma((n_devs,)),
                dma((2,)),
                dma((k,)),
                dma((k,)),
                dma((2,)),
                dma((n_devs,)),
                dma((2 * k,)),
                dma((2,)),
            ],
            compiler_params=pltpu.CompilerParams(has_side_effects=True, vmem_limit_bytes=60 * 2**20),
            name="strata",
        )(ratings, observed, user_init, item_init.T)
        return user_new, item_new.T

    return jax.shard_map(local, mesh=mesh, in_specs=(row_spec,) * 4, out_specs=(row_spec, row_spec), check_vma=False)
```

```python
import functools
import math

import jax
import jax.numpy as jnp
from jax import lax
from jax.experimental import pallas as pl
from jax.experimental.pallas import tpu as pltpu
from jax.sharding import PartitionSpec as P

STRATUM_STEPS = 4
EPOCHS = 2
ITEM_BLOCKS = 4
SLOTS = 9
UNASKED = 8
AHEAD = 12
SOON = 2
HALF_STEPS = 2 * STRATUM_STEPS
LEAD = SLOTS - HALF_STEPS + 1

ROW_BY_ROW = (((1,), (1,)), ((), ()))
PLAIN = (((1,), (0,)), ((), ()))


def dot(lhs, rhs, dims):
    return lax.dot_general(lhs, rhs, dims, preferred_element_type=jnp.float32)


def worker_device(worker, n_devs):
    if n_devs != 128:
        return worker
    quarter = worker // 8
    row = worker % 8 // 2
    y = row + quarter % 2 * (3 - 2 * row)
    far = (row + worker) % 2
    half = quarter // 2
    x = 1 - far + half * (1 + 2 * far)
    plane = (quarter + half) % 2
    return ((plane * 4 + y) * 4 + x) * 2 + 1


def worker_of(dev, n_devs):
    if n_devs != 128:
        return dev
    chip = dev // 2
    plane = (chip // 16) % 2
    y = (chip // 4) % 4
    x = chip % 4
    half = x // 2
    quarter = 2 * half + (plane + half) % 2
    row = y + quarter % 2 * (3 - 2 * y)
    far = 1 - x + half * (2 * x - 3)
    return 8 * quarter + 2 * row + (far + row) % 2


def is_worker(dev, n_devs):
    if n_devs != 128:
        return dev < n_devs // ITEM_BLOCKS
    return jnp.logical_and(dev % 2 == 1, dev < 64)


def is_low(dev, n_devs):
    return dev < n_devs // 2


def mirror(dev, n_devs):
    quarter = n_devs // 4
    return dev + quarter * (3 - 2 * (dev // quarter))


def kernel(n_devs, strata, step_size, weight_decay, ratings, observed, user_init, item_init, user_out, item_out,
           masked, seen, rated, turned,
           arriving, handed, handed_bf, leaving, user, user_bf, item, item_bf, user_start, item_start,
           ratings_here, seen_here, more_own, more_relayed, relay_send, first_send, first_recv, block_send, block_recv,
           start_send, user_recv, item_recv, hop_send, hop_recv, end_send, end_recv):
    k = ITEM_BLOCKS
    workers = n_devs // k
    items = item_init.shape[1]
    wide = k * items
    me = lax.axis_index("shard")
    last = k - 1

    def remote(src, dst, send, recv, dev):
        return pltpu.make_async_remote_copy(
            src_ref=src, dst_ref=dst, send_sem=send, recv_sem=recv, device_id={"shard": dev}, device_id_type=pl.DeviceIdType.MESH
        )

    def arrival(like, dst, recv):
        return pltpu.make_async_copy(like, dst, recv)

    def send(src, dst, send_sem, recv_sem, dev):
        @pl.when(dev != me)
        def _():
            remote(src, dst, send_sem, recv_sem, dev).start()

        @pl.when(dev == me)
        def _():
            pltpu.make_async_copy(src, dst, recv_sem).start()

    def wait_sent(src, dst, send_sem, recv_sem, dev):
        @pl.when(dev != me)
        def _():
            remote(src, dst, send_sem, recv_sem, dev).wait_send()

    low = is_low(me, n_devs)
    across = mirror(me, n_devs)
    pair_here = me % k
    home = worker_device(me // k, n_devs)

    def columns_of(dev, turn):
        worker = (dev // k + turn) % workers
        return worker_device(worker, n_devs), pl.ds(pl.multiple_of(worker * wide, 128), wide)

    def fetch(turn):
        _, columns = columns_of(me, turn)
        return (
            pltpu.make_async_copy(ratings.at[:, columns], masked.at[:, columns], ratings_here.at[turn]),
            pltpu.make_async_copy(observed.at[:, columns], seen.at[:, columns], seen_here.at[turn]),
        )

    def mask(turn):
        for copy in fetch(turn):
            copy.wait()
        _, columns = columns_of(me, turn)
        masked[:, columns] = jnp.where(seen[:, columns] != 0, masked[:, columns], jnp.nan)

    for copy in fetch(0):
        copy.start()
    user_copy = (user_init, user_start.at[pair_here], start_send.at[0], user_recv.at[pair_here], home)
    item_copy = (item_init, item_start.at[pair_here], start_send.at[1], item_recv.at[pair_here], home)
    send(*user_copy)
    send(*item_copy)

    @pl.loop(1, workers)
    def _(turn):
        for copy in fetch(turn):
            copy.start()

    def part_copy(ahead):
        pair = (pair_here + ahead) % k
        here = pl.ds(pl.multiple_of((me // k) * wide + pair * items, 128), items)
        there = pl.ds(pl.multiple_of(pair * items, 128), items)
        sent, received = (first_send, first_recv.at[pair]) if ahead == 0 else (block_send.at[0], block_recv.at[me])
        return masked.at[:, here], rated.at[me, :, there], sent, received, home

    mask(0)
    for ahead in range(k):
        send(*part_copy(ahead))

    def block_copy(turn):
        to, columns = columns_of(me, turn)
        return masked.at[:, columns], rated.at[me], block_send.at[turn], block_recv.at[me], to

    def up_copy(turn):
        _, columns = columns_of(me, turn)
        return remote(masked.at[:, columns], rated.at[turn], block_send.at[turn], block_recv.at[turn], across)

    def relay_copy(turn):
        to, _ = columns_of(across, turn)
        return remote(rated.at[turn], rated.at[across], relay_send.at[turn], block_recv.at[across], to)

    def block_out(turn):
        return remote(*block_copy(turn))

    @pl.loop(1, SOON)
    def _(turn):
        mask(turn)

    wait_sent(*user_copy)
    wait_sent(*item_copy)
    wait_sent(*part_copy(0))

    @pl.loop(1, SOON)
    def _(turn):
        send(*block_copy(turn))

    def send_up():
        @pl.loop(SOON, workers)
        def _(turn):
            mask(turn)
            to, _ = columns_of(me, turn)

            @pl.when(to != me)
            def _():
                up_copy(turn).start()

            @pl.when(to == me)
            def _():
                source, target, _, received, _ = block_copy(turn)
                pltpu.make_async_copy(source, target, received).start()

    working = is_worker(me, n_devs)

    @pl.when(low)
    def _():
        send_up()

    @pl.when(jnp.logical_not(low))
    def _():
        @pl.loop(SOON, workers)
        def _(turn):
            mask(turn)

        @pl.loop(1, SOON)
        def _(turn):
            wait_sent(*block_copy(turn))

        @pl.loop(SOON, workers)
        def _(turn):
            to, _ = columns_of(across, turn)
            relays = to != across

            @pl.when(turn * k - me % k > UNASKED)
            def _():
                pl.semaphore_wait(more_own, 1)

                @pl.when(relays)
                def _():
                    pl.semaphore_wait(more_relayed, 1)

            block_out(turn).start()

            @pl.when(relays)
            def _():
                arrival(rated.at[turn], rated.at[turn], block_recv.at[turn]).wait()
                relay_copy(turn).start()

    @pl.when(working)
    def _():
        mine = worker_of(me, n_devs)
        first = mine * k
        after = worker_device((mine + 1) % workers, n_devs)

        def wait_block(block):
            arrival(rated.at[block], rated.at[block], block_recv.at[block]).wait()

        def hop(stratum):
            slot = (stratum + 1) % n_devs
            return remote(leaving.at[stratum % 2], arriving.at[slot], hop_send.at[stratum % 2], hop_recv.at[slot], after)

        for c in range(k):
            arrival(user_init, user_start.at[c], user_recv.at[c]).wait()
            arrival(item_init, item_start.at[c], item_recv.at[c]).wait()
            part = rated.at[first + c, :, c * items : (c + 1) * items]
            arrival(part, part, first_recv.at[c]).wait()
        def ask(stratum):
            asked = (first - stratum + 2 * n_devs) % n_devs

            @pl.when(jnp.logical_and(stratum <= n_devs - k, asked != me))
            def _():
                @pl.when(is_low(asked, n_devs))
                def _():
                    pl.semaphore_signal(more_relayed, inc=1, device_id={"shard": mirror(asked, n_devs)}, device_id_type=pl.DeviceIdType.MESH)

                @pl.when(jnp.logical_not(is_low(asked, n_devs)))
                def _():
                    pl.semaphore_signal(more_own, inc=1, device_id={"shard": asked}, device_id_type=pl.DeviceIdType.MESH)

        for stratum in range(UNASKED + 1, AHEAD + 1):
            ask(stratum)
        for c in range(k):
            if c == 0:
                arriving[0] = user_start[0]
            else:
                handed[c - 1] = user_start[c]
                handed_bf[c - 1] = user_start[c].astype(jnp.bfloat16)
            item[c] = item_start[c].T
            item_bf[c] = item[c].astype(jnp.bfloat16)

        def steps_of(c, half, stratum, send_user):
            kept = {}

            def predict():
                items_now = fresh.pop(("item", c)) if ("item", c) in fresh else item_bf[c]
                if half == 0 and c == 0:
                    users_now = arriving[stratum % n_devs].astype(jnp.bfloat16)
                elif half == 0:
                    users_now = fresh.pop(("handed", c)) if ("handed", c) in fresh else handed_bf[c - 1]
                else:
                    users_now = fresh.pop(("user", c)) if ("user", c) in fresh else user_bf[c]
                if half % 2 == 0:
                    kept["predicted"] = dot(users_now, items_now, ROW_BY_ROW)
                else:
                    kept["predicted"] = dot(items_now, users_now, ROW_BY_ROW)

            def descend():
                if half % 2 == 0:
                    block = (first + c - stratum + 2 * n_devs) % n_devs
                    known = rated[block, :, c * items : (c + 1) * items]
                    if half == 0:
                        turned[c] = known.T
                else:
                    known = turned[c]
                residual = jnp.where(known != known, 0.0, kept["predicted"] - known).astype(jnp.bfloat16)
                kept["grad"] = dot(residual, item_bf[c] if half % 2 == 0 else user_bf[c], PLAIN)

            def update():
                if half % 2 == 0:
                    if half > 0:
                        old = user[c]
                    elif c == 0:
                        old = arriving[stratum % n_devs]
                    else:
                        old = handed[c - 1]
                else:
                    old = item[c]
                new = old * (1 - step_size * weight_decay) - step_size * kept["grad"]
                new_bf = new.astype(jnp.bfloat16)
                if half % 2 == 1:
                    item[c] = new
                    item_bf[c] = new_bf
                    fresh["item", c] = new_bf
                    return
                user_bf[c] = new_bf
                fresh["user", c] = new_bf
                if half < HALF_STEPS - 2:
                    user[c] = new
                elif c < last:
                    handed[c] = new
                    handed_bf[c] = new_bf
                    fresh["handed", c + 1] = new_bf
                else:
                    leaving[stratum % 2] = new
                    if send_user is not None:
                        send_user(stratum)

            return predict, descend, update

        fresh = {}

        def slot(work, send_user=None):
            steps = [steps_of(c, half, stratum, send_user) for c, half, stratum in reversed(work)]
            for step in zip(*steps):
                for of_pair in step:
                    of_pair()

        def work_of(s, stratum, first_only=False):
            work = []
            for c in range(k):
                place = s + LEAD * c
                if place < 0 or (first_only and place >= SLOTS):
                    continue
                if place % SLOTS < HALF_STEPS:
                    work.append((c, place % SLOTS, stratum + place // SLOTS))
            return work

        def stratum_body(stratum, begins=False, moving=False, ends=False):
            if not begins:
                slot_in = stratum % n_devs
                arrival(leaving.at[0], arriving.at[slot_in], hop_recv.at[slot_in]).wait()
                hop(stratum - 1).wait_send()
            if moving:
                wait_block((first - stratum + n_devs) % n_devs)
                ask(stratum + AHEAD)

            fresh.clear()
            for s in range(SLOTS):
                slot(work_of(s, stratum, ends), None if ends else send_user)
            fresh.clear()

        def send_user(stratum):
            hop(stratum).start()

        for s in range(-LEAD * last, 0):
            slot(work_of(s, 0))

        for c in range(k):
            some = rated.at[first + c, :, pl.ds(0, last * items)]
            arrival(some, some, block_recv.at[first + c]).wait()

        stratum_body(0, begins=True)

        @pl.loop(1, n_devs - k + 1)
        def _(stratum):
            stratum_body(stratum, moving=True)

        @pl.loop(n_devs - k + 1, strata - 1)
        def _(stratum):
            stratum_body(stratum)

        stratum_body(strata - 1, ends=True)

        def end_copies(c):
            done = handed.at[c] if c < last else leaving.at[(strata - 1) % 2]
            block = first + c
            return (
                (done, user_out, end_send.at[2 * c], end_recv.at[0], (block + 1) % n_devs),
                (item_start.at[c], item_out, end_send.at[2 * c + 1], end_recv.at[1], block),
            )

        for c in range(k):
            item_start[c] = item[c].T
        for c in range(k):
            for copy in end_copies(c):
                send(*copy)
        for c in range(k):
            for copy in end_copies(c):
                wait_sent(*copy)


    @pl.when(home != me)
    def _():
        some = rated.at[me, :, pl.ds(0, last * items)]
        arrival(some, some, block_send.at[0]).wait()

    @pl.when(low)
    def _():
        @pl.loop(1, SOON)
        def _(turn):
            wait_sent(*block_copy(turn))

        @pl.loop(SOON, workers)
        def _(turn):
            to, _ = columns_of(me, turn)

            @pl.when(to != me)
            def _():
                up_copy(turn).wait_send()

    @pl.when(jnp.logical_not(low))
    def _():
        @pl.loop(SOON, workers)
        def _(turn):
            block_out(turn).wait_send()
            to, _ = columns_of(across, turn)

            @pl.when(to != across)
            def _():
                relay_copy(turn).wait_send()

    arrival(user_init, user_out, end_recv.at[0]).wait()
    arrival(item_init, item_out, end_recv.at[1]).wait()


def solution(mesh):
    n_devs = mesh.shape["shard"]
    row_spec = P(("rep", "shard"), None)
    k = ITEM_BLOCKS
    workers = n_devs // k

    def local(ratings, observed, user_init, item_init):
        users, rank = user_init.shape
        items = item_init.shape[0]
        wide = k * items
        step_scale = (users + items + rank) / math.sqrt(rank)
        step_size = 0.5 / step_scale
        weight_decay = 0.03 * math.sqrt(users * items / rank)
        dma = pltpu.SemaphoreType.DMA
        user_new, item_new = pl.pallas_call(
            functools.partial(kernel, n_devs, EPOCHS * n_devs, step_size, weight_decay),
            out_shape=(jax.ShapeDtypeStruct((users, rank), jnp.float32), jax.ShapeDtypeStruct((rank, items), jnp.float32)),
            in_specs=[pl.BlockSpec(memory_space=pl.ANY)] * 4,
            out_specs=(pl.BlockSpec(memory_space=pl.ANY),) * 2,
            scratch_shapes=[
                pltpu.VMEM((users, n_devs * items), jnp.float32),
                pltpu.VMEM((users, n_devs * items), jnp.int32),
                pltpu.VMEM((n_devs, users, wide), jnp.float32),
                pltpu.VMEM((k, items, users), jnp.float32),
                pltpu.VMEM((n_devs, users, rank), jnp.float32),
                pltpu.VMEM((k - 1, users, rank), jnp.float32),
                pltpu.VMEM((k - 1, users, rank), jnp.bfloat16),
                pltpu.VMEM((2, users, rank), jnp.float32),
                pltpu.VMEM((k, users, rank), jnp.float32),
                pltpu.VMEM((k, users, rank), jnp.bfloat16),
                pltpu.VMEM((k, items, rank), jnp.float32),
                pltpu.VMEM((k, items, rank), jnp.bfloat16),
                pltpu.VMEM((k, users, rank), jnp.float32),
                pltpu.VMEM((k, rank, items), jnp.float32),
                dma((workers,)),
                dma((workers,)),
                pltpu.SemaphoreType.REGULAR,
                pltpu.SemaphoreType.REGULAR,
                dma((workers,)),
                dma,
                dma((k,)),
                dma((workers,)),
                dma((n_devs,)),
                dma((2,)),
                dma((k,)),
                dma((k,)),
                dma((2,)),
                dma((n_devs,)),
                dma((2 * k,)),
                dma((2,)),
            ],
            compiler_params=pltpu.CompilerParams(has_side_effects=True, vmem_limit_bytes=60 * 2**20),
            name="strata",
        )(ratings, observed, user_init, item_init.T)
        return user_new, item_new.T

    return jax.shard_map(local, mesh=mesh, in_specs=(row_spec,) * 4, out_specs=(row_spec, row_spec), check_vma=False)
```

```python
import functools
import math

import jax
import jax.numpy as jnp
from jax import lax
from jax.experimental import pallas as pl
from jax.experimental.pallas import tpu as pltpu
from jax.sharding import PartitionSpec as P

STRATUM_STEPS = 4
EPOCHS = 2
ITEM_BLOCKS = 4
SLOTS = 9
UNASKED = 8
AHEAD = 12
SOON = 2
HALF_STEPS = 2 * STRATUM_STEPS
LEAD = SLOTS - HALF_STEPS + 1

ROW_BY_ROW = (((1,), (1,)), ((), ()))
PLAIN = (((1,), (0,)), ((), ()))


def dot(lhs, rhs, dims):
    return lax.dot_general(lhs, rhs, dims, preferred_element_type=jnp.float32)


def worker_device(worker, n_devs):
    if n_devs != 128:
        return worker
    plane = worker // 16
    place = worker + plane * (31 - 2 * worker)
    y = place // 4
    odd = y % 2
    x = place % 4
    x = x + odd * (3 - 2 * x)
    return ((plane * 4 + y) * 4 + x) * 2 + 1


def worker_of(dev, n_devs):
    if n_devs != 128:
        return dev
    chip = dev // 2
    plane = (chip // 16) % 2
    y = (chip // 4) % 4
    x = chip % 4
    place = y * 4 + x + (y % 2) * (3 - 2 * x)
    return place + plane * (31 - 2 * place)


def is_worker(dev, n_devs):
    if n_devs != 128:
        return dev < n_devs // ITEM_BLOCKS
    return jnp.logical_and(dev % 2 == 1, dev < 64)


def is_low(dev, n_devs):
    return dev < n_devs // 2


def mirror(dev, n_devs):
    quarter = n_devs // 4
    return dev + quarter * (3 - 2 * (dev // quarter))


def kernel(n_devs, strata, step_size, weight_decay, ratings, observed, user_init, item_init, user_out, item_out,
           masked, seen, rated, turned,
           arriving, handed, handed_bf, leaving, user, user_bf, item, item_bf, user_start, item_start,
           ratings_here, seen_here, more_own, more_relayed, relay_send, first_send, first_recv, block_send, block_recv,
           start_send, user_recv, item_recv, hop_send, hop_recv, end_send, end_recv):
    k = ITEM_BLOCKS
    workers = n_devs // k
    items = item_init.shape[1]
    wide = k * items
    me = lax.axis_index("shard")
    last = k - 1

    def remote(src, dst, send, recv, dev):
        return pltpu.make_async_remote_copy(
            src_ref=src, dst_ref=dst, send_sem=send, recv_sem=recv, device_id={"shard": dev}, device_id_type=pl.DeviceIdType.MESH
        )

    def arrival(like, dst, recv):
        return pltpu.make_async_copy(like, dst, recv)

    def send(src, dst, send_sem, recv_sem, dev):
        @pl.when(dev != me)
        def _():
            remote(src, dst, send_sem, recv_sem, dev).start()

        @pl.when(dev == me)
        def _():
            pltpu.make_async_copy(src, dst, recv_sem).start()

    def wait_sent(src, dst, send_sem, recv_sem, dev):
        @pl.when(dev != me)
        def _():
            remote(src, dst, send_sem, recv_sem, dev).wait_send()

    low = is_low(me, n_devs)
    across = mirror(me, n_devs)
    pair_here = me % k
    home = worker_device(me // k, n_devs)

    def columns_of(dev, turn):
        worker = (dev // k + turn) % workers
        return worker_device(worker, n_devs), pl.ds(pl.multiple_of(worker * wide, 128), wide)

    def fetch(turn):
        _, columns = columns_of(me, turn)
        return (
            pltpu.make_async_copy(ratings.at[:, columns], masked.at[:, columns], ratings_here.at[turn]),
            pltpu.make_async_copy(observed.at[:, columns], seen.at[:, columns], seen_here.at[turn]),
        )

    def mask(turn):
        for copy in fetch(turn):
            copy.wait()
        _, columns = columns_of(me, turn)
        masked[:, columns] = jnp.where(seen[:, columns] != 0, masked[:, columns], jnp.nan)

    for copy in fetch(0):
        copy.start()
    user_copy = (user_init, user_start.at[pair_here], start_send.at[0], user_recv.at[pair_here], home)
    item_copy = (item_init, item_start.at[pair_here], start_send.at[1], item_recv.at[pair_here], home)
    send(*user_copy)
    send(*item_copy)

    @pl.loop(1, workers)
    def _(turn):
        for copy in fetch(turn):
            copy.start()

    def part_copy(ahead):
        pair = (pair_here + ahead) % k
        here = pl.ds(pl.multiple_of((me // k) * wide + pair * items, 128), items)
        there = pl.ds(pl.multiple_of(pair * items, 128), items)
        sent, received = (first_send, first_recv.at[pair]) if ahead == 0 else (block_send.at[0], block_recv.at[me])
        return masked.at[:, here], rated.at[me, :, there], sent, received, home

    mask(0)
    for ahead in range(k):
        send(*part_copy(ahead))

    def block_copy(turn):
        to, columns = columns_of(me, turn)
        return masked.at[:, columns], rated.at[me], block_send.at[turn], block_recv.at[me], to

    def up_copy(turn):
        _, columns = columns_of(me, turn)
        return remote(masked.at[:, columns], rated.at[turn], block_send.at[turn], block_recv.at[turn], across)

    def relay_copy(turn):
        to, _ = columns_of(across, turn)
        return remote(rated.at[turn], rated.at[across], relay_send.at[turn], block_recv.at[across], to)

    def block_out(turn):
        return remote(*block_copy(turn))

    @pl.loop(1, SOON)
    def _(turn):
        mask(turn)

    wait_sent(*user_copy)
    wait_sent(*item_copy)
    wait_sent(*part_copy(0))

    @pl.loop(1, SOON)
    def _(turn):
        send(*block_copy(turn))

    def send_up():
        @pl.loop(SOON, workers)
        def _(turn):
            mask(turn)
            to, _ = columns_of(me, turn)

            @pl.when(to != me)
            def _():
                up_copy(turn).start()

            @pl.when(to == me)
            def _():
                source, target, _, received, _ = block_copy(turn)
                pltpu.make_async_copy(source, target, received).start()

    working = is_worker(me, n_devs)

    @pl.when(low)
    def _():
        send_up()

    @pl.when(jnp.logical_not(low))
    def _():
        @pl.loop(SOON, workers)
        def _(turn):
            mask(turn)

        @pl.loop(1, SOON)
        def _(turn):
            wait_sent(*block_copy(turn))

        @pl.loop(SOON, workers)
        def _(turn):
            to, _ = columns_of(across, turn)
            relays = to != across

            @pl.when(turn * k - me % k > UNASKED)
            def _():
                pl.semaphore_wait(more_own, 1)

                @pl.when(relays)
                def _():
                    pl.semaphore_wait(more_relayed, 1)

            block_out(turn).start()

            @pl.when(relays)
            def _():
                arrival(rated.at[turn], rated.at[turn], block_recv.at[turn]).wait()
                relay_copy(turn).start()

    @pl.when(working)
    def _():
        mine = worker_of(me, n_devs)
        first = mine * k
        after = worker_device((mine + 1) % workers, n_devs)

        def wait_block(block):
            arrival(rated.at[block], rated.at[block], block_recv.at[block]).wait()

        def hop(stratum):
            slot = (stratum + 1) % n_devs
            return remote(leaving.at[stratum % 2], arriving.at[slot], hop_send.at[stratum % 2], hop_recv.at[slot], after)

        for c in range(k):
            arrival(user_init, user_start.at[c], user_recv.at[c]).wait()
            arrival(item_init, item_start.at[c], item_recv.at[c]).wait()
            part = rated.at[first + c, :, c * items : (c + 1) * items]
            arrival(part, part, first_recv.at[c]).wait()
        def ask(stratum):
            asked = (first - stratum + 2 * n_devs) % n_devs

            @pl.when(jnp.logical_and(stratum <= n_devs - k, asked != me))
            def _():
                @pl.when(is_low(asked, n_devs))
                def _():
                    pl.semaphore_signal(more_relayed, inc=1, device_id={"shard": mirror(asked, n_devs)}, device_id_type=pl.DeviceIdType.MESH)

                @pl.when(jnp.logical_not(is_low(asked, n_devs)))
                def _():
                    pl.semaphore_signal(more_own, inc=1, device_id={"shard": asked}, device_id_type=pl.DeviceIdType.MESH)

        for stratum in range(UNASKED + 1, AHEAD + 1):
            ask(stratum)
        for c in range(k):
            if c == 0:
                arriving[0] = user_start[0]
            else:
                handed[c - 1] = user_start[c]
                handed_bf[c - 1] = user_start[c].astype(jnp.bfloat16)
            item[c] = item_start[c].T
            item_bf[c] = item[c].astype(jnp.bfloat16)

        def steps_of(c, half, stratum, send_user):
            kept = {}

            def predict():
                items_now = fresh.pop(("item", c)) if ("item", c) in fresh else item_bf[c]
                if half == 0 and c == 0:
                    users_now = arriving[stratum % n_devs].astype(jnp.bfloat16)
                elif half == 0:
                    users_now = fresh.pop(("handed", c)) if ("handed", c) in fresh else handed_bf[c - 1]
                else:
                    users_now = fresh.pop(("user", c)) if ("user", c) in fresh else user_bf[c]
                if half % 2 == 0:
                    kept["predicted"] = dot(users_now, items_now, ROW_BY_ROW)
                else:
                    kept["predicted"] = jnp.concatenate(
                        [dot(items_now[r : r + items // 2], users_now, ROW_BY_ROW) for r in (0, items // 2)], axis=0
                    )

            def descend():
                if half % 2 == 0:
                    block = (first + c - stratum + 2 * n_devs) % n_devs
                    known = rated[block, :, c * items : (c + 1) * items]
                    if half == 0:
                        turned[c] = known.T
                else:
                    known = turned[c]
                residual = jnp.where(known != known, 0.0, kept["predicted"] - known).astype(jnp.bfloat16)
                if half % 2 == 0:
                    kept["grad"] = dot(residual, item_bf[c], PLAIN)
                else:
                    rows = items // 2
                    kept["grad"] = jnp.concatenate([dot(residual[r : r + rows], user_bf[c], PLAIN) for r in (0, rows)], axis=0)

            def update():
                if half % 2 == 0:
                    if half > 0:
                        old = user[c]
                    elif c == 0:
                        old = arriving[stratum % n_devs]
                    else:
                        old = handed[c - 1]
                else:
                    old = item[c]
                new = old * (1 - step_size * weight_decay) - step_size * kept["grad"]
                new_bf = new.astype(jnp.bfloat16)
                if half % 2 == 1:
                    item[c] = new
                    item_bf[c] = new_bf
                    fresh["item", c] = new_bf
                    return
                user_bf[c] = new_bf
                fresh["user", c] = new_bf
                if half < HALF_STEPS - 2:
                    user[c] = new
                elif c < last:
                    handed[c] = new
                    handed_bf[c] = new_bf
                    fresh["handed", c + 1] = new_bf
                else:
                    leaving[stratum % 2] = new
                    if send_user is not None:
                        send_user()

            return predict, descend, update

        fresh = {}

        def slot(work, send_user=None, await_user=None):
            steps = [steps_of(c, half, stratum, send_user) for c, half, stratum in reversed(work)]
            for number, step in enumerate(zip(*steps)):
                for place, of_pair in enumerate(step):
                    if number == 0 and place == len(step) - 1 and await_user is not None:
                        await_user()
                    of_pair()

        def work_of(s, stratum, first_only=False):
            work = []
            for c in range(k):
                place = s + LEAD * c
                if place < 0 or (first_only and place >= SLOTS):
                    continue
                if place % SLOTS < HALF_STEPS:
                    work.append((c, place % SLOTS, stratum + place // SLOTS))
            return work

        def stratum_body(stratum, begins=False, moving=False, ends=False):
            def await_user():
                slot_in = stratum % n_devs
                arrival(leaving.at[0], arriving.at[slot_in], hop_recv.at[slot_in]).wait()

            if not begins:
                hop(stratum - 1).wait_send()
            if moving:
                wait_block((first - stratum + n_devs) % n_devs)

            def send_on():
                hop(stratum).start()
                if moving:
                    ask(stratum + AHEAD)

            fresh.clear()
            for s in range(SLOTS):
                slot(work_of(s, stratum, ends), None if ends else send_on, await_user if s == 0 and not begins else None)
            fresh.clear()

        for s in range(-LEAD * last, 0):
            slot(work_of(s, 0))

        for c in range(k):
            some = rated.at[first + c, :, pl.ds(0, last * items)]
            arrival(some, some, block_recv.at[first + c]).wait()

        stratum_body(0, begins=True)

        @pl.loop(1, n_devs - k + 1)
        def _(stratum):
            stratum_body(stratum, moving=True)

        @pl.loop(n_devs - k + 1, strata - 1)
        def _(stratum):
            stratum_body(stratum)

        stratum_body(strata - 1, ends=True)

        def end_copies(c):
            done = handed.at[c] if c < last else leaving.at[(strata - 1) % 2]
            block = first + c
            return (
                (done, user_out, end_send.at[2 * c], end_recv.at[0], (block + 1) % n_devs),
                (item_start.at[c], item_out, end_send.at[2 * c + 1], end_recv.at[1], block),
            )

        for c in range(k):
            item_start[c] = item[c].T
        for c in range(k):
            for copy in end_copies(c):
                send(*copy)
        for c in range(k):
            for copy in end_copies(c):
                wait_sent(*copy)


    @pl.when(home != me)
    def _():
        some = rated.at[me, :, pl.ds(0, last * items)]
        arrival(some, some, block_send.at[0]).wait()

    @pl.when(low)
    def _():
        @pl.loop(1, SOON)
        def _(turn):
            wait_sent(*block_copy(turn))

        @pl.loop(SOON, workers)
        def _(turn):
            to, _ = columns_of(me, turn)

            @pl.when(to != me)
            def _():
                up_copy(turn).wait_send()

    @pl.when(jnp.logical_not(low))
    def _():
        @pl.loop(SOON, workers)
        def _(turn):
            block_out(turn).wait_send()
            to, _ = columns_of(across, turn)

            @pl.when(to != across)
            def _():
                relay_copy(turn).wait_send()

    arrival(user_init, user_out, end_recv.at[0]).wait()
    arrival(item_init, item_out, end_recv.at[1]).wait()


def solution(mesh):
    n_devs = mesh.shape["shard"]
    row_spec = P(("rep", "shard"), None)
    k = ITEM_BLOCKS
    workers = n_devs // k

    def local(ratings, observed, user_init, item_init):
        users, rank = user_init.shape
        items = item_init.shape[0]
        wide = k * items
        step_scale = (users + items + rank) / math.sqrt(rank)
        step_size = 0.5 / step_scale
        weight_decay = 0.03 * math.sqrt(users * items / rank)
        dma = pltpu.SemaphoreType.DMA
        user_new, item_new = pl.pallas_call(
            functools.partial(kernel, n_devs, EPOCHS * n_devs, step_size, weight_decay),
            out_shape=(jax.ShapeDtypeStruct((users, rank), jnp.float32), jax.ShapeDtypeStruct((rank, items), jnp.float32)),
            in_specs=[pl.BlockSpec(memory_space=pl.ANY)] * 4,
            out_specs=(pl.BlockSpec(memory_space=pl.ANY),) * 2,
            scratch_shapes=[
                pltpu.VMEM((users, n_devs * items), jnp.float32),
                pltpu.VMEM((users, n_devs * items), jnp.int32),
                pltpu.VMEM((n_devs, users, wide), jnp.float32),
                pltpu.VMEM((k, items, users), jnp.float32),
                pltpu.VMEM((n_devs, users, rank), jnp.float32),
                pltpu.VMEM((k - 1, users, rank), jnp.float32),
                pltpu.VMEM((k - 1, users, rank), jnp.bfloat16),
                pltpu.VMEM((2, users, rank), jnp.float32),
                pltpu.VMEM((k, users, rank), jnp.float32),
                pltpu.VMEM((k, users, rank), jnp.bfloat16),
                pltpu.VMEM((k, items, rank), jnp.float32),
                pltpu.VMEM((k, items, rank), jnp.bfloat16),
                pltpu.VMEM((k, users, rank), jnp.float32),
                pltpu.VMEM((k, rank, items), jnp.float32),
                dma((workers,)),
                dma((workers,)),
                pltpu.SemaphoreType.REGULAR,
                pltpu.SemaphoreType.REGULAR,
                dma((workers,)),
                dma,
                dma((k,)),
                dma((workers,)),
                dma((n_devs,)),
                dma((2,)),
                dma((k,)),
                dma((k,)),
                dma((2,)),
                dma((n_devs,)),
                dma((2 * k,)),
                dma((2,)),
            ],
            compiler_params=pltpu.CompilerParams(has_side_effects=True, vmem_limit_bytes=60 * 2**20),
            name="strata",
        )(ratings, observed, user_init, item_init.T)
        return user_new, item_new.T

    return jax.shard_map(local, mesh=mesh, in_specs=(row_spec,) * 4, out_specs=(row_spec, row_spec), check_vma=False)
```

```python
import functools
import math

import jax
import jax.numpy as jnp
from jax import lax
from jax.experimental import pallas as pl
from jax.experimental.pallas import tpu as pltpu
from jax.sharding import PartitionSpec as P

STRATUM_STEPS = 4
EPOCHS = 2
ITEM_BLOCKS = 4
SLOTS = 9
UNASKED = 8
AHEAD = 12
SOON = 2
HALF_STEPS = 2 * STRATUM_STEPS
LEAD = SLOTS - HALF_STEPS + 1

ROW_BY_ROW = (((1,), (1,)), ((), ()))
PLAIN = (((1,), (0,)), ((), ()))


def dot(lhs, rhs, dims):
    return lax.dot_general(lhs, rhs, dims, preferred_element_type=jnp.float32)


def worker_device(worker, n_devs):
    if n_devs != 128:
        return worker
    plane = worker // 16
    place = worker + plane * (31 - 2 * worker)
    y = place // 4
    odd = y % 2
    x = place % 4
    x = x + odd * (3 - 2 * x)
    return ((plane * 4 + y) * 4 + x) * 2 + 1


def worker_of(dev, n_devs):
    if n_devs != 128:
        return dev
    chip = dev // 2
    plane = (chip // 16) % 2
    y = (chip // 4) % 4
    x = chip % 4
    place = y * 4 + x + (y % 2) * (3 - 2 * x)
    return place + plane * (31 - 2 * place)


def is_worker(dev, n_devs):
    if n_devs != 128:
        return dev < n_devs // ITEM_BLOCKS
    return jnp.logical_and(dev % 2 == 1, dev < 64)


def is_low(dev, n_devs):
    return dev < n_devs // 2


def mirror(dev, n_devs):
    quarter = n_devs // 4
    return dev + quarter * (3 - 2 * (dev // quarter))


def kernel(n_devs, strata, step_size, weight_decay, ratings, observed, user_init, item_init, user_out, item_out,
           masked, seen, rated, turned,
           arriving, handed, handed_bf, leaving, user, user_bf, item, item_bf, user_start, item_start,
           ratings_here, seen_here, more_own, more_relayed, relay_send, first_send, first_recv, block_send, block_recv,
           start_send, user_recv, item_recv, hop_send, hop_recv, end_send, end_recv):
    k = ITEM_BLOCKS
    workers = n_devs // k
    items = item_init.shape[1]
    wide = k * items
    me = lax.axis_index("shard")
    last = k - 1

    def remote(src, dst, send, recv, dev):
        return pltpu.make_async_remote_copy(
            src_ref=src, dst_ref=dst, send_sem=send, recv_sem=recv, device_id={"shard": dev}, device_id_type=pl.DeviceIdType.MESH
        )

    def arrival(like, dst, recv):
        return pltpu.make_async_copy(like, dst, recv)

    def send(src, dst, send_sem, recv_sem, dev):
        @pl.when(dev != me)
        def _():
            remote(src, dst, send_sem, recv_sem, dev).start()

        @pl.when(dev == me)
        def _():
            pltpu.make_async_copy(src, dst, recv_sem).start()

    def wait_sent(src, dst, send_sem, recv_sem, dev):
        @pl.when(dev != me)
        def _():
            remote(src, dst, send_sem, recv_sem, dev).wait_send()

    low = is_low(me, n_devs)
    across = mirror(me, n_devs)
    pair_here = me % k
    home = worker_device(me // k, n_devs)

    def columns_of(dev, turn):
        worker = (dev // k + turn) % workers
        return worker_device(worker, n_devs), pl.ds(pl.multiple_of(worker * wide, 128), wide)

    def fetch(turn):
        _, columns = columns_of(me, turn)
        return (
            pltpu.make_async_copy(ratings.at[:, columns], masked.at[:, columns], ratings_here.at[turn]),
            pltpu.make_async_copy(observed.at[:, columns], seen.at[:, columns], seen_here.at[turn]),
        )

    def mask(turn):
        for copy in fetch(turn):
            copy.wait()
        _, columns = columns_of(me, turn)
        masked[:, columns] = jnp.where(seen[:, columns] != 0, masked[:, columns], jnp.nan)

    for copy in fetch(0):
        copy.start()
    user_copy = (user_init, user_start.at[pair_here], start_send.at[0], user_recv.at[pair_here], home)
    item_copy = (item_init, item_start.at[pair_here], start_send.at[1], item_recv.at[pair_here], home)
    send(*user_copy)
    send(*item_copy)

    @pl.loop(1, workers)
    def _(turn):
        for copy in fetch(turn):
            copy.start()

    def part_copy(ahead):
        pair = (pair_here + ahead) % k
        here = pl.ds(pl.multiple_of((me // k) * wide + pair * items, 128), items)
        there = pl.ds(pl.multiple_of(pair * items, 128), items)
        sent, received = (first_send, first_recv.at[pair]) if ahead == 0 else (block_send.at[0], block_recv.at[me])
        return masked.at[:, here], rated.at[me, :, there], sent, received, home

    mask(0)
    for ahead in range(k):
        send(*part_copy(ahead))

    def block_copy(turn):
        to, columns = columns_of(me, turn)
        return masked.at[:, columns], rated.at[me], block_send.at[turn], block_recv.at[me], to

    def up_copy(turn):
        _, columns = columns_of(me, turn)
        return remote(masked.at[:, columns], rated.at[turn], block_send.at[turn], block_recv.at[turn], across)

    def relay_copy(turn):
        to, _ = columns_of(across, turn)
        return remote(rated.at[turn], rated.at[across], relay_send.at[turn], block_recv.at[across], to)

    def block_out(turn):
        return remote(*block_copy(turn))

    @pl.loop(1, SOON)
    def _(turn):
        mask(turn)

    wait_sent(*user_copy)
    wait_sent(*item_copy)
    wait_sent(*part_copy(0))

    @pl.loop(1, SOON)
    def _(turn):
        send(*block_copy(turn))

    def send_up():
        @pl.loop(SOON, workers)
        def _(turn):
            mask(turn)
            to, _ = columns_of(me, turn)

            @pl.when(to != me)
            def _():
                up_copy(turn).start()

            @pl.when(to == me)
            def _():
                source, target, _, received, _ = block_copy(turn)
                pltpu.make_async_copy(source, target, received).start()

    working = is_worker(me, n_devs)

    @pl.when(low)
    def _():
        send_up()

    @pl.when(jnp.logical_not(low))
    def _():
        @pl.loop(SOON, workers)
        def _(turn):
            mask(turn)

        @pl.loop(1, SOON)
        def _(turn):
            wait_sent(*block_copy(turn))

        @pl.loop(SOON, workers)
        def _(turn):
            to, _ = columns_of(across, turn)
            relays = to != across

            @pl.when(turn * k - me % k > UNASKED)
            def _():
                pl.semaphore_wait(more_own, 1)

                @pl.when(relays)
                def _():
                    pl.semaphore_wait(more_relayed, 1)

            block_out(turn).start()

            @pl.when(relays)
            def _():
                arrival(rated.at[turn], rated.at[turn], block_recv.at[turn]).wait()
                relay_copy(turn).start()

    @pl.when(working)
    def _():
        mine = worker_of(me, n_devs)
        first = mine * k
        after = worker_device((mine + 1) % workers, n_devs)

        def wait_block(block):
            arrival(rated.at[block], rated.at[block], block_recv.at[block]).wait()

        def hop(stratum):
            slot = (stratum + 1) % n_devs
            return remote(leaving.at[stratum % 2], arriving.at[slot], hop_send.at[stratum % 2], hop_recv.at[slot], after)

        for c in range(k):
            arrival(user_init, user_start.at[c], user_recv.at[c]).wait()
            arrival(item_init, item_start.at[c], item_recv.at[c]).wait()
            part = rated.at[first + c, :, c * items : (c + 1) * items]
            arrival(part, part, first_recv.at[c]).wait()
        def ask(stratum):
            asked = (first - stratum + 2 * n_devs) % n_devs

            @pl.when(jnp.logical_and(stratum <= n_devs - k, asked != me))
            def _():
                @pl.when(is_low(asked, n_devs))
                def _():
                    pl.semaphore_signal(more_relayed, inc=1, device_id={"shard": mirror(asked, n_devs)}, device_id_type=pl.DeviceIdType.MESH)

                @pl.when(jnp.logical_not(is_low(asked, n_devs)))
                def _():
                    pl.semaphore_signal(more_own, inc=1, device_id={"shard": asked}, device_id_type=pl.DeviceIdType.MESH)

        for stratum in range(UNASKED + 1, AHEAD + 1):
            ask(stratum)
        for c in range(k):
            if c == 0:
                arriving[0] = user_start[0]
            else:
                handed[c - 1] = user_start[c]
                handed_bf[c - 1] = user_start[c].astype(jnp.bfloat16)
            item[c] = item_start[c].T
            item_bf[c] = item[c].astype(jnp.bfloat16)

        def steps_of(c, half, stratum, send_user):
            kept = {}

            def predict():
                items_now = fresh.pop(("item", c)) if ("item", c) in fresh else item_bf[c]
                if half == 0 and c == 0:
                    users_now = arriving[stratum % n_devs].astype(jnp.bfloat16)
                elif half == 0:
                    users_now = fresh.pop(("handed", c)) if ("handed", c) in fresh else handed_bf[c - 1]
                else:
                    users_now = fresh.pop(("user", c)) if ("user", c) in fresh else user_bf[c]
                if half % 2 == 0:
                    kept["predicted"] = dot(users_now, items_now, ROW_BY_ROW)
                else:
                    kept["predicted"] = dot(items_now, users_now, ROW_BY_ROW)

            def descend():
                if half % 2 == 0:
                    block = (first + c - stratum + 2 * n_devs) % n_devs
                    known = rated[block, :, c * items : (c + 1) * items]
                    if half == 0:
                        turned[c] = known.T
                else:
                    known = turned[c]
                residual = jnp.where(known != known, 0.0, kept["predicted"] - known).astype(jnp.bfloat16)
                kept["grad"] = dot(residual, item_bf[c] if half % 2 == 0 else user_bf[c], PLAIN)

            def update():
                if half % 2 == 0:
                    if half > 0:
                        old = user[c]
                    elif c == 0:
                        old = arriving[stratum % n_devs]
                    else:
                        old = handed[c - 1]
                else:
                    old = item[c]
                new = old * (1 - step_size * weight_decay) - step_size * kept["grad"]
                new_bf = new.astype(jnp.bfloat16)
                if half % 2 == 1:
                    item[c] = new
                    item_bf[c] = new_bf
                    fresh["item", c] = new_bf
                    return
                user_bf[c] = new_bf
                fresh["user", c] = new_bf
                if half < HALF_STEPS - 2:
                    user[c] = new
                elif c < last:
                    handed[c] = new
                    handed_bf[c] = new_bf
                    fresh["handed", c + 1] = new_bf
                else:
                    leaving[stratum % 2] = new
                    if send_user is not None:
                        send_user()

            return predict, descend, update

        fresh = {}

        def slot(work, send_user=None):
            steps = [steps_of(c, half, stratum, send_user) for c, half, stratum in reversed(work)]
            for step in zip(*steps):
                for of_pair in step:
                    of_pair()

        def work_of(s, stratum, first_only=False):
            work = []
            for c in range(k):
                place = s + LEAD * c
                if place < 0 or (first_only and place >= SLOTS):
                    continue
                if place % SLOTS < HALF_STEPS:
                    work.append((c, place % SLOTS, stratum + place // SLOTS))
            return work

        def stratum_body(stratum, begins=False, moving=False, ends=False):
            def send_user():
                hop(stratum).start()
                if not begins:
                    hop(stratum - 1).wait_send()
                if moving:
                    ask(stratum + AHEAD)

            if not begins:
                slot_in = stratum % n_devs
                arrival(leaving.at[0], arriving.at[slot_in], hop_recv.at[slot_in]).wait()
            if ends:
                hop(stratum - 1).wait_send()
            if moving:
                wait_block((first - stratum + n_devs) % n_devs)

            fresh.clear()
            for s in range(SLOTS):
                slot(work_of(s, stratum, ends), None if ends else send_user)
            fresh.clear()

        for s in range(-LEAD * last, 0):
            slot(work_of(s, 0))

        for c in range(k):
            some = rated.at[first + c, :, pl.ds(0, last * items)]
            arrival(some, some, block_recv.at[first + c]).wait()

        stratum_body(0, begins=True)

        @pl.loop(1, n_devs - k + 1)
        def _(stratum):
            stratum_body(stratum, moving=True)

        @pl.loop(n_devs - k + 1, strata - 1)
        def _(stratum):
            stratum_body(stratum)

        stratum_body(strata - 1, ends=True)

        def end_copies(c):
            done = handed.at[c] if c < last else leaving.at[(strata - 1) % 2]
            block = first + c
            return (
                (done, user_out, end_send.at[2 * c], end_recv.at[0], (block + 1) % n_devs),
                (item_start.at[c], item_out, end_send.at[2 * c + 1], end_recv.at[1], block),
            )

        for c in range(k):
            item_start[c] = item[c].T
        for c in range(k):
            for copy in end_copies(c):
                send(*copy)
        for c in range(k):
            for copy in end_copies(c):
                wait_sent(*copy)


    @pl.when(home != me)
    def _():
        some = rated.at[me, :, pl.ds(0, last * items)]
        arrival(some, some, block_send.at[0]).wait()

    @pl.when(low)
    def _():
        @pl.loop(1, SOON)
        def _(turn):
            wait_sent(*block_copy(turn))

        @pl.loop(SOON, workers)
        def _(turn):
            to, _ = columns_of(me, turn)

            @pl.when(to != me)
            def _():
                up_copy(turn).wait_send()

    @pl.when(jnp.logical_not(low))
    def _():
        @pl.loop(SOON, workers)
        def _(turn):
            block_out(turn).wait_send()
            to, _ = columns_of(across, turn)

            @pl.when(to != across)
            def _():
                relay_copy(turn).wait_send()

    arrival(user_init, user_out, end_recv.at[0]).wait()
    arrival(item_init, item_out, end_recv.at[1]).wait()


def solution(mesh):
    n_devs = mesh.shape["shard"]
    row_spec = P(("rep", "shard"), None)
    k = ITEM_BLOCKS
    workers = n_devs // k

    def local(ratings, observed, user_init, item_init):
        users, rank = user_init.shape
        items = item_init.shape[0]
        wide = k * items
        step_scale = (users + items + rank) / math.sqrt(rank)
        step_size = 0.5 / step_scale
        weight_decay = 0.03 * math.sqrt(users * items / rank)
        dma = pltpu.SemaphoreType.DMA
        user_new, item_new = pl.pallas_call(
            functools.partial(kernel, n_devs, EPOCHS * n_devs, step_size, weight_decay),
            out_shape=(jax.ShapeDtypeStruct((users, rank), jnp.float32), jax.ShapeDtypeStruct((rank, items), jnp.float32)),
            in_specs=[pl.BlockSpec(memory_space=pl.ANY)] * 4,
            out_specs=(pl.BlockSpec(memory_space=pl.ANY),) * 2,
            scratch_shapes=[
                pltpu.VMEM((users, n_devs * items), jnp.float32),
                pltpu.VMEM((users, n_devs * items), jnp.int32),
                pltpu.VMEM((n_devs, users, wide), jnp.float32),
                pltpu.VMEM((k, items, users), jnp.float32),
                pltpu.VMEM((n_devs, users, rank), jnp.float32),
                pltpu.VMEM((k - 1, users, rank), jnp.float32),
                pltpu.VMEM((k - 1, users, rank), jnp.bfloat16),
                pltpu.VMEM((2, users, rank), jnp.float32),
                pltpu.VMEM((k, users, rank), jnp.float32),
                pltpu.VMEM((k, users, rank), jnp.bfloat16),
                pltpu.VMEM((k, items, rank), jnp.float32),
                pltpu.VMEM((k, items, rank), jnp.bfloat16),
                pltpu.VMEM((k, users, rank), jnp.float32),
                pltpu.VMEM((k, rank, items), jnp.float32),
                dma((workers,)),
                dma((workers,)),
                pltpu.SemaphoreType.REGULAR,
                pltpu.SemaphoreType.REGULAR,
                dma((workers,)),
                dma,
                dma((k,)),
                dma((workers,)),
                dma((n_devs,)),
                dma((2,)),
                dma((k,)),
                dma((k,)),
                dma((2,)),
                dma((n_devs,)),
                dma((2 * k,)),
                dma((2,)),
            ],
            compiler_params=pltpu.CompilerParams(has_side_effects=True, vmem_limit_bytes=60 * 2**20),
            name="strata",
        )(ratings, observed, user_init, item_init.T)
        return user_new, item_new.T

    return jax.shard_map(local, mesh=mesh, in_specs=(row_spec,) * 4, out_specs=(row_spec, row_spec), check_vma=False)
```

```python
import functools
import math

import jax
import jax.numpy as jnp
from jax import lax
from jax.experimental import pallas as pl
from jax.experimental.pallas import tpu as pltpu
from jax.sharding import PartitionSpec as P

STRATUM_STEPS = 4
EPOCHS = 2
ITEM_BLOCKS = 4
SLOTS = 9
UNASKED = 8
AHEAD = 12
SOON = 2
HALF_STEPS = 2 * STRATUM_STEPS
LEAD = SLOTS - HALF_STEPS + 1

ROW_BY_ROW = (((1,), (1,)), ((), ()))
PLAIN = (((1,), (0,)), ((), ()))


LANES = 128


def joined(first, second, place):
    return jnp.concatenate([first[place], second[place]], axis=1)


def put(first, second, place, values):
    first[place] = values[:, :LANES]
    second[place] = values[:, LANES:]


def dot(lhs, rhs, dims):
    return lax.dot_general(lhs, rhs, dims, preferred_element_type=jnp.float32)


def worker_device(worker, n_devs):
    if n_devs != 128:
        return worker
    plane = worker // 16
    place = worker + plane * (31 - 2 * worker)
    y = place // 4
    odd = y % 2
    x = place % 4
    x = x + odd * (3 - 2 * x)
    return ((plane * 4 + y) * 4 + x) * 2 + 1


def worker_of(dev, n_devs):
    if n_devs != 128:
        return dev
    chip = dev // 2
    plane = (chip // 16) % 2
    y = (chip // 4) % 4
    x = chip % 4
    place = y * 4 + x + (y % 2) * (3 - 2 * x)
    return place + plane * (31 - 2 * place)


def is_worker(dev, n_devs):
    if n_devs != 128:
        return dev < n_devs // ITEM_BLOCKS
    return jnp.logical_and(dev % 2 == 1, dev < 64)


def is_low(dev, n_devs):
    return dev < n_devs // 2


def mirror(dev, n_devs):
    quarter = n_devs // 4
    return dev + quarter * (3 - 2 * (dev // quarter))


def kernel(n_devs, strata, step_size, weight_decay, ratings, observed, user_init, item_init, user_out, item_out,
           masked, seen, rated, turned,
           arriving, arriving_2, handed, handed_bf, leaving, leaving_2, user, user_bf, item, item_bf, user_start, item_start,
           ratings_here, seen_here, more_own, more_relayed, relay_send, first_send, first_recv, block_send, block_recv,
           start_send, user_recv, item_recv, hop_send, hop_recv, hop_send_2, hop_recv_2, end_send, end_recv):
    k = ITEM_BLOCKS
    workers = n_devs // k
    items = item_init.shape[1]
    wide = k * items
    me = lax.axis_index("shard")
    last = k - 1

    def remote(src, dst, send, recv, dev):
        return pltpu.make_async_remote_copy(
            src_ref=src, dst_ref=dst, send_sem=send, recv_sem=recv, device_id={"shard": dev}, device_id_type=pl.DeviceIdType.MESH
        )

    def arrival(like, dst, recv):
        return pltpu.make_async_copy(like, dst, recv)

    def send(src, dst, send_sem, recv_sem, dev):
        @pl.when(dev != me)
        def _():
            remote(src, dst, send_sem, recv_sem, dev).start()

        @pl.when(dev == me)
        def _():
            pltpu.make_async_copy(src, dst, recv_sem).start()

    def wait_sent(src, dst, send_sem, recv_sem, dev):
        @pl.when(dev != me)
        def _():
            remote(src, dst, send_sem, recv_sem, dev).wait_send()

    low = is_low(me, n_devs)
    across = mirror(me, n_devs)
    pair_here = me % k
    home = worker_device(me // k, n_devs)

    def columns_of(dev, turn):
        worker = (dev // k + turn) % workers
        return worker_device(worker, n_devs), pl.ds(pl.multiple_of(worker * wide, 128), wide)

    def fetch(turn):
        _, columns = columns_of(me, turn)
        return (
            pltpu.make_async_copy(ratings.at[:, columns], masked.at[:, columns], ratings_here.at[turn]),
            pltpu.make_async_copy(observed.at[:, columns], seen.at[:, columns], seen_here.at[turn]),
        )

    def mask(turn):
        for copy in fetch(turn):
            copy.wait()
        _, columns = columns_of(me, turn)
        masked[:, columns] = jnp.where(seen[:, columns] != 0, masked[:, columns], jnp.nan)

    for copy in fetch(0):
        copy.start()
    user_copy = (user_init, user_start.at[pair_here], start_send.at[0], user_recv.at[pair_here], home)
    item_copy = (item_init, item_start.at[pair_here], start_send.at[1], item_recv.at[pair_here], home)
    send(*user_copy)
    send(*item_copy)

    @pl.loop(1, workers)
    def _(turn):
        for copy in fetch(turn):
            copy.start()

    def part_copy(ahead):
        pair = (pair_here + ahead) % k
        here = pl.ds(pl.multiple_of((me // k) * wide + pair * items, 128), items)
        there = pl.ds(pl.multiple_of(pair * items, 128), items)
        sent, received = (first_send, first_recv.at[pair]) if ahead == 0 else (block_send.at[0], block_recv.at[me])
        return masked.at[:, here], rated.at[me, :, there], sent, received, home

    mask(0)
    for ahead in range(k):
        send(*part_copy(ahead))

    def block_copy(turn):
        to, columns = columns_of(me, turn)
        return masked.at[:, columns], rated.at[me], block_send.at[turn], block_recv.at[me], to

    def up_copy(turn):
        _, columns = columns_of(me, turn)
        return remote(masked.at[:, columns], rated.at[turn], block_send.at[turn], block_recv.at[turn], across)

    def relay_copy(turn):
        to, _ = columns_of(across, turn)
        return remote(rated.at[turn], rated.at[across], relay_send.at[turn], block_recv.at[across], to)

    def block_out(turn):
        return remote(*block_copy(turn))

    @pl.loop(1, SOON)
    def _(turn):
        mask(turn)

    wait_sent(*user_copy)
    wait_sent(*item_copy)
    wait_sent(*part_copy(0))

    @pl.loop(1, SOON)
    def _(turn):
        send(*block_copy(turn))

    def send_up():
        @pl.loop(SOON, workers)
        def _(turn):
            mask(turn)
            to, _ = columns_of(me, turn)

            @pl.when(to != me)
            def _():
                up_copy(turn).start()

            @pl.when(to == me)
            def _():
                source, target, _, received, _ = block_copy(turn)
                pltpu.make_async_copy(source, target, received).start()

    working = is_worker(me, n_devs)

    @pl.when(low)
    def _():
        send_up()

    @pl.when(jnp.logical_not(low))
    def _():
        @pl.loop(SOON, workers)
        def _(turn):
            mask(turn)

        @pl.loop(1, SOON)
        def _(turn):
            wait_sent(*block_copy(turn))

        @pl.loop(SOON, workers)
        def _(turn):
            to, _ = columns_of(across, turn)
            relays = to != across

            @pl.when(turn * k - me % k > UNASKED)
            def _():
                pl.semaphore_wait(more_own, 1)

                @pl.when(relays)
                def _():
                    pl.semaphore_wait(more_relayed, 1)

            block_out(turn).start()

            @pl.when(relays)
            def _():
                arrival(rated.at[turn], rated.at[turn], block_recv.at[turn]).wait()
                relay_copy(turn).start()

    @pl.when(working)
    def _():
        mine = worker_of(me, n_devs)
        first = mine * k
        after = worker_device((mine + 1) % workers, n_devs)

        def wait_block(block):
            arrival(rated.at[block], rated.at[block], block_recv.at[block]).wait()

        def hop(stratum):
            here, there = stratum % 2, (stratum + 1) % n_devs
            return (
                remote(leaving.at[here], arriving.at[there], hop_send.at[here], hop_recv.at[there], after),
                remote(leaving_2.at[here], arriving_2.at[there], hop_send_2.at[here], hop_recv_2.at[there], after),
            )

        for c in range(k):
            arrival(user_init, user_start.at[c], user_recv.at[c]).wait()
            arrival(item_init, item_start.at[c], item_recv.at[c]).wait()
            part = rated.at[first + c, :, c * items : (c + 1) * items]
            arrival(part, part, first_recv.at[c]).wait()
        def ask(stratum):
            asked = (first - stratum + 2 * n_devs) % n_devs

            @pl.when(jnp.logical_and(stratum <= n_devs - k, asked != me))
            def _():
                @pl.when(is_low(asked, n_devs))
                def _():
                    pl.semaphore_signal(more_relayed, inc=1, device_id={"shard": mirror(asked, n_devs)}, device_id_type=pl.DeviceIdType.MESH)

                @pl.when(jnp.logical_not(is_low(asked, n_devs)))
                def _():
                    pl.semaphore_signal(more_own, inc=1, device_id={"shard": asked}, device_id_type=pl.DeviceIdType.MESH)

        for stratum in range(UNASKED + 1, AHEAD + 1):
            ask(stratum)
        for c in range(k):
            if c == 0:
                put(arriving, arriving_2, 0, user_start[0])
            else:
                handed[c - 1] = user_start[c]
                handed_bf[c - 1] = user_start[c].astype(jnp.bfloat16)
            item[c] = item_start[c].T
            item_bf[c] = item[c].astype(jnp.bfloat16)

        def steps_of(c, half, stratum, send_user):
            kept = {}

            def predict():
                items_now = fresh.pop(("item", c)) if ("item", c) in fresh else item_bf[c]
                if half == 0 and c == 0:
                    kept["arrived"] = joined(arriving, arriving_2, stratum % n_devs)
                    users_now = kept["arrived"].astype(jnp.bfloat16)
                elif half == 0:
                    users_now = fresh.pop(("handed", c)) if ("handed", c) in fresh else handed_bf[c - 1]
                else:
                    users_now = fresh.pop(("user", c)) if ("user", c) in fresh else user_bf[c]
                if half % 2 == 0:
                    kept["predicted"] = dot(users_now, items_now, ROW_BY_ROW)
                else:
                    kept["predicted"] = dot(items_now, users_now, ROW_BY_ROW)

            def descend():
                if half % 2 == 0:
                    block = (first + c - stratum + 2 * n_devs) % n_devs
                    known = rated[block, :, c * items : (c + 1) * items]
                    if half == 0:
                        turned[c] = known.T
                else:
                    known = turned[c]
                residual = jnp.where(known != known, 0.0, kept["predicted"] - known).astype(jnp.bfloat16)
                kept["grad"] = dot(residual, item_bf[c] if half % 2 == 0 else user_bf[c], PLAIN)

            def update():
                if half % 2 == 0:
                    if half > 0:
                        old = user[c]
                    elif c == 0:
                        old = kept["arrived"]
                    else:
                        old = handed[c - 1]
                else:
                    old = item[c]
                new = old * (1 - step_size * weight_decay) - step_size * kept["grad"]
                new_bf = new.astype(jnp.bfloat16)
                if half % 2 == 1:
                    item[c] = new
                    item_bf[c] = new_bf
                    fresh["item", c] = new_bf
                    return
                user_bf[c] = new_bf
                fresh["user", c] = new_bf
                if half < HALF_STEPS - 2:
                    user[c] = new
                elif c < last:
                    handed[c] = new
                    handed_bf[c] = new_bf
                    fresh["handed", c + 1] = new_bf
                else:
                    put(leaving, leaving_2, stratum % 2, new)
                    if send_user is not None:
                        send_user()

            return predict, descend, update

        fresh = {}

        def slot(work, send_user=None):
            steps = [steps_of(c, half, stratum, send_user) for c, half, stratum in reversed(work)]
            for step in zip(*steps):
                for of_pair in step:
                    of_pair()

        def work_of(s, stratum, first_only=False):
            work = []
            for c in range(k):
                place = s + LEAD * c
                if place < 0 or (first_only and place >= SLOTS):
                    continue
                if place % SLOTS < HALF_STEPS:
                    work.append((c, place % SLOTS, stratum + place // SLOTS))
            return work

        def stratum_body(stratum, begins=False, moving=False, ends=False):
            def send_user():
                for copy in hop(stratum):
                    copy.start()
                if not begins:
                    for copy in hop(stratum - 1):
                        copy.wait_send()
                if moving:
                    ask(stratum + AHEAD)

            if not begins:
                slot_in = stratum % n_devs
                arrival(leaving.at[0], arriving.at[slot_in], hop_recv.at[slot_in]).wait()
                arrival(leaving_2.at[0], arriving_2.at[slot_in], hop_recv_2.at[slot_in]).wait()
            if ends:
                for copy in hop(stratum - 1):
                    copy.wait_send()
            if moving:
                wait_block((first - stratum + n_devs) % n_devs)

            fresh.clear()
            for s in range(SLOTS):
                slot(work_of(s, stratum, ends), None if ends else send_user)
            fresh.clear()

        for s in range(-LEAD * last, 0):
            slot(work_of(s, 0))

        for c in range(k):
            some = rated.at[first + c, :, pl.ds(0, last * items)]
            arrival(some, some, block_recv.at[first + c]).wait()

        stratum_body(0, begins=True)

        @pl.loop(1, n_devs - k + 1)
        def _(stratum):
            stratum_body(stratum, moving=True)

        @pl.loop(n_devs - k + 1, strata - 1)
        def _(stratum):
            stratum_body(stratum)

        stratum_body(strata - 1, ends=True)

        def end_copies(c):
            done = handed.at[c] if c < last else user_start.at[last]
            block = first + c
            return (
                (done, user_out, end_send.at[2 * c], end_recv.at[0], (block + 1) % n_devs),
                (item_start.at[c], item_out, end_send.at[2 * c + 1], end_recv.at[1], block),
            )

        user_start[last] = joined(leaving, leaving_2, (strata - 1) % 2)
        for c in range(k):
            item_start[c] = item[c].T
        for c in range(k):
            for copy in end_copies(c):
                send(*copy)
        for c in range(k):
            for copy in end_copies(c):
                wait_sent(*copy)


    @pl.when(home != me)
    def _():
        some = rated.at[me, :, pl.ds(0, last * items)]
        arrival(some, some, block_send.at[0]).wait()

    @pl.when(low)
    def _():
        @pl.loop(1, SOON)
        def _(turn):
            wait_sent(*block_copy(turn))

        @pl.loop(SOON, workers)
        def _(turn):
            to, _ = columns_of(me, turn)

            @pl.when(to != me)
            def _():
                up_copy(turn).wait_send()

    @pl.when(jnp.logical_not(low))
    def _():
        @pl.loop(SOON, workers)
        def _(turn):
            block_out(turn).wait_send()
            to, _ = columns_of(across, turn)

            @pl.when(to != across)
            def _():
                relay_copy(turn).wait_send()

    arrival(user_init, user_out, end_recv.at[0]).wait()
    arrival(item_init, item_out, end_recv.at[1]).wait()


def solution(mesh):
    n_devs = mesh.shape["shard"]
    row_spec = P(("rep", "shard"), None)
    k = ITEM_BLOCKS
    workers = n_devs // k

    def local(ratings, observed, user_init, item_init):
        users, rank = user_init.shape
        items = item_init.shape[0]
        wide = k * items
        step_scale = (users + items + rank) / math.sqrt(rank)
        step_size = 0.5 / step_scale
        weight_decay = 0.03 * math.sqrt(users * items / rank)
        dma = pltpu.SemaphoreType.DMA
        user_new, item_new = pl.pallas_call(
            functools.partial(kernel, n_devs, EPOCHS * n_devs, step_size, weight_decay),
            out_shape=(jax.ShapeDtypeStruct((users, rank), jnp.float32), jax.ShapeDtypeStruct((rank, items), jnp.float32)),
            in_specs=[pl.BlockSpec(memory_space=pl.ANY)] * 4,
            out_specs=(pl.BlockSpec(memory_space=pl.ANY),) * 2,
            scratch_shapes=[
                pltpu.VMEM((users, n_devs * items), jnp.float32),
                pltpu.VMEM((users, n_devs * items), jnp.int32),
                pltpu.VMEM((n_devs, users, wide), jnp.float32),
                pltpu.VMEM((k, items, users), jnp.float32),
                pltpu.VMEM((n_devs, users, LANES), jnp.float32),
                pltpu.VMEM((n_devs, users, rank - LANES), jnp.float32),
                pltpu.VMEM((k - 1, users, rank), jnp.float32),
                pltpu.VMEM((k - 1, users, rank), jnp.bfloat16),
                pltpu.VMEM((2, users, LANES), jnp.float32),
                pltpu.VMEM((2, users, rank - LANES), jnp.float32),
                pltpu.VMEM((k, users, rank), jnp.float32),
                pltpu.VMEM((k, users, rank), jnp.bfloat16),
                pltpu.VMEM((k, items, rank), jnp.float32),
                pltpu.VMEM((k, items, rank), jnp.bfloat16),
                pltpu.VMEM((k, users, rank), jnp.float32),
                pltpu.VMEM((k, rank, items), jnp.float32),
                dma((workers,)),
                dma((workers,)),
                pltpu.SemaphoreType.REGULAR,
                pltpu.SemaphoreType.REGULAR,
                dma((workers,)),
                dma,
                dma((k,)),
                dma((workers,)),
                dma((n_devs,)),
                dma((2,)),
                dma((k,)),
                dma((k,)),
                dma((2,)),
                dma((n_devs,)),
                dma((2,)),
                dma((n_devs,)),
                dma((2 * k,)),
                dma((2,)),
            ],
            compiler_params=pltpu.CompilerParams(has_side_effects=True, vmem_limit_bytes=60 * 2**20),
            name="strata",
        )(ratings, observed, user_init, item_init.T)
        return user_new, item_new.T

    return jax.shard_map(local, mesh=mesh, in_specs=(row_spec,) * 4, out_specs=(row_spec, row_spec), check_vma=False)
```
